32 devices in a mesh: dp: 8 (over y, x, core), mp: 4 (over z).
Axes of the slice: x: 2, y: 2, z: 4, core: 2. Of those that a mesh axis runs over, the one named last changes fastest.
Arguments:
- grad_parts: bfloat16 [8, 4, 1024, 4096], P('dp', None, None, 'mp'), may hold values from -4000 to 4000
- master: float32 [4, 1024, 4096], P(None, 'dp', 'mp'), may hold values from -6 to 6
- first_moment: float32 [4, 1024, 4096], P(None, 'dp', 'mp'), may hold values from -4 to 4
- second_moment: float32 [4, 1024, 4096], P(None, 'dp', 'mp'), may hold values from 0.25 to 4
- left_basis: bfloat16 [4, 1024, 4096], P(None, 'dp', 'mp'), may hold values from -1 to 1, as said below
- right_basis: bfloat16 [4, 1024, 4096], P(None, 'dp', 'mp'), may hold values from -1 to 1, as said below
Outputs:
- weights: bfloat16 [4, 1024, 4096], P(None, None, 'mp')
- new_master: float32 [4, 1024, 4096], P(None, 'dp', 'mp')
- new_first: float32 [4, 1024, 4096], P(None, 'dp', 'mp')
- new_second: float32 [4, 1024, 4096], P(None, 'dp', 'mp')
The draws below stay inside these ranges and needn't reach their ends.
Inputs may be any that keep to these rules, and one draw needn't show every extreme that they name: Each block left_basis[i, :, j * 1024 : (j + 1) * 1024] is an orthogonal 1024 x 1024 matrix up to rounding. Each block right_basis[i, :, j * 1024 : (j + 1) * 1024] is an orthogonal 1024 x 1024 matrix up to rounding.
All inputs are finite; a program needn't handle non-finite values.
Results may differ from the reference program's by a relative error of at most 0.02.
Values may be sent and summed in bfloat16 or wider, within the bound.
A program may use at most 128 MiB of HBM per device.

```python
import math
import jax
import jax.numpy as jnp
from jax import lax

D = 4096
BLK = 1024
STEP = 10
NB = 4
N_DP = 8


def orthogonal_blocks(key):
    block_count = D // BLK
    normal_part = jax.random.normal(key, (block_count, block_count, BLK, BLK), jnp.float32)
    factors = jnp.linalg.qr(normal_part)
    return factors[0].transpose(0, 2, 1, 3).reshape(block_count, BLK, D).astype(jnp.bfloat16)


def draw_left_basis(key, part):
    return orthogonal_blocks(jax.random.fold_in(key, 21))


def draw_right_basis(key, part):
    return orthogonal_blocks(jax.random.fold_in(key, 22))


def draw_grad_parts(key, part):
    subkeys = jax.random.split(jax.random.fold_in(key, 11), 5)
    places = jnp.arange(D, dtype=jnp.float32) / D
    row_scale = 10.0 ** (places + 0.3 * jax.random.uniform(subkeys[0], (D,), jnp.float32) - 0.15)
    column_scale = 10.0 ** (places + 0.3 * jax.random.uniform(subkeys[1], (D,), jnp.float32) - 0.15)
    normal_part = jax.random.normal(subkeys[4], (N_DP, D, D), jnp.float32)
    scaled = normal_part * row_scale[None, :, None] * column_scale[None, None, :]
    return scaled.reshape(N_DP, D // BLK, BLK, D).astype(jnp.bfloat16)


def level_of(stream_key, extent, cuts, least, top_value):
    factor_of = 1.0
    for position, blocks in cuts:
        steps = jax.random.uniform(jax.random.fold_in(jax.random.fold_in(stream_key, 6), position), (blocks,), jnp.float32, least / len(cuts), top_value / len(cuts))
        factor_of = factor_of * jnp.repeat(jnp.exp(steps), extent[position] // blocks).reshape((-1,) + (1,) * (len(extent) - 1 - position))
    return factor_of


def scatter_about(rng, shape, width, reach, cuts=(), held_as=jnp.bfloat16):
    entries = jax.random.normal(rng, shape, jnp.float32) * width
    if len(cuts) > 0:
        entries = level_of(rng, shape, cuts, -0.22, 0.18) * entries
    return jnp.clip(entries, min=-reach, max=reach).astype(held_as)


def setup_inputs(seed: int = 0) -> dict:
    splits = jax.random.split(jax.random.key(seed), 7)
    grad_parts = draw_grad_parts(jax.random.fold_in(splits[6], 71), 0)
    master = scatter_about(splits[1], (NB, BLK, D), 1.0, 6.0, ((1, 8), (2, 4)), jnp.float32)
    first_moment = scatter_about(splits[2], (NB, BLK, D), 0.5, 4.0, ((1, 8), (2, 4)), jnp.float32)
    second_moment = jnp.clip(jnp.exp(math.log(4.0) - 2.7725887 * jax.random.uniform(splits[3], (NB, BLK, D), jnp.float32) ** level_of(splits[3], (NB, BLK, D), ((1, 8), (2, 4)), -0.2, 0.2)), 0.25, 4.0)
    left_basis = draw_left_basis(jax.random.fold_in(splits[6], 71), 0)
    right_basis = draw_right_basis(jax.random.fold_in(splits[6], 71), 0)
    return dict(grad_parts=grad_parts, master=master, first_moment=first_moment, second_moment=second_moment, left_basis=left_basis, right_basis=right_basis)


beta_one = 0.95
beta_two = 0.95
epsilon = 1e-08
norm_epsilon = 1e-06
learning_rate = 0.3
decay_rate = 0.1

def reference(grad_parts, master, first_moment, second_moment, left_basis, right_basis):

    def add_part(running_sum, partial_value):
        return (running_sum + partial_value.astype(jnp.float32).reshape(D, D), None)
    gradient, unused_out = lax.scan(add_part, jnp.zeros((D, D), jnp.float32), grad_parts)
    squares_sum = jnp.sum(gradient * gradient)
    clip_scale = jnp.minimum(1.0, 2.0 * D / jnp.sqrt(squares_sum + norm_epsilon))
    grad_low = gradient.astype(jnp.bfloat16)
    master_flat = master.reshape(D, D)
    first_flat = first_moment.reshape(D, D)
    second_flat = second_moment.reshape(D, D)
    left_flat = left_basis.reshape(D, D)
    right_flat = right_basis.reshape(D, D)
    owner_rows = BLK // N_DP
    group_size = N_DP
    block_count = D // BLK
    bias_one = 1.0 - beta_one ** STEP
    bias_two = 1.0 - beta_two ** STEP
    master_rows, first_rows, second_rows = ([], [], [])
    for block_row in range(block_count):
        master_cols, first_cols, second_cols = ([], [], [])
        for block_column in range(block_count):
            row_span = slice(block_row * BLK, (block_row + 1) * BLK)
            column_span = slice(block_column * BLK, (block_column + 1) * BLK)
            grad_block = grad_low[row_span, column_span]
            left_block = left_flat[row_span, column_span]
            right_block = right_flat[row_span, column_span]
            turned = jnp.dot(grad_block.astype(jnp.float32), right_block.astype(jnp.float32), preferred_element_type=jnp.float32).astype(jnp.bfloat16)
            block_terms = jnp.einsum('gra,grb->gab', left_block.reshape(group_size, owner_rows, BLK).astype(jnp.float32), turned.reshape(group_size, owner_rows, BLK).astype(jnp.float32))
            rounded_terms = lax.optimization_barrier(block_terms.astype(jnp.bfloat16))
            rotated = lax.optimization_barrier(jnp.sum(rounded_terms.astype(jnp.float32), axis=0))
            clipped = clip_scale * rotated
            first_new = beta_one * first_flat[row_span, column_span] + (1.0 - beta_one) * clipped
            second_new = beta_two * second_flat[row_span, column_span] + (1.0 - beta_two) * clipped * clipped
            direction = (first_new / bias_one / (jnp.sqrt(second_new / bias_two) + epsilon)).astype(jnp.bfloat16)
            back_rows = jnp.dot(direction.astype(jnp.float32), right_block.T.astype(jnp.float32), preferred_element_type=jnp.float32).astype(jnp.bfloat16)
            update = jnp.dot(left_block.astype(jnp.float32), back_rows.astype(jnp.float32), preferred_element_type=jnp.float32)
            master_new = master_flat[row_span, column_span] * (1.0 - learning_rate * decay_rate) - learning_rate * update
            master_cols.append(master_new)
            first_cols.append(first_new)
            second_cols.append(second_new)
        master_rows.append(jnp.concatenate(master_cols, axis=1))
        first_rows.append(jnp.concatenate(first_cols, axis=1))
        second_rows.append(jnp.concatenate(second_cols, axis=1))
    new_master = jnp.concatenate(master_rows, axis=0).reshape(D // BLK, BLK, D)
    new_first = jnp.concatenate(first_rows, axis=0).reshape(D // BLK, BLK, D)
    new_second = jnp.concatenate(second_rows, axis=0).reshape(D // BLK, BLK, D)
    return (new_master.astype(jnp.bfloat16), new_master, new_first, new_second)
```

```python
import functools

import jax
import jax.numpy as jnp
from jax import lax
from jax.experimental import pallas as pl
from jax.experimental.pallas import tpu as pltpu
from jax.sharding import PartitionSpec as P

D = 4096
STEP = 10


beta_one = 0.95
beta_two = 0.95
epsilon = 1e-08
norm_epsilon = 1e-06
learning_rate = 0.3
decay_rate = 0.1

VMEM = pl.BlockSpec(memory_space=pltpu.VMEM)
MESH = pl.DeviceIdType.MESH


def remote(src, dst, send, recv, axis, index):
    return pltpu.make_async_remote_copy(
        src_ref=src,
        dst_ref=dst,
        send_sem=send,
        recv_sem=recv,
        device_id={axis: index},
        device_id_type=MESH,
    )


def enter(axes):
    barrier = pltpu.get_barrier_semaphore()
    total = 0
    for axis, size in axes:
        me = lax.axis_index(axis)
        for step in range(1, size):
            pl.semaphore_signal(
                barrier,
                inc=1,
                device_id={axis: lax.rem(me + step, size)},
                device_id_type=MESH,
            )
        total += size - 1
    pl.semaphore_wait(barrier, total)


class Gather:
    def __init__(self, n, nb, x, y, local, first, recv, second):
        self.n, self.nb, self.q = n, nb, n // nb
        self.x, self.y = x, y
        self.local, self.first, self.recv, self.second = local, first, recv, second
        self.me = lax.axis_index("dp")
        self.g, self.r = self.me // self.q, lax.rem(self.me, self.q)
        self.sent = []

    def go(self, src, slot, send, target):
        copy = remote(src, self.y.at[slot], send, self.recv.at[slot], "dp", target)
        copy.start()
        self.sent.append(copy)

    def arrived(self, slot):
        remote(
            self.y.at[slot], self.y.at[slot], self.first.at[0], self.recv.at[slot], "dp", self.me
        ).wait_recv()

    def start(self):
        nb, q, me, g, r = self.nb, self.q, self.me, self.g, self.r
        for j in range(1, nb):
            other = lax.rem(g + j, nb)
            self.go(self.x.at[other], me, self.first.at[j], other * q + r)
        for p in range(1, q):
            self.go(self.x.at[g], me, self.second.at[p], g * q + lax.rem(r + p, q))
        self.own = pltpu.make_async_copy(self.x.at[g], self.y.at[me], self.local.at[0])
        self.own.start()

    def forward(self):
        nb, q, g, r = self.nb, self.q, self.g, self.r
        for j in range(1, nb):
            slot = lax.rem(g + nb - j, nb) * q + r
            self.arrived(slot)
            for p in range(1, q):
                self.go(
                    self.y.at[slot], slot, self.second.at[j * q + p], g * q + lax.rem(r + p, q)
                )

    def finish(self):
        nb, q, r = self.nb, self.q, self.r
        self.own.wait()
        for p in range(1, q):
            for j in range(nb):
                self.arrived(j * q + lax.rem(r + p, q))
        for copy in self.sent:
            copy.wait_send()

    @staticmethod
    def scratch(n, nb):
        return [
            pltpu.SemaphoreType.DMA((1,)),
            pltpu.SemaphoreType.DMA((nb,)),
            pltpu.SemaphoreType.DMA((n,)),
            pltpu.SemaphoreType.DMA((n,)),
        ]


class Exchange:
    def __init__(self, n, nb, to_rows, x, y, local, send, recv):
        q = n // nb
        me = lax.axis_index("dp")
        self.nb, self.x, self.y = nb, x, y
        self.local, self.send, self.recv, self.me = local, send, recv, me
        owner = lax.rem(me, q) * nb
        first = me // nb
        if to_rows:
            self.targets = [owner + k for k in range(nb)]
            self.slot = me // q
            self.sources = [k * q + first for k in range(nb)]
        else:
            self.targets = [k * q + first for k in range(nb)]
            self.slot = lax.rem(me, nb)
            self.sources = [owner + k for k in range(nb)]

    def copy(self, k):
        return remote(
            self.x.at[k],
            self.y.at[self.slot],
            self.send.at[k],
            self.recv.at[self.slot],
            "dp",
            self.targets[k],
        )

    def mine(self, k):
        return pltpu.make_async_copy(self.x.at[k], self.y.at[self.slot], self.local.at[0])

    def start(self):
        for k in range(self.nb):

            @pl.when(self.targets[k] != self.me)
            def _():
                self.copy(k).start()

            @pl.when(self.targets[k] == self.me)
            def _():
                self.mine(k).start()

    def finish(self):
        for k in range(self.nb):

            @pl.when(self.sources[k] != self.me)
            def _():
                remote(
                    self.y.at[k], self.y.at[k], self.send.at[k], self.recv.at[k], "dp", self.me
                ).wait_recv()

            @pl.when(self.targets[k] != self.me)
            def _():
                self.copy(k).wait_send()

            @pl.when(self.targets[k] == self.me)
            def _():
                self.mine(k).wait()

    @staticmethod
    def scratch(nb):
        return [
            pltpu.SemaphoreType.DMA((1,)),
            pltpu.SemaphoreType.DMA((nb,)),
            pltpu.SemaphoreType.DMA((nb,)),
        ]


class Share:
    def __init__(self, axis, size, x, y, local, send, recv):
        self.axis, self.size, self.x, self.y = axis, size, x, y
        self.local, self.send, self.recv = local, send, recv
        self.me = lax.axis_index(axis)

    def copy(self, j):
        return remote(
            self.x,
            self.y.at[self.me],
            self.send.at[j],
            self.recv.at[self.me],
            self.axis,
            lax.rem(self.me + j, self.size),
        )

    def start(self):
        for j in range(1, self.size):
            self.copy(j).start()
        self.own = pltpu.make_async_copy(self.x, self.y.at[self.me], self.local.at[0])
        self.own.start()

    def finish(self):
        self.own.wait()
        for j in range(1, self.size):
            slot = lax.rem(self.me + j, self.size)
            remote(
                self.y.at[slot], self.y.at[slot], self.send.at[j], self.recv.at[slot], self.axis, slot
            ).wait_recv()
        for j in range(1, self.size):
            self.copy(j).wait_send()

    @staticmethod
    def scratch(size):
        return [
            pltpu.SemaphoreType.DMA((1,)),
            pltpu.SemaphoreType.DMA((size,)),
            pltpu.SemaphoreType.DMA((size,)),
        ]


def bases_kernel(n, nb, left, right, master, left_out, right_out, master_out, *sems):
    enter([("dp", n)])
    one = Gather(n, nb, right, right_out, *sems[0:4])
    two = Gather(n, nb, left, left_out, *sems[4:8])
    three = Exchange(n, nb, False, master, master_out, *sems[8:11])
    one.start()
    two.start()
    three.start()
    one.forward()
    two.forward()
    one.finish()
    two.finish()
    three.finish()


def gather_kernel(n, nb, x, y, *sems):
    enter([("dp", n)])
    one = Gather(n, nb, x, y, *sems)
    one.start()
    one.forward()
    one.finish()


def scatter_kernel(n, nb, x, y, *sems):
    enter([("dp", n)])
    one = Exchange(n, nb, True, x, y, *sems)
    one.start()
    one.finish()


def scatter_sum_kernel(n, m, nb, x, part, y, parts, *sems):
    enter([("dp", n), ("mp", m)])
    two = Share("mp", m, part, parts, *sems[3:6])
    two.start()
    one = Exchange(n, nb, True, x, y, *sems[0:3])
    one.start()
    two.finish()
    one.finish()


def group_kernel(n, nb, x, part, y, parts, *sems):
    enter([("dp", n)])
    q = n // nb
    me = lax.axis_index("dp")
    g, r = me // q, lax.rem(me, q)
    local, send, recv = sems[0:3]
    copies = []
    for p in range(1, q):
        copy = remote(
            x, y.at[r], send.at[p], recv.at[r], "dp", g * q + lax.rem(r + p, q)
        )
        copy.start()
        copies.append(copy)
    two = Share("dp", n, part, parts, *sems[3:6])
    two.start()
    own = pltpu.make_async_copy(x, y.at[r], local.at[0])
    own.start()
    own.wait()
    for p in range(1, q):
        slot = lax.rem(r + p, q)
        remote(y.at[slot], y.at[slot], send.at[p], recv.at[slot], "dp", me).wait_recv()
    two.finish()
    for copy in copies:
        copy.wait_send()


def call(kernel, shapes, scratch, collective_id, *args):
    moved = sum(s.size * s.dtype.itemsize for s in shapes)
    return pl.pallas_call(
        kernel,
        out_shape=shapes,
        in_specs=[VMEM] * len(args),
        out_specs=[VMEM] * len(shapes),
        scratch_shapes=scratch,
        compiler_params=pltpu.CompilerParams(
            collective_id=collective_id, has_side_effects=True, vmem_limit_bytes=32 * 1024 * 1024
        ),
        cost_estimate=pl.CostEstimate(flops=0, bytes_accessed=16 * moved, transcendentals=0),
    )(*args)


def per_device_general(n, m, grad_parts, master, first_moment, second_moment, left_basis, right_basis):
    bf16, f32 = jnp.bfloat16, jnp.float32
    nb, rb, cols = master.shape
    blk = rb * n
    q = n // nb
    hb = blk // q
    r = lax.rem(lax.axis_index("dp"), q)
    pieces = jax.ShapeDtypeStruct((nb, rb, cols), bf16)
    block = jax.ShapeDtypeStruct((n, rb, cols), bf16)
    low_sum = lax.psum_scatter(
        grad_parts.reshape(nb * blk, cols), "dp", scatter_dimension=0, tiled=True
    )
    left, right, master_low = call(
        functools.partial(bases_kernel, n, nb),
        [block, block, pieces],
        Gather.scratch(n, nb) * 2 + Exchange.scratch(nb),
        0,
        left_basis,
        right_basis,
        master.astype(bf16),
    )
    left, right = left.reshape(blk, cols), right.reshape(blk, cols)
    left_cols = lax.dynamic_slice_in_dim(left, r * hb, hb, axis=1)
    left_rows = lax.dynamic_slice_in_dim(left, r * hb, hb, axis=0)
    gradient = low_sum.astype(f32)
    part = jnp.full((8, 128), jnp.sum(gradient * gradient), f32)
    grad_block, parts = call(
        functools.partial(group_kernel, n, nb),
        [
            jax.ShapeDtypeStruct((q, hb, cols), bf16),
            jax.ShapeDtypeStruct((n, 8, 128), f32),
        ],
        Share.scratch(q) + Share.scratch(n),
        1,
        low_sum,
        part,
    )
    part = jnp.sum(parts, axis=0)
    turned = jnp.dot(
        grad_block.reshape(blk, cols), right, preferred_element_type=f32
    ).astype(bf16)
    rotated_rows = lax.dot_general(
        left_cols, turned, (((0,), (0,)), ((), ())), preferred_element_type=f32
    ).astype(bf16)
    rotated, parts = call(
        functools.partial(scatter_sum_kernel, n, m, nb),
        [pieces, jax.ShapeDtypeStruct((m, 8, 128), f32)],
        Exchange.scratch(nb) + Share.scratch(m),
        2,
        rotated_rows.reshape(nb, rb, cols),
        part,
    )
    squares_sum = jnp.sum(parts[:, 0, 0])
    clip_scale = jnp.minimum(1.0, 2.0 * D / jnp.sqrt(squares_sum + norm_epsilon))
    clipped = clip_scale * rotated.astype(f32)
    new_first = beta_one * first_moment + (1.0 - beta_one) * clipped
    new_second = beta_two * second_moment + (1.0 - beta_two) * clipped * clipped
    bias_one = 1.0 - beta_one**STEP
    bias_two = 1.0 - beta_two**STEP
    direction = (new_first / bias_one / (jnp.sqrt(new_second / bias_two) + epsilon)).astype(bf16)
    (direction_block,) = call(
        functools.partial(gather_kernel, n, nb), [block], Gather.scratch(n, nb), 3, direction
    )
    back = lax.dot_general(
        direction_block.reshape(blk, cols),
        right,
        (((1,), (1,)), ((), ())),
        preferred_element_type=f32,
    ).astype(bf16)
    update = jnp.dot(left_rows, back, preferred_element_type=f32)
    keep = 1.0 - learning_rate * decay_rate
    weight_rows = (
        master_low.reshape(hb, cols).astype(f32) * keep - learning_rate * update
    ).astype(bf16)
    weights = lax.all_gather(weight_rows, "dp", axis=0, tiled=True).reshape(nb, blk, cols)
    (update_rows,) = call(
        functools.partial(scatter_kernel, n, nb),
        [pieces],
        Exchange.scratch(nb),
        4,
        update.astype(bf16).reshape(nb, rb, cols),
    )
    new_master = master * keep - learning_rate * update_rows.astype(f32)
    return (weights, new_master, new_first, new_second)


SEMAPHORES = (
    ("local", 5),
    ("grad", 4),
    ("pair_s", 4),
    ("pair_r", 4),
    ("right_s", 8),
    ("right_r", 8),
    ("left_s", 8),
    ("left_r", 8),
    ("one_s", 8),
    ("one_r", 8),
    ("two_s", 4),
    ("two_r", 4),
    ("turned_s", 4),
    ("turned_r", 4),
    ("rot_s", 4),
    ("rot_r", 4),
    ("dir_s", 4),
    ("dir_r", 4),
    ("back_s", 4),
    ("back_r", 4),
    ("low_s", 4),
    ("low_r", 4),
    ("out_s", 12),
    ("pass_s", 16),
    ("out_r", 32),
    ("norm_s", 8),
    ("norm_r", 8),
    ("mesh_s", 8),
    ("mesh_r", 8),
)


def step_kernel(
    n,
    m,
    grad,
    master,
    first,
    second,
    left_in,
    right_in,
    weights,
    new_master,
    new_first,
    new_second,
    acc,
    pair_recv,
    left,
    right,
    left_t,
    hop_one,
    hop_two,
    turned,
    rot_send,
    rot_recv,
    dir_send,
    dir_recv,
    back,
    low_send,
    low_recv,
    squares,
    part,
    parts_dp,
    total,
    parts_mp,
    *sem_refs,
):
    sem = {name: ref for (name, _), ref in zip(SEMAPHORES, sem_refs)}
    f32, bf16 = jnp.float32, jnp.bfloat16
    nb, rb, cols = master.shape
    half = nb * rb
    wide = cols // 2
    me = lax.axis_index("dp")
    c, k = me // 2, lax.rem(me, 2)
    cy, cx = c // 2, lax.rem(c, 2)
    xn, yn = 2 * cy + (1 - cx), 2 * (1 - cy) + cx
    one, two = (1 - k) * xn + k * yn, k * xn + (1 - k) * yn
    partner = me + 1 - 2 * k
    swapped = (0, 2, 1, 3)
    keep = 1.0 - learning_rate * decay_rate

    def chip(i):
        return c + (1 - i // 2) * (one - c) + (1 - i % 2) * (two - c)

    def device(i):
        return 2 * chip(i) + k

    def rows(s):
        return pl.ds(pl.multiple_of(s * rb, rb), rb)

    def send(src, dst, send_sem, recv_sem, target):
        remote(src, dst, send_sem, recv_sem, "dp", target).start()

    def received(ref, recv_sem):
        remote(ref, ref, recv_sem, recv_sem, "dp", me).wait_recv()

    def sent(ref, send_sem):
        remote(ref, ref, send_sem, send_sem, "dp", me).wait_send()

    def strips(body, step=32):
        @pl.loop(0, rb // step)
        def _(t):
            body(lambda base: pl.ds(pl.multiple_of(base + t * step, step), step))

    enter([("dp", n), ("mp", m)])

    bases = ((right_in, right, "right", 0), (left_in, left, "left", 1))
    locals_in = []

    def fetch(src, dst, local_sem):
        copy = pltpu.make_async_copy(src, dst, local_sem)
        copy.start()
        locals_in.append(copy)

    for x_in, x, name, _ in bases:
        for i in range(3):
            send(
                x_in.at[chip(i)],
                x.at[rows(me)],
                sem[name + "_s"].at[i],
                sem[name + "_r"].at[me],
                device(i),
            )
    for i in range(nb):
        b = chip(i)
        send(
            grad.at[b, pl.ds((1 - k) * half, half)],
            pair_recv.at[i],
            sem["pair_s"].at[i],
            sem["pair_r"].at[i],
            partner,
        )
        fetch(grad.at[b, pl.ds(k * half, half)], acc.at[i], sem["grad"].at[i])
    for x_in, x, name, slot in bases:
        send(x_in.at[c], x.at[rows(me)], sem[name + "_s"].at[3], sem[name + "_r"].at[me], partner)
        fetch(x_in.at[c], x.at[rows(me)], sem["local"].at[slot])
    fetch(master, new_master, sem["local"].at[2])
    fetch(first, new_first, sem["local"].at[3])
    fetch(second, new_second, sem["local"].at[4])

    for i in range(nb):
        j = swapped[i]
        locals_in[i].wait()
        received(pair_recv.at[j], sem["pair_r"].at[j])

        @pl.loop(0, nb)
        def _(q):
            def add(at):
                r = at(q * rb)
                acc[i, r] = (acc[i, r].astype(f32) + pair_recv[j, r].astype(f32)).astype(bf16)

            strips(add)
            if i < 2:
                send(
                    acc.at[i, rows(q)],
                    hop_one.at[i, rows(q)],
                    sem["one_s"].at[i * nb + q],
                    sem["one_r"].at[i * nb + q],
                    2 * one + k,
                )

    locals_in[6].wait()

    @pl.loop(0, nb)
    def _(b):
        def narrow(at):
            low_send[b, at(0)] = new_master[b, at(0)].astype(bf16)

        strips(narrow)

    def own_low(at):
        low_recv[c, at(0)] = new_master[c, at(0)].astype(bf16)

    strips(own_low)

    def send_low(i):
        send(
            low_send.at[chip(i)], low_recv.at[c], sem["low_s"].at[i], sem["low_r"].at[c], device(i)
        )

    for _, x, name, slot in bases:
        for i in range(3):
            s = device(i)
            received(x.at[rows(s)], sem[name + "_r"].at[s])
            send(
                x.at[rows(s)],
                x.at[rows(s)],
                sem[name + "_s"].at[4 + i],
                sem[name + "_r"].at[s],
                partner,
            )

    @pl.loop(0, nb)
    def _(q):
        received(hop_one.at[0, rows(q)], sem["one_r"].at[q])

        def add(at):
            r = at(q * rb)
            acc[2, r] = (acc[2, r].astype(f32) + hop_one[0, r].astype(f32)).astype(bf16)

        strips(add)
        send(
            acc.at[2, rows(q)],
            hop_two.at[rows(q)],
            sem["two_s"].at[q],
            sem["two_r"].at[q],
            2 * two + k,
        )

    send_low(0)
    for _, x, name, slot in bases:
        locals_in[4 + slot].wait()
        for i in range(4):
            s = 2 * chip(i) + 1 - k
            received(x.at[rows(s)], sem[name + "_r"].at[s])

    @pl.loop(0, nb)
    def _(i):
        left_t[i] = left[:, rows(device(i))].T

    squares[...] = jnp.zeros_like(squares)

    @pl.loop(0, nb)
    def _(q):
        received(hop_two.at[rows(q)], sem["two_r"].at[q])
        received(hop_one.at[1, rows(q)], sem["one_r"].at[nb + q])

        def add(at):
            r = at(q * rb)
            g = acc[3, r].astype(f32) + hop_one[1, r].astype(f32) + hop_two[r].astype(f32)
            acc[3, r] = g.astype(bf16)
            squares[...] += jnp.sum((g * g).reshape(-1, 8, cols), axis=0)

        strips(add)

        @pl.when(q == nb - 1)
        def _():
            folded = squares[:, 0:128]
            for t in range(1, cols // 128):
                folded = folded + squares[:, t * 128 : (t + 1) * 128]
            part[...] = folded
            for j in range(1, n):
                send(
                    part,
                    parts_dp.at[me],
                    sem["norm_s"].at[j],
                    sem["norm_r"].at[me],
                    lax.rem(me + j, n),
                )

        s = k * nb + q
        for t in range(2):
            at = pl.ds(t * wide, wide)
            turned[rows(s), at] = jnp.dot(
                acc[3, rows(q)], right[:, at], preferred_element_type=f32
            ).astype(bf16)
        send(
            turned.at[rows(s)],
            turned.at[rows(s)],
            sem["turned_s"].at[q],
            sem["turned_r"].at[q],
            partner,
        )

    for q in range(nb):
        received(turned.at[rows((1 - k) * nb + q)], sem["turned_r"].at[q])

    @pl.loop(0, nb)
    def _(i):
        for t in range(2):
            at = pl.ds(t * wide, wide)
            rot_send[i, :, at] = jnp.dot(
                left_t[i], turned[:, at], preferred_element_type=f32
            ).astype(bf16)

        @pl.when(i < 3)
        def _():
            send(
                rot_send.at[i], rot_recv.at[i], sem["rot_s"].at[i], sem["rot_r"].at[i], device(i)
            )

    send_low(1)

    folded = part[...]
    for j in range(1, n):
        s = lax.rem(me + j, n)
        received(parts_dp.at[s], sem["norm_r"].at[s])
        folded = folded + parts_dp[s]
    total[...] = folded
    z = lax.axis_index("mp")
    for j in range(1, m):
        remote(
            total,
            parts_mp.at[z],
            sem["mesh_s"].at[j],
            sem["mesh_r"].at[z],
            "mp",
            lax.rem(z + j, m),
        ).start()
    for j in range(1, m):
        s = lax.rem(z + j, m)
        remote(
            parts_mp.at[s], parts_mp.at[s], sem["mesh_s"].at[j], sem["mesh_r"].at[s], "mp", z
        ).wait_recv()
        folded = folded + parts_mp[s]
    squares_sum = jnp.sum(folded)
    clip_scale = jnp.minimum(
        1.0, 2.0 * D / jnp.sqrt(jnp.full((8, 128), squares_sum + norm_epsilon, f32))
    )
    total_scale = clip_scale[0:1, 0:1]

    locals_in[7].wait()
    locals_in[8].wait()
    bias_one = 1.0 - beta_one**STEP
    bias_two = 1.0 - beta_two**STEP

    def moments(i, src):
        b = chip(i)

        def strip(at):
            r = at(0)
            clipped = total_scale * src[i, r].astype(f32)
            mean = beta_one * new_first[b, r] + (1.0 - beta_one) * clipped
            var = beta_two * new_second[b, r] + (1.0 - beta_two) * clipped * clipped
            new_first[b, r] = mean
            new_second[b, r] = var
            dir_send[i, r] = (
                mean / bias_one / (jnp.sqrt(var / bias_two) + epsilon)
            ).astype(bf16)

        strips(strip, 16)

    moments(3, rot_send)

    @pl.loop(0, 3)
    def _(i):
        received(rot_recv.at[i], sem["rot_r"].at[i])
        moments(i, rot_recv)
        send(dir_send.at[i], dir_recv.at[i], sem["dir_s"].at[i], sem["dir_r"].at[i], device(i))

    send_low(2)

    def back_slab(i, src):
        s = device(i)
        for t in range(2):
            at = pl.ds(t * wide, wide)
            back[rows(s), at] = lax.dot_general(
                src[i], right[at, :], (((1,), (1,)), ((), ())), preferred_element_type=f32
            ).astype(bf16)
        send(back.at[rows(s)], back.at[rows(s)], sem["back_s"].at[i], sem["back_r"].at[i], partner)

    back_slab(3, dir_send)

    @pl.loop(0, 3)
    def _(i):
        received(dir_recv.at[i], sem["dir_r"].at[i])
        back_slab(i, dir_recv)

    for i in range(3):
        received(low_recv.at[chip(i)], sem["low_r"].at[chip(i)])
    for i in range(4):
        received(back.at[rows(2 * chip(swapped[i]) + 1 - k)], sem["back_r"].at[i])

    def hand_on(b, s, send_sem, target):
        send(
            weights.at[b, rows(s)], weights.at[b, rows(s)], send_sem, sem["out_r"].at[b * n + s], target
        )

    def arrived(b, s):
        received(weights.at[b, rows(s)], sem["out_r"].at[b * n + s])

    @pl.loop(0, nb)
    def _(q):
        s = 2 * q + k
        for t in range(2):
            at = pl.ds(t * wide, wide)
            update = jnp.dot(left[rows(s)], back[:, at], preferred_element_type=f32)
            weights[c, rows(s), at] = (
                low_recv[q, :, at].astype(f32) * keep - learning_rate * update
            ).astype(bf16)
        hand_on(c, s, sem["out_s"].at[q], 2 * one + k)
        hand_on(c, s, sem["out_s"].at[nb + q], 2 * two + k)
        hand_on(c, s, sem["out_s"].at[2 * nb + q], partner)

    def finish(i):
        b = chip(i)

        def strip(at):
            r = at(0)
            low = low_send[b, r].astype(f32)
            new_master[b, r] = weights[b, at(me * rb)].astype(f32) + keep * (new_master[b, r] - low)

        strips(strip)

    finish(3)

    @pl.loop(0, nb)
    def _(q):
        s = 2 * q + k
        arrived(one, s)
        hand_on(one, s, sem["pass_s"].at[q], 2 * two + k)
        hand_on(one, s, sem["pass_s"].at[nb + q], partner)
        arrived(two, s)
        hand_on(two, s, sem["pass_s"].at[2 * nb + q], partner)

    finish(1)
    finish(2)

    @pl.loop(0, nb)
    def _(q):
        s = 2 * q + k
        arrived(chip(0), s)
        hand_on(chip(0), s, sem["pass_s"].at[3 * nb + q], partner)

    finish(0)

    for i in range(4):
        sent(pair_recv.at[i], sem["pair_s"].at[i])
        sent(turned.at[rows(i)], sem["turned_s"].at[i])
        sent(back.at[rows(i)], sem["back_s"].at[i])
        sent(hop_two.at[rows(i)], sem["two_s"].at[i])
    for i in range(3):
        sent(rot_send.at[i], sem["rot_s"].at[i])
        sent(dir_send.at[i], sem["dir_s"].at[i])
        sent(low_send.at[i], sem["low_s"].at[i])
    for i in range(7):
        sent(right.at[rows(i)], sem["right_s"].at[i])
        sent(left.at[rows(i)], sem["left_s"].at[i])
    for i in range(8):
        sent(hop_two.at[rows(0)], sem["one_s"].at[i])
    for j in range(1, n):
        sent(part, sem["norm_s"].at[j])
    for j in range(1, m):
        remote(
            total, total, sem["mesh_s"].at[j], sem["mesh_r"].at[j], "mp", z
        ).wait_send()
    for i in range(12):
        sent(weights.at[0, rows(0)], sem["out_s"].at[i])
    for i in range(16):
        sent(weights.at[0, rows(0)], sem["pass_s"].at[i])

    @pl.loop(0, nb)
    def _(b):
        for q in range(nb):
            arrived(b, 2 * q + 1 - k)


def per_device(n, m, grad_parts, master, first_moment, second_moment, left_basis, right_basis):
    nb, rb, cols = master.shape
    blk = rb * n
    args = (grad_parts, master, first_moment, second_moment, left_basis, right_basis)
    if n != 2 * nb or nb != 4 or m > 8:
        return per_device_general(n, m, *args)
    bf16, f32 = jnp.bfloat16, jnp.float32
    half = blk // 2
    scratch = [
        pltpu.VMEM((nb, half, cols), bf16),
        pltpu.VMEM((nb, half, cols), bf16),
        pltpu.VMEM((blk, cols), bf16),
        pltpu.VMEM((blk, cols), bf16),
        pltpu.VMEM((nb, rb, blk), bf16),
        pltpu.VMEM((2, half, cols), bf16),
        pltpu.VMEM((half, cols), bf16),
        pltpu.VMEM((blk, cols), bf16),
        pltpu.VMEM((nb, rb, cols), bf16),
        pltpu.VMEM((nb, rb, cols), bf16),
        pltpu.VMEM((nb, rb, cols), bf16),
        pltpu.VMEM((nb, rb, cols), bf16),
        pltpu.VMEM((blk, cols), bf16),
        pltpu.VMEM((nb, rb, cols), bf16),
        pltpu.VMEM((nb, rb, cols), bf16),
        pltpu.VMEM((8, cols), f32),
        pltpu.VMEM((8, 128), f32),
        pltpu.VMEM((n, 8, 128), f32),
        pltpu.VMEM((8, 128), f32),
        pltpu.VMEM((m, 8, 128), f32),
    ] + [pltpu.SemaphoreType.DMA((size,)) for _, size in SEMAPHORES]
    shapes = [
        jax.ShapeDtypeStruct((nb, blk, cols), bf16),
        jax.ShapeDtypeStruct(master.shape, f32),
        jax.ShapeDtypeStruct(master.shape, f32),
        jax.ShapeDtypeStruct(master.shape, f32),
    ]
    hbm = pl.BlockSpec(memory_space=pl.ANY)
    return pl.pallas_call(
        functools.partial(step_kernel, n, m),
        out_shape=shapes,
        in_specs=[hbm] * 6,
        out_specs=[VMEM] * 4,
        scratch_shapes=scratch,
        compiler_params=pltpu.CompilerParams(
            collective_id=0, has_side_effects=True, vmem_limit_bytes=44 * 1024 * 1024
        ),
    )(grad_parts.reshape(nb, blk, cols), *args[1:])


def solution(mesh):
    n, m = mesh.shape["dp"], mesh.shape["mp"]
    return jax.shard_map(
        functools.partial(per_device, n, m),
        mesh=mesh,
        in_specs=(
            P("dp", None, None, "mp"),
            P(None, "dp", "mp"),
            P(None, "dp", "mp"),
            P(None, "dp", "mp"),
            P(None, "dp", "mp"),
            P(None, "dp", "mp"),
        ),
        out_specs=(
            P(None, None, "mp"),
            P(None, "dp", "mp"),
            P(None, "dp", "mp"),
            P(None, "dp", "mp"),
        ),
        check_vma=False,
    )
```

```python
import functools

import jax
import jax.numpy as jnp
from jax import lax
from jax.experimental import pallas as pl
from jax.experimental.pallas import tpu as pltpu
from jax.sharding import PartitionSpec as P

D = 4096
STEP = 10


beta_one = 0.95
beta_two = 0.95
epsilon = 1e-08
norm_epsilon = 1e-06
learning_rate = 0.3
decay_rate = 0.1

VMEM = pl.BlockSpec(memory_space=pltpu.VMEM)
MESH = pl.DeviceIdType.MESH


def remote(src, dst, send, recv, axis, index):
    return pltpu.make_async_remote_copy(
        src_ref=src,
        dst_ref=dst,
        send_sem=send,
        recv_sem=recv,
        device_id={axis: index},
        device_id_type=MESH,
    )


def enter(axes):
    barrier = pltpu.get_barrier_semaphore()
    total = 0
    for axis, size in axes:
        me = lax.axis_index(axis)
        for step in range(1, size):
            pl.semaphore_signal(
                barrier,
                inc=1,
                device_id={axis: lax.rem(me + step, size)},
                device_id_type=MESH,
            )
        total += size - 1
    pl.semaphore_wait(barrier, total)


class Gather:
    def __init__(self, n, nb, x, y, local, first, recv, second):
        self.n, self.nb, self.q = n, nb, n // nb
        self.x, self.y = x, y
        self.local, self.first, self.recv, self.second = local, first, recv, second
        self.me = lax.axis_index("dp")
        self.g, self.r = self.me // self.q, lax.rem(self.me, self.q)
        self.sent = []

    def go(self, src, slot, send, target):
        copy = remote(src, self.y.at[slot], send, self.recv.at[slot], "dp", target)
        copy.start()
        self.sent.append(copy)

    def arrived(self, slot):
        remote(
            self.y.at[slot], self.y.at[slot], self.first.at[0], self.recv.at[slot], "dp", self.me
        ).wait_recv()

    def start(self):
        nb, q, me, g, r = self.nb, self.q, self.me, self.g, self.r
        for j in range(1, nb):
            other = lax.rem(g + j, nb)
            self.go(self.x.at[other], me, self.first.at[j], other * q + r)
        for p in range(1, q):
            self.go(self.x.at[g], me, self.second.at[p], g * q + lax.rem(r + p, q))
        self.own = pltpu.make_async_copy(self.x.at[g], self.y.at[me], self.local.at[0])
        self.own.start()

    def forward(self):
        nb, q, g, r = self.nb, self.q, self.g, self.r
        for j in range(1, nb):
            slot = lax.rem(g + nb - j, nb) * q + r
            self.arrived(slot)
            for p in range(1, q):
                self.go(
                    self.y.at[slot], slot, self.second.at[j * q + p], g * q + lax.rem(r + p, q)
                )

    def finish(self):
        nb, q, r = self.nb, self.q, self.r
        self.own.wait()
        for p in range(1, q):
            for j in range(nb):
                self.arrived(j * q + lax.rem(r + p, q))
        for copy in self.sent:
            copy.wait_send()

    @staticmethod
    def scratch(n, nb):
        return [
            pltpu.SemaphoreType.DMA((1,)),
            pltpu.SemaphoreType.DMA((nb,)),
            pltpu.SemaphoreType.DMA((n,)),
            pltpu.SemaphoreType.DMA((n,)),
        ]


class Exchange:
    def __init__(self, n, nb, to_rows, x, y, local, send, recv):
        q = n // nb
        me = lax.axis_index("dp")
        self.nb, self.x, self.y = nb, x, y
        self.local, self.send, self.recv, self.me = local, send, recv, me
        owner = lax.rem(me, q) * nb
        first = me // nb
        if to_rows:
            self.targets = [owner + k for k in range(nb)]
            self.slot = me // q
            self.sources = [k * q + first for k in range(nb)]
        else:
            self.targets = [k * q + first for k in range(nb)]
            self.slot = lax.rem(me, nb)
            self.sources = [owner + k for k in range(nb)]

    def copy(self, k):
        return remote(
            self.x.at[k],
            self.y.at[self.slot],
            self.send.at[k],
            self.recv.at[self.slot],
            "dp",
            self.targets[k],
        )

    def mine(self, k):
        return pltpu.make_async_copy(self.x.at[k], self.y.at[self.slot], self.local.at[0])

    def start(self):
        for k in range(self.nb):

            @pl.when(self.targets[k] != self.me)
            def _():
                self.copy(k).start()

            @pl.when(self.targets[k] == self.me)
            def _():
                self.mine(k).start()

    def finish(self):
        for k in range(self.nb):

            @pl.when(self.sources[k] != self.me)
            def _():
                remote(
                    self.y.at[k], self.y.at[k], self.send.at[k], self.recv.at[k], "dp", self.me
                ).wait_recv()

            @pl.when(self.targets[k] != self.me)
            def _():
                self.copy(k).wait_send()

            @pl.when(self.targets[k] == self.me)
            def _():
                self.mine(k).wait()

    @staticmethod
    def scratch(nb):
        return [
            pltpu.SemaphoreType.DMA((1,)),
            pltpu.SemaphoreType.DMA((nb,)),
            pltpu.SemaphoreType.DMA((nb,)),
        ]


class Share:
    def __init__(self, axis, size, x, y, local, send, recv):
        self.axis, self.size, self.x, self.y = axis, size, x, y
        self.local, self.send, self.recv = local, send, recv
        self.me = lax.axis_index(axis)

    def copy(self, j):
        return remote(
            self.x,
            self.y.at[self.me],
            self.send.at[j],
            self.recv.at[self.me],
            self.axis,
            lax.rem(self.me + j, self.size),
        )

    def start(self):
        for j in range(1, self.size):
            self.copy(j).start()
        self.own = pltpu.make_async_copy(self.x, self.y.at[self.me], self.local.at[0])
        self.own.start()

    def finish(self):
        self.own.wait()
        for j in range(1, self.size):
            slot = lax.rem(self.me + j, self.size)
            remote(
                self.y.at[slot], self.y.at[slot], self.send.at[j], self.recv.at[slot], self.axis, slot
            ).wait_recv()
        for j in range(1, self.size):
            self.copy(j).wait_send()

    @staticmethod
    def scratch(size):
        return [
            pltpu.SemaphoreType.DMA((1,)),
            pltpu.SemaphoreType.DMA((size,)),
            pltpu.SemaphoreType.DMA((size,)),
        ]


def bases_kernel(n, nb, left, right, master, left_out, right_out, master_out, *sems):
    enter([("dp", n)])
    one = Gather(n, nb, right, right_out, *sems[0:4])
    two = Gather(n, nb, left, left_out, *sems[4:8])
    three = Exchange(n, nb, False, master, master_out, *sems[8:11])
    one.start()
    two.start()
    three.start()
    one.forward()
    two.forward()
    one.finish()
    two.finish()
    three.finish()


def gather_kernel(n, nb, x, y, *sems):
    enter([("dp", n)])
    one = Gather(n, nb, x, y, *sems)
    one.start()
    one.forward()
    one.finish()


def scatter_kernel(n, nb, x, y, *sems):
    enter([("dp", n)])
    one = Exchange(n, nb, True, x, y, *sems)
    one.start()
    one.finish()


def scatter_sum_kernel(n, m, nb, x, part, y, parts, *sems):
    enter([("dp", n), ("mp", m)])
    two = Share("mp", m, part, parts, *sems[3:6])
    two.start()
    one = Exchange(n, nb, True, x, y, *sems[0:3])
    one.start()
    two.finish()
    one.finish()


def group_kernel(n, nb, x, part, y, parts, *sems):
    enter([("dp", n)])
    q = n // nb
    me = lax.axis_index("dp")
    g, r = me // q, lax.rem(me, q)
    local, send, recv = sems[0:3]
    copies = []
    for p in range(1, q):
        copy = remote(
            x, y.at[r], send.at[p], recv.at[r], "dp", g * q + lax.rem(r + p, q)
        )
        copy.start()
        copies.append(copy)
    two = Share("dp", n, part, parts, *sems[3:6])
    two.start()
    own = pltpu.make_async_copy(x, y.at[r], local.at[0])
    own.start()
    own.wait()
    for p in range(1, q):
        slot = lax.rem(r + p, q)
        remote(y.at[slot], y.at[slot], send.at[p], recv.at[slot], "dp", me).wait_recv()
    two.finish()
    for copy in copies:
        copy.wait_send()


def call(kernel, shapes, scratch, collective_id, *args):
    moved = sum(s.size * s.dtype.itemsize for s in shapes)
    return pl.pallas_call(
        kernel,
        out_shape=shapes,
        in_specs=[VMEM] * len(args),
        out_specs=[VMEM] * len(shapes),
        scratch_shapes=scratch,
        compiler_params=pltpu.CompilerParams(
            collective_id=collective_id, has_side_effects=True, vmem_limit_bytes=32 * 1024 * 1024
        ),
        cost_estimate=pl.CostEstimate(flops=0, bytes_accessed=16 * moved, transcendentals=0),
    )(*args)


def per_device_general(n, m, grad_parts, master, first_moment, second_moment, left_basis, right_basis):
    bf16, f32 = jnp.bfloat16, jnp.float32
    nb, rb, cols = master.shape
    blk = rb * n
    q = n // nb
    hb = blk // q
    r = lax.rem(lax.axis_index("dp"), q)
    pieces = jax.ShapeDtypeStruct((nb, rb, cols), bf16)
    block = jax.ShapeDtypeStruct((n, rb, cols), bf16)
    low_sum = lax.psum_scatter(
        grad_parts.reshape(nb * blk, cols), "dp", scatter_dimension=0, tiled=True
    )
    left, right, master_low = call(
        functools.partial(bases_kernel, n, nb),
        [block, block, pieces],
        Gather.scratch(n, nb) * 2 + Exchange.scratch(nb),
        0,
        left_basis,
        right_basis,
        master.astype(bf16),
    )
    left, right = left.reshape(blk, cols), right.reshape(blk, cols)
    left_cols = lax.dynamic_slice_in_dim(left, r * hb, hb, axis=1)
    left_rows = lax.dynamic_slice_in_dim(left, r * hb, hb, axis=0)
    gradient = low_sum.astype(f32)
    part = jnp.full((8, 128), jnp.sum(gradient * gradient), f32)
    grad_block, parts = call(
        functools.partial(group_kernel, n, nb),
        [
            jax.ShapeDtypeStruct((q, hb, cols), bf16),
            jax.ShapeDtypeStruct((n, 8, 128), f32),
        ],
        Share.scratch(q) + Share.scratch(n),
        1,
        low_sum,
        part,
    )
    part = jnp.sum(parts, axis=0)
    turned = jnp.dot(
        grad_block.reshape(blk, cols), right, preferred_element_type=f32
    ).astype(bf16)
    rotated_rows = lax.dot_general(
        left_cols, turned, (((0,), (0,)), ((), ())), preferred_element_type=f32
    ).astype(bf16)
    rotated, parts = call(
        functools.partial(scatter_sum_kernel, n, m, nb),
        [pieces, jax.ShapeDtypeStruct((m, 8, 128), f32)],
        Exchange.scratch(nb) + Share.scratch(m),
        2,
        rotated_rows.reshape(nb, rb, cols),
        part,
    )
    squares_sum = jnp.sum(parts[:, 0, 0])
    clip_scale = jnp.minimum(1.0, 2.0 * D / jnp.sqrt(squares_sum + norm_epsilon))
    clipped = clip_scale * rotated.astype(f32)
    new_first = beta_one * first_moment + (1.0 - beta_one) * clipped
    new_second = beta_two * second_moment + (1.0 - beta_two) * clipped * clipped
    bias_one = 1.0 - beta_one**STEP
    bias_two = 1.0 - beta_two**STEP
    direction = (new_first / bias_one / (jnp.sqrt(new_second / bias_two) + epsilon)).astype(bf16)
    (direction_block,) = call(
        functools.partial(gather_kernel, n, nb), [block], Gather.scratch(n, nb), 3, direction
    )
    back = lax.dot_general(
        direction_block.reshape(blk, cols),
        right,
        (((1,), (1,)), ((), ())),
        preferred_element_type=f32,
    ).astype(bf16)
    update = jnp.dot(left_rows, back, preferred_element_type=f32)
    keep = 1.0 - learning_rate * decay_rate
    weight_rows = (
        master_low.reshape(hb, cols).astype(f32) * keep - learning_rate * update
    ).astype(bf16)
    weights = lax.all_gather(weight_rows, "dp", axis=0, tiled=True).reshape(nb, blk, cols)
    (update_rows,) = call(
        functools.partial(scatter_kernel, n, nb),
        [pieces],
        Exchange.scratch(nb),
        4,
        update.astype(bf16).reshape(nb, rb, cols),
    )
    new_master = master * keep - learning_rate * update_rows.astype(f32)
    return (weights, new_master, new_first, new_second)


SEMAPHORES = (
    ("local", 7),
    ("grad", 4),
    ("pair_s", 4),
    ("pair_r", 4),
    ("right_s", 8),
    ("right_r", 8),
    ("left_s", 8),
    ("left_r", 8),
    ("one_s", 8),
    ("one_r", 8),
    ("two_s", 4),
    ("two_r", 4),
    ("turned_s", 4),
    ("turned_r", 4),
    ("rot_s", 4),
    ("rot_r", 4),
    ("dir_s", 4),
    ("dir_r", 4),
    ("back_s", 4),
    ("back_r", 4),
    ("low_s", 4),
    ("low_r", 4),
    ("low_part_r", 2),
    ("out_s", 12),
    ("pass_s", 16),
    ("out_r", 32),
    ("norm_s", 8),
    ("norm_r", 8),
    ("mesh_s", 8),
    ("mesh_r", 8),
)


def step_kernel(
    n,
    m,
    grad,
    master,
    first,
    second,
    left_in,
    right_in,
    weights,
    new_master,
    new_first,
    new_second,
    acc,
    pair_recv,
    left,
    right,
    left_t,
    hop_one,
    hop_two,
    turned,
    rot_send,
    rot_recv,
    dir_send,
    dir_recv,
    back,
    low_send,
    low_recv,
    squares,
    part,
    parts_dp,
    totals,
    parts_mp,
    *sem_refs,
):
    sem = {name: ref for (name, _), ref in zip(SEMAPHORES, sem_refs)}
    f32, bf16 = jnp.float32, jnp.bfloat16
    nb, rb, cols = master.shape
    half = nb * rb
    wide = cols // 2
    me = lax.axis_index("dp")
    c, k = me // 2, lax.rem(me, 2)
    cy, cx = c // 2, lax.rem(c, 2)
    xn, yn = 2 * cy + (1 - cx), 2 * (1 - cy) + cx
    one, two = (1 - k) * xn + k * yn, k * xn + (1 - k) * yn
    partner = me + 1 - 2 * k
    swapped = (0, 2, 1, 3)
    keep = 1.0 - learning_rate * decay_rate

    def chip(i):
        return c + (1 - i // 2) * (one - c) + (1 - i % 2) * (two - c)

    def device(i):
        return 2 * chip(i) + k

    def rows(s):
        return pl.ds(pl.multiple_of(s * rb, rb), rb)

    def send(src, dst, send_sem, recv_sem, target):
        remote(src, dst, send_sem, recv_sem, "dp", target).start()

    def received(ref, recv_sem):
        remote(ref, ref, recv_sem, recv_sem, "dp", me).wait_recv()

    def sent(ref, send_sem):
        remote(ref, ref, send_sem, send_sem, "dp", me).wait_send()

    def strips(body, step=32):
        @pl.loop(0, rb // step)
        def _(t):
            body(lambda base: pl.ds(pl.multiple_of(base + t * step, step), step))

    bases = ((dir_send, right, "right", 4), (rot_send, left, "left", 5))
    locals_in = []

    def fetch(src, dst, local_sem):
        copy = pltpu.make_async_copy(src, dst, local_sem)
        copy.start()
        locals_in.append(copy)

    stages = []
    for t, (src, stage) in enumerate(((right_in, dir_send), (left_in, rot_send))):
        stages.append(pltpu.make_async_copy(src, stage, sem["local"].at[5 + t]))
        stages[t].start()
    for i in range(nb):
        fetch(grad.at[chip(i), pl.ds(k * half, half)], acc.at[i], sem["grad"].at[i])
    fetch(right_in.at[c], right.at[rows(me)], sem["local"].at[0])
    fetch(left_in.at[c], left.at[rows(me)], sem["local"].at[1])
    fetch(master, new_master, sem["local"].at[2])
    fetch(first, new_first, sem["local"].at[3])
    fetch(second, new_second, sem["local"].at[4])

    z = lax.axis_index("mp")
    z_peers = (z + 1 - 2 * lax.rem(z, 2), m - 1 - z)
    barrier = pltpu.get_barrier_semaphore()
    for j in range(1, n):
        pl.semaphore_signal(
            barrier, inc=1, device_id={"dp": lax.rem(me + j, n)}, device_id_type=MESH
        )
    for peer in z_peers:
        pl.semaphore_signal(barrier, inc=1, device_id={"mp": peer}, device_id_type=MESH)
    pl.semaphore_wait(barrier, n - 1 + len(z_peers))

    for t, (stage, x, name, _) in enumerate(bases):
        stages[t].wait()
        for i in range(3):
            send(
                stage.at[chip(i)],
                x.at[rows(me)],
                sem[name + "_s"].at[i],
                sem[name + "_r"].at[me],
                device(i),
            )
    for i in range(nb):
        send(
            grad.at[chip(i), pl.ds((1 - k) * half, half)],
            pair_recv.at[i],
            sem["pair_s"].at[i],
            sem["pair_r"].at[i],
            partner,
        )
    for stage, x, name, _ in bases:
        send(stage.at[c], x.at[rows(me)], sem[name + "_s"].at[3], sem[name + "_r"].at[me], partner)

    for i in range(nb):
        j = swapped[i]
        locals_in[i].wait()
        received(pair_recv.at[j], sem["pair_r"].at[j])

        @pl.loop(0, nb)
        def _(q):
            def add(at):
                r = at(q * rb)
                acc[i, r] = (acc[i, r].astype(f32) + pair_recv[j, r].astype(f32)).astype(bf16)

            strips(add)
            if i < 2:
                send(
                    acc.at[i, rows(q)],
                    hop_one.at[i, rows(q)],
                    sem["one_s"].at[i * nb + q],
                    sem["one_r"].at[i * nb + q],
                    2 * one + k,
                )

    locals_in[6].wait()

    @pl.loop(0, nb)
    def _(b):
        def narrow(at):
            low_send[b, at(0)] = new_master[b, at(0)].astype(bf16)

        strips(narrow)

    def own_low(at):
        low_recv[c, at(0)] = new_master[c, at(0)].astype(bf16)

    strips(own_low)

    def send_low(i):
        send(
            low_send.at[chip(i)], low_recv.at[c], sem["low_s"].at[i], sem["low_r"].at[c], device(i)
        )

    def send_low_part(t):
        part_rows = pl.ds(t * rb // 2, rb // 2)
        send(
            low_send.at[chip(0), part_rows],
            low_recv.at[c, part_rows],
            sem["low_s"].at[3 * t],
            sem["low_part_r"].at[t],
            device(0),
        )

    send_low(1)

    for _, x, name, slot in bases:
        for i in range(3):
            s = device(i)
            received(x.at[rows(s)], sem[name + "_r"].at[s])
            send(
                x.at[rows(s)],
                x.at[rows(s)],
                sem[name + "_s"].at[4 + i],
                sem[name + "_r"].at[s],
                partner,
            )

    @pl.loop(0, nb)
    def _(q):
        received(hop_one.at[0, rows(q)], sem["one_r"].at[q])

        def add(at):
            r = at(q * rb)
            acc[2, r] = (acc[2, r].astype(f32) + hop_one[0, r].astype(f32)).astype(bf16)

        strips(add)
        send(
            acc.at[2, rows(q)],
            hop_two.at[rows(q)],
            sem["two_s"].at[q],
            sem["two_r"].at[q],
            2 * two + k,
        )

    for _, x, name, slot in bases:
        locals_in[slot].wait()
        for i in range(4):
            s = 2 * chip(i) + 1 - k
            received(x.at[rows(s)], sem[name + "_r"].at[s])

    @pl.loop(0, nb)
    def _(i):
        left_t[i] = left[:, rows(device(i))].T

    squares[...] = jnp.zeros_like(squares)

    @pl.loop(0, nb)
    def _(q):
        received(hop_two.at[rows(q)], sem["two_r"].at[q])
        received(hop_one.at[1, rows(q)], sem["one_r"].at[nb + q])

        def add(at):
            r = at(q * rb)
            g = acc[3, r].astype(f32) + hop_one[1, r].astype(f32) + hop_two[r].astype(f32)
            acc[3, r] = g.astype(bf16)
            squares[...] += jnp.sum((g * g).reshape(-1, 8, cols), axis=0)

        strips(add)

        @pl.when(q == nb - 1)
        def _():
            send_low_part(0)
            folded = squares[:, 0:128]
            for t in range(1, cols // 128):
                folded = folded + squares[:, t * 128 : (t + 1) * 128]
            part[...] = folded
            for j in range(1, n):
                send(
                    part,
                    parts_dp.at[me],
                    sem["norm_s"].at[j],
                    sem["norm_r"].at[me],
                    lax.rem(me + j, n),
                )

        s = k * nb + q
        for t in range(2):
            at = pl.ds(t * wide, wide)
            turned[rows(s), at] = jnp.dot(
                acc[3, rows(q)], right[:, at], preferred_element_type=f32
            ).astype(bf16)
        send(
            turned.at[rows(s)],
            turned.at[rows(s)],
            sem["turned_s"].at[q],
            sem["turned_r"].at[q],
            partner,
        )

    for q in range(nb):
        received(turned.at[rows((1 - k) * nb + q)], sem["turned_r"].at[q])

    def mesh_copy(t):
        return remote(
            totals.at[t], parts_mp.at[t], sem["mesh_s"].at[t], sem["mesh_r"].at[t], "mp", z_peers[t]
        )

    def send_total(t):
        mesh_copy(t).start()

    def receive_total(t):
        remote(
            parts_mp.at[t], parts_mp.at[t], sem["mesh_s"].at[t], sem["mesh_r"].at[t], "mp", z
        ).wait_recv()

    for i in range(4):
        sent(left.at[rows(i)], sem["left_s"].at[i])

    @pl.loop(0, nb)
    def _(i):
        for t in range(2):
            at = pl.ds(t * wide, wide)
            rot_send[i, :, at] = jnp.dot(
                left_t[i], turned[:, at], preferred_element_type=f32
            ).astype(bf16)

        @pl.when(i < 3)
        def _():
            send(
                rot_send.at[i], rot_recv.at[i], sem["rot_s"].at[i], sem["rot_r"].at[i], device(i)
            )

        @pl.when(i == 0)
        def _():
            folded = part[...]
            for j in range(1, n):
                s = lax.rem(me + j, n)
                received(parts_dp.at[s], sem["norm_r"].at[s])
                folded = folded + parts_dp[s]
            totals[0] = folded
            send_total(0)

    receive_total(0)
    totals[1] = totals[0] + parts_mp[0]
    send_total(1)
    receive_total(1)
    squares_sum = jnp.sum(totals[1] + parts_mp[1])
    clip_scale = jnp.minimum(
        1.0, 2.0 * D / jnp.sqrt(jnp.full((8, 128), squares_sum + norm_epsilon, f32))
    )
    total_scale = clip_scale[0:1, 0:1]

    locals_in[7].wait()
    locals_in[8].wait()
    bias_one = 1.0 - beta_one**STEP
    bias_two = 1.0 - beta_two**STEP

    def moments(i, src):
        b = chip(i)

        def strip(at):
            r = at(0)
            clipped = total_scale * src[i, r].astype(f32)
            mean = beta_one * new_first[b, r] + (1.0 - beta_one) * clipped
            var = beta_two * new_second[b, r] + (1.0 - beta_two) * clipped * clipped
            new_first[b, r] = mean
            new_second[b, r] = var
            dir_send[i, r] = (
                mean / bias_one / (jnp.sqrt(var / bias_two) + epsilon)
            ).astype(bf16)

        strips(strip, 16)

    for i in range(4):
        sent(right.at[rows(i)], sem["right_s"].at[i])
    moments(3, rot_send)

    @pl.loop(0, 3)
    def _(i):
        received(rot_recv.at[i], sem["rot_r"].at[i])
        moments(i, rot_recv)
        send(dir_send.at[i], dir_recv.at[i], sem["dir_s"].at[i], sem["dir_r"].at[i], device(i))

    def back_slab(i, src):
        s = device(i)
        for t in range(2):
            at = pl.ds(t * wide, wide)
            back[rows(s), at] = lax.dot_general(
                src[i], right[at, :], (((1,), (1,)), ((), ())), preferred_element_type=f32
            ).astype(bf16)
        send(back.at[rows(s)], back.at[rows(s)], sem["back_s"].at[i], sem["back_r"].at[i], partner)

    back_slab(3, dir_send)

    @pl.loop(0, 3)
    def _(i):
        received(dir_recv.at[i], sem["dir_r"].at[i])

        @pl.when(i == 0)
        def _():
            send_low(2)
            send_low_part(1)

        back_slab(i, dir_recv)

    for i in range(4):
        received(back.at[rows(2 * chip(swapped[i]) + 1 - k)], sem["back_r"].at[i])

    def hand_on(b, s, send_sem, target):
        send(
            weights.at[b, rows(s)], weights.at[b, rows(s)], send_sem, sem["out_r"].at[b * n + s], target
        )

    def arrived(b, s):
        received(weights.at[b, rows(s)], sem["out_r"].at[b * n + s])

    def relative(first_flip, second_flip):
        return c + first_flip * (one - c) + second_flip * (two - c)

    @pl.loop(0, nb)
    def _(q):
        b = relative(q % 2, q // 2)
        s = 2 * b + k

        @pl.when((q == 1) + (q == 2) > 0)
        def _():
            received(low_recv.at[b], sem["low_r"].at[b])

        @pl.when(q == 3)
        def _():
            for t in range(2):
                received(low_recv.at[b, pl.ds(0, rb // 2)], sem["low_part_r"].at[t])

        for t in range(2):
            at = pl.ds(t * wide, wide)
            update = jnp.dot(left[rows(s)], back[:, at], preferred_element_type=f32)
            weights[c, rows(s), at] = (
                low_recv[b, :, at].astype(f32) * keep - learning_rate * update
            ).astype(bf16)
        hand_on(c, s, sem["out_s"].at[q], 2 * one + k)
        hand_on(c, s, sem["out_s"].at[nb + q], 2 * two + k)
        hand_on(c, s, sem["out_s"].at[2 * nb + q], partner)

    def finish(i):
        b = chip(i)

        def strip(at):
            r = at(0)
            low = low_send[b, r].astype(f32)
            new_master[b, r] = weights[b, at(me * rb)].astype(f32) + keep * (new_master[b, r] - low)

        strips(strip)

    finish(3)

    for q in range(nb):
        s = 2 * relative(1 - q % 2, q // 2) + k
        arrived(one, s)
        hand_on(one, s, sem["pass_s"].at[q], 2 * two + k)
        hand_on(one, s, sem["pass_s"].at[nb + q], partner)
        s = 2 * relative(q % 2, 1 - q // 2) + k
        arrived(two, s)
        hand_on(two, s, sem["pass_s"].at[2 * nb + q], partner)

    finish(1)
    finish(2)

    for q in range(nb):
        s = 2 * relative(1 - q % 2, 1 - q // 2) + k
        arrived(chip(0), s)
        hand_on(chip(0), s, sem["pass_s"].at[3 * nb + q], partner)

    finish(0)

    for i in range(4):
        sent(pair_recv.at[i], sem["pair_s"].at[i])
        sent(turned.at[rows(i)], sem["turned_s"].at[i])
        sent(back.at[rows(i)], sem["back_s"].at[i])
        sent(hop_two.at[rows(i)], sem["two_s"].at[i])
    for i in range(3):
        sent(rot_send.at[i], sem["rot_s"].at[i])
        sent(dir_send.at[i], sem["dir_s"].at[i])
        sent(right.at[rows(i)], sem["right_s"].at[4 + i])
        sent(left.at[rows(i)], sem["left_s"].at[4 + i])
    for i in (1, 2):
        sent(low_send.at[i], sem["low_s"].at[i])
    for t in range(2):
        sent(low_send.at[0, pl.ds(0, rb // 2)], sem["low_s"].at[3 * t])
    for i in range(8):
        sent(hop_two.at[rows(0)], sem["one_s"].at[i])
    for j in range(1, n):
        sent(part, sem["norm_s"].at[j])
    for t in range(2):
        mesh_copy(t).wait_send()
    for i in range(12):
        sent(weights.at[0, rows(0)], sem["out_s"].at[i])
    for i in range(16):
        sent(weights.at[0, rows(0)], sem["pass_s"].at[i])

    @pl.loop(0, nb)
    def _(b):
        for q in range(nb):
            arrived(b, 2 * q + 1 - k)


def store_kernel(weights, master, first, second, weights_out, master_out, first_out, second_out, sem):
    nb = weights.shape[0]
    pairs = [(weights.at[b], weights_out.at[b]) for b in range(nb)]
    pairs += [(master, master_out), (first, first_out), (second, second_out)]
    copies = [
        pltpu.make_async_copy(src, dst, sem.at[i]) for i, (src, dst) in enumerate(pairs)
    ]
    for copy in copies:
        copy.start()
    for copy in copies:
        copy.wait()


def per_device(n, m, grad_parts, master, first_moment, second_moment, left_basis, right_basis):
    nb, rb, cols = master.shape
    blk = rb * n
    args = (grad_parts, master, first_moment, second_moment, left_basis, right_basis)
    if n != 2 * nb or nb != 4 or m != 4:
        return per_device_general(n, m, *args)
    bf16, f32 = jnp.bfloat16, jnp.float32
    half = blk // 2
    scratch = [
        pltpu.VMEM((nb, half, cols), bf16),
        pltpu.VMEM((nb, half, cols), bf16),
        pltpu.VMEM((blk, cols), bf16),
        pltpu.VMEM((blk, cols), bf16),
        pltpu.VMEM((nb, rb, blk), bf16),
        pltpu.VMEM((2, half, cols), bf16),
        pltpu.VMEM((half, cols), bf16),
        pltpu.VMEM((blk, cols), bf16),
        pltpu.VMEM((nb, rb, cols), bf16),
        pltpu.VMEM((nb, rb, cols), bf16),
        pltpu.VMEM((nb, rb, cols), bf16),
        pltpu.VMEM((nb, rb, cols), bf16),
        pltpu.VMEM((blk, cols), bf16),
        pltpu.VMEM((nb, rb, cols), bf16),
        pltpu.VMEM((nb, rb, cols), bf16),
        pltpu.VMEM((8, cols), f32),
        pltpu.VMEM((8, 128), f32),
        pltpu.VMEM((n, 8, 128), f32),
        pltpu.VMEM((2, 8, 128), f32),
        pltpu.VMEM((2, 8, 128), f32),
    ] + [pltpu.SemaphoreType.DMA((size,)) for _, size in SEMAPHORES]
    shapes = [
        jax.ShapeDtypeStruct((nb, blk, cols), bf16),
        jax.ShapeDtypeStruct(master.shape, f32),
        jax.ShapeDtypeStruct(master.shape, f32),
        jax.ShapeDtypeStruct(master.shape, f32),
    ]
    hbm = pl.BlockSpec(memory_space=pltpu.HBM)
    results = pl.pallas_call(
        functools.partial(step_kernel, n, m),
        out_shape=[pltpu.VMEM(shape.shape, shape.dtype) for shape in shapes],
        in_specs=[hbm] * 6,
        out_specs=[VMEM] * 4,
        scratch_shapes=scratch,
        compiler_params=pltpu.CompilerParams(
            collective_id=0, has_side_effects=True, vmem_limit_bytes=44 * 1024 * 1024
        ),
    )(grad_parts.reshape(nb, blk, cols), *args[1:])
    return pl.pallas_call(
        store_kernel,
        out_shape=shapes,
        in_specs=[VMEM] * 4,
        out_specs=[hbm] * 4,
        scratch_shapes=[pltpu.SemaphoreType.DMA((nb + 3,))],
        compiler_params=pltpu.CompilerParams(vmem_limit_bytes=1024 * 1024),
    )(*results)


def solution(mesh):
    n, m = mesh.shape["dp"], mesh.shape["mp"]
    return jax.shard_map(
        functools.partial(per_device, n, m),
        mesh=mesh,
        in_specs=(
            P("dp", None, None, "mp"),
            P(None, "dp", "mp"),
            P(None, "dp", "mp"),
            P(None, "dp", "mp"),
            P(None, "dp", "mp"),
            P(None, "dp", "mp"),
        ),
        out_specs=(
            P(None, None, "mp"),
            P(None, "dp", "mp"),
            P(None, "dp", "mp"),
            P(None, "dp", "mp"),
        ),
        check_vma=False,
    )
```

```python
import functools

import jax
import jax.numpy as jnp
from jax import lax
from jax.experimental import pallas as pl
from jax.experimental.pallas import tpu as pltpu
from jax.sharding import PartitionSpec as P

D = 4096
STEP = 10


beta_one = 0.95
beta_two = 0.95
epsilon = 1e-08
norm_epsilon = 1e-06
learning_rate = 0.3
decay_rate = 0.1

VMEM = pl.BlockSpec(memory_space=pltpu.VMEM)
MESH = pl.DeviceIdType.MESH


def remote(src, dst, send, recv, axis, index):
    return pltpu.make_async_remote_copy(
        src_ref=src,
        dst_ref=dst,
        send_sem=send,
        recv_sem=recv,
        device_id={axis: index},
        device_id_type=MESH,
    )


def enter(axes):
    barrier = pltpu.get_barrier_semaphore()
    total = 0
    for axis, size in axes:
        me = lax.axis_index(axis)
        for step in range(1, size):
            pl.semaphore_signal(
                barrier,
                inc=1,
                device_id={axis: lax.rem(me + step, size)},
                device_id_type=MESH,
            )
        total += size - 1
    pl.semaphore_wait(barrier, total)


class Gather:
    def __init__(self, n, nb, x, y, local, first, recv, second):
        self.n, self.nb, self.q = n, nb, n // nb
        self.x, self.y = x, y
        self.local, self.first, self.recv, self.second = local, first, recv, second
        self.me = lax.axis_index("dp")
        self.g, self.r = self.me // self.q, lax.rem(self.me, self.q)
        self.sent = []

    def go(self, src, slot, send, target):
        copy = remote(src, self.y.at[slot], send, self.recv.at[slot], "dp", target)
        copy.start()
        self.sent.append(copy)

    def arrived(self, slot):
        remote(
            self.y.at[slot], self.y.at[slot], self.first.at[0], self.recv.at[slot], "dp", self.me
        ).wait_recv()

    def start(self):
        nb, q, me, g, r = self.nb, self.q, self.me, self.g, self.r
        for j in range(1, nb):
            other = lax.rem(g + j, nb)
            self.go(self.x.at[other], me, self.first.at[j], other * q + r)
        for p in range(1, q):
            self.go(self.x.at[g], me, self.second.at[p], g * q + lax.rem(r + p, q))
        self.own = pltpu.make_async_copy(self.x.at[g], self.y.at[me], self.local.at[0])
        self.own.start()

    def forward(self):
        nb, q, g, r = self.nb, self.q, self.g, self.r
        for j in range(1, nb):
            slot = lax.rem(g + nb - j, nb) * q + r
            self.arrived(slot)
            for p in range(1, q):
                self.go(
                    self.y.at[slot], slot, self.second.at[j * q + p], g * q + lax.rem(r + p, q)
                )

    def finish(self):
        nb, q, r = self.nb, self.q, self.r
        self.own.wait()
        for p in range(1, q):
            for j in range(nb):
                self.arrived(j * q + lax.rem(r + p, q))
        for copy in self.sent:
            copy.wait_send()

    @staticmethod
    def scratch(n, nb):
        return [
            pltpu.SemaphoreType.DMA((1,)),
            pltpu.SemaphoreType.DMA((nb,)),
            pltpu.SemaphoreType.DMA((n,)),
            pltpu.SemaphoreType.DMA((n,)),
        ]


class Exchange:
    def __init__(self, n, nb, to_rows, x, y, local, send, recv):
        q = n // nb
        me = lax.axis_index("dp")
        self.nb, self.x, self.y = nb, x, y
        self.local, self.send, self.recv, self.me = local, send, recv, me
        owner = lax.rem(me, q) * nb
        first = me // nb
        if to_rows:
            self.targets = [owner + k for k in range(nb)]
            self.slot = me // q
            self.sources = [k * q + first for k in range(nb)]
        else:
            self.targets = [k * q + first for k in range(nb)]
            self.slot = lax.rem(me, nb)
            self.sources = [owner + k for k in range(nb)]

    def copy(self, k):
        return remote(
            self.x.at[k],
            self.y.at[self.slot],
            self.send.at[k],
            self.recv.at[self.slot],
            "dp",
            self.targets[k],
        )

    def mine(self, k):
        return pltpu.make_async_copy(self.x.at[k], self.y.at[self.slot], self.local.at[0])

    def start(self):
        for k in range(self.nb):

            @pl.when(self.targets[k] != self.me)
            def _():
                self.copy(k).start()

            @pl.when(self.targets[k] == self.me)
            def _():
                self.mine(k).start()

    def finish(self):
        for k in range(self.nb):

            @pl.when(self.sources[k] != self.me)
            def _():
                remote(
                    self.y.at[k], self.y.at[k], self.send.at[k], self.recv.at[k], "dp", self.me
                ).wait_recv()

            @pl.when(self.targets[k] != self.me)
            def _():
                self.copy(k).wait_send()

            @pl.when(self.targets[k] == self.me)
            def _():
                self.mine(k).wait()

    @staticmethod
    def scratch(nb):
        return [
            pltpu.SemaphoreType.DMA((1,)),
            pltpu.SemaphoreType.DMA((nb,)),
            pltpu.SemaphoreType.DMA((nb,)),
        ]


class Share:
    def __init__(self, axis, size, x, y, local, send, recv):
        self.axis, self.size, self.x, self.y = axis, size, x, y
        self.local, self.send, self.recv = local, send, recv
        self.me = lax.axis_index(axis)

    def copy(self, j):
        return remote(
            self.x,
            self.y.at[self.me],
            self.send.at[j],
            self.recv.at[self.me],
            self.axis,
            lax.rem(self.me + j, self.size),
        )

    def start(self):
        for j in range(1, self.size):
            self.copy(j).start()
        self.own = pltpu.make_async_copy(self.x, self.y.at[self.me], self.local.at[0])
        self.own.start()

    def finish(self):
        self.own.wait()
        for j in range(1, self.size):
            slot = lax.rem(self.me + j, self.size)
            remote(
                self.y.at[slot], self.y.at[slot], self.send.at[j], self.recv.at[slot], self.axis, slot
            ).wait_recv()
        for j in range(1, self.size):
            self.copy(j).wait_send()

    @staticmethod
    def scratch(size):
        return [
            pltpu.SemaphoreType.DMA((1,)),
            pltpu.SemaphoreType.DMA((size,)),
            pltpu.SemaphoreType.DMA((size,)),
        ]


def bases_kernel(n, nb, left, right, master, left_out, right_out, master_out, *sems):
    enter([("dp", n)])
    one = Gather(n, nb, right, right_out, *sems[0:4])
    two = Gather(n, nb, left, left_out, *sems[4:8])
    three = Exchange(n, nb, False, master, master_out, *sems[8:11])
    one.start()
    two.start()
    three.start()
    one.forward()
    two.forward()
    one.finish()
    two.finish()
    three.finish()


def gather_kernel(n, nb, x, y, *sems):
    enter([("dp", n)])
    one = Gather(n, nb, x, y, *sems)
    one.start()
    one.forward()
    one.finish()


def scatter_kernel(n, nb, x, y, *sems):
    enter([("dp", n)])
    one = Exchange(n, nb, True, x, y, *sems)
    one.start()
    one.finish()


def scatter_sum_kernel(n, m, nb, x, part, y, parts, *sems):
    enter([("dp", n), ("mp", m)])
    two = Share("mp", m, part, parts, *sems[3:6])
    two.start()
    one = Exchange(n, nb, True, x, y, *sems[0:3])
    one.start()
    two.finish()
    one.finish()


def group_kernel(n, nb, x, part, y, parts, *sems):
    enter([("dp", n)])
    q = n // nb
    me = lax.axis_index("dp")
    g, r = me // q, lax.rem(me, q)
    local, send, recv = sems[0:3]
    copies = []
    for p in range(1, q):
        copy = remote(
            x, y.at[r], send.at[p], recv.at[r], "dp", g * q + lax.rem(r + p, q)
        )
        copy.start()
        copies.append(copy)
    two = Share("dp", n, part, parts, *sems[3:6])
    two.start()
    own = pltpu.make_async_copy(x, y.at[r], local.at[0])
    own.start()
    own.wait()
    for p in range(1, q):
        slot = lax.rem(r + p, q)
        remote(y.at[slot], y.at[slot], send.at[p], recv.at[slot], "dp", me).wait_recv()
    two.finish()
    for copy in copies:
        copy.wait_send()


def call(kernel, shapes, scratch, collective_id, *args):
    moved = sum(s.size * s.dtype.itemsize for s in shapes)
    return pl.pallas_call(
        kernel,
        out_shape=shapes,
        in_specs=[VMEM] * len(args),
        out_specs=[VMEM] * len(shapes),
        scratch_shapes=scratch,
        compiler_params=pltpu.CompilerParams(
            collective_id=collective_id, has_side_effects=True, vmem_limit_bytes=32 * 1024 * 1024
        ),
        cost_estimate=pl.CostEstimate(flops=0, bytes_accessed=16 * moved, transcendentals=0),
    )(*args)


def per_device_general(n, m, grad_parts, master, first_moment, second_moment, left_basis, right_basis):
    bf16, f32 = jnp.bfloat16, jnp.float32
    nb, rb, cols = master.shape
    blk = rb * n
    q = n // nb
    hb = blk // q
    r = lax.rem(lax.axis_index("dp"), q)
    pieces = jax.ShapeDtypeStruct((nb, rb, cols), bf16)
    block = jax.ShapeDtypeStruct((n, rb, cols), bf16)
    low_sum = lax.psum_scatter(
        grad_parts.reshape(nb * blk, cols), "dp", scatter_dimension=0, tiled=True
    )
    left, right, master_low = call(
        functools.partial(bases_kernel, n, nb),
        [block, block, pieces],
        Gather.scratch(n, nb) * 2 + Exchange.scratch(nb),
        0,
        left_basis,
        right_basis,
        master.astype(bf16),
    )
    left, right = left.reshape(blk, cols), right.reshape(blk, cols)
    left_cols = lax.dynamic_slice_in_dim(left, r * hb, hb, axis=1)
    left_rows = lax.dynamic_slice_in_dim(left, r * hb, hb, axis=0)
    gradient = low_sum.astype(f32)
    part = jnp.full((8, 128), jnp.sum(gradient * gradient), f32)
    grad_block, parts = call(
        functools.partial(group_kernel, n, nb),
        [
            jax.ShapeDtypeStruct((q, hb, cols), bf16),
            jax.ShapeDtypeStruct((n, 8, 128), f32),
        ],
        Share.scratch(q) + Share.scratch(n),
        1,
        low_sum,
        part,
    )
    part = jnp.sum(parts, axis=0)
    turned = jnp.dot(
        grad_block.reshape(blk, cols), right, preferred_element_type=f32
    ).astype(bf16)
    rotated_rows = lax.dot_general(
        left_cols, turned, (((0,), (0,)), ((), ())), preferred_element_type=f32
    ).astype(bf16)
    rotated, parts = call(
        functools.partial(scatter_sum_kernel, n, m, nb),
        [pieces, jax.ShapeDtypeStruct((m, 8, 128), f32)],
        Exchange.scratch(nb) + Share.scratch(m),
        2,
        rotated_rows.reshape(nb, rb, cols),
        part,
    )
    squares_sum = jnp.sum(parts[:, 0, 0])
    clip_scale = jnp.minimum(1.0, 2.0 * D / jnp.sqrt(squares_sum + norm_epsilon))
    clipped = clip_scale * rotated.astype(f32)
    new_first = beta_one * first_moment + (1.0 - beta_one) * clipped
    new_second = beta_two * second_moment + (1.0 - beta_two) * clipped * clipped
    bias_one = 1.0 - beta_one**STEP
    bias_two = 1.0 - beta_two**STEP
    direction = (new_first / bias_one / (jnp.sqrt(new_second / bias_two) + epsilon)).astype(bf16)
    (direction_block,) = call(
        functools.partial(gather_kernel, n, nb), [block], Gather.scratch(n, nb), 3, direction
    )
    back = lax.dot_general(
        direction_block.reshape(blk, cols),
        right,
        (((1,), (1,)), ((), ())),
        preferred_element_type=f32,
    ).astype(bf16)
    update = jnp.dot(left_rows, back, preferred_element_type=f32)
    keep = 1.0 - learning_rate * decay_rate
    weight_rows = (
        master_low.reshape(hb, cols).astype(f32) * keep - learning_rate * update
    ).astype(bf16)
    weights = lax.all_gather(weight_rows, "dp", axis=0, tiled=True).reshape(nb, blk, cols)
    (update_rows,) = call(
        functools.partial(scatter_kernel, n, nb),
        [pieces],
        Exchange.scratch(nb),
        4,
        update.astype(bf16).reshape(nb, rb, cols),
    )
    new_master = master * keep - learning_rate * update_rows.astype(f32)
    return (weights, new_master, new_first, new_second)


SEMAPHORES = (
    ("local", 7),
    ("grad", 4),
    ("pair_s", 1),
    ("pair_r", 4),
    ("right_s", 1),
    ("right_r", 3),
    ("right_pass_r", 1),
    ("left_s", 1),
    ("left_r", 3),
    ("left_pass_r", 1),
    ("pass_bases_s", 1),
    ("one_s", 1),
    ("one_r", 8),
    ("two_s", 1),
    ("two_r", 4),
    ("turned_s", 1),
    ("turned_r", 1),
    ("rot_s", 1),
    ("rot_r", 3),
    ("dir_s", 1),
    ("dir_r", 3),
    ("back_s", 1),
    ("back_r", 1),
    ("low_s", 1),
    ("low_r", 3),
    ("out_s", 1),
    ("pass_s", 1),
    ("out_r", 12),
    ("out_pass_r", 1),
    ("norm_s", 1),
    ("norm_r", 1),
    ("mesh_s", 1),
    ("mesh_r", 3),
)


def step_kernel(
    n,
    m,
    grad,
    master,
    first,
    second,
    left_in,
    right_in,
    weights,
    new_master,
    new_first,
    new_second,
    acc,
    pair_recv,
    left,
    right,
    left_t,
    hop_one,
    hop_two,
    turned,
    rot_send,
    rot_recv,
    dir_send,
    dir_recv,
    back,
    low_send,
    low_recv,
    squares,
    part,
    parts_dp,
    totals,
    parts_mp,
    *sem_refs,
):
    sem = {name: ref for (name, _), ref in zip(SEMAPHORES, sem_refs)}
    f32, bf16 = jnp.float32, jnp.bfloat16
    nb, rb, cols = master.shape
    half = nb * rb
    wide = cols // 2
    me = lax.axis_index("dp")
    c, k = me // 2, lax.rem(me, 2)
    cy, cx = c // 2, lax.rem(c, 2)
    xn, yn = 2 * cy + (1 - cx), 2 * (1 - cy) + cx
    one, two = (1 - k) * xn + k * yn, k * xn + (1 - k) * yn
    partner = me + 1 - 2 * k
    swapped = (0, 2, 1, 3)
    keep = 1.0 - learning_rate * decay_rate

    def chip(i):
        return c + (1 - i // 2) * (one - c) + (1 - i % 2) * (two - c)

    def device(i):
        return 2 * chip(i) + k

    def rows(s):
        return pl.ds(pl.multiple_of(s * rb, rb), rb)

    def send(src, dst, send_sem, recv_sem, target):
        remote(src, dst, send_sem, recv_sem, "dp", target).start()

    def received(ref, recv_sem):
        remote(ref, ref, recv_sem, recv_sem, "dp", me).wait_recv()

    def sent(ref, send_sem):
        remote(ref, ref, send_sem, send_sem, "dp", me).wait_send()

    def strips(body, step=32):
        @pl.loop(0, rb // step)
        def _(t):
            body(lambda base: pl.ds(pl.multiple_of(base + t * step, step), step))

    bases = ((dir_send, right, "right", 4), (rot_send, left, "left", 5))
    locals_in = []

    def fetch(src, dst, local_sem):
        copy = pltpu.make_async_copy(src, dst, local_sem)
        copy.start()
        locals_in.append(copy)

    stages = []
    for t, (src, stage) in enumerate(((right_in, dir_send), (left_in, rot_send))):
        stages.append(pltpu.make_async_copy(src, stage, sem["local"].at[4 + t]))
        stages[t].start()
    for i in range(nb):
        fetch(grad.at[chip(i), pl.ds(k * half, half)], acc.at[i], sem["grad"].at[i])
    fetch(right_in.at[c], right.at[rows(me)], sem["local"].at[0])
    fetch(left_in.at[c], left.at[rows(me)], sem["local"].at[1])
    fetch(master, new_master, sem["local"].at[2])
    fetch(first, new_first, sem["local"].at[3])
    fetch(second, new_second, sem["local"].at[6])

    z = lax.axis_index("mp")
    barrier = pltpu.get_barrier_semaphore()
    for j in range(1, n):
        pl.semaphore_signal(
            barrier, inc=1, device_id={"dp": lax.rem(me + j, n)}, device_id_type=MESH
        )

    @pl.when(z == 0)
    def _():
        for j in range(1, m):
            pl.semaphore_signal(barrier, inc=1, device_id={"mp": j}, device_id_type=MESH)
        pl.semaphore_wait(barrier, n - 1)

    @pl.when(z > 0)
    def _():
        pl.semaphore_wait(barrier, n)

    for t, (stage, x, name, _) in enumerate(bases):
        stages[t].wait()
        for i in range(3):
            send(
                stage.at[chip(i)],
                x.at[rows(me)],
                sem[name + "_s"].at[0],
                sem[name + "_r"].at[i],
                device(i),
            )
    for i in range(nb):
        send(
            grad.at[chip(i), pl.ds((1 - k) * half, half)],
            pair_recv.at[i],
            sem["pair_s"].at[0],
            sem["pair_r"].at[i],
            partner,
        )
    for stage, x, name, _ in bases:
        send(
            stage.at[c], x.at[rows(me)], sem[name + "_s"].at[0], sem[name + "_pass_r"].at[0], partner
        )

    for i in range(nb):
        j = swapped[i]
        locals_in[i].wait()
        received(pair_recv.at[j], sem["pair_r"].at[j])

        @pl.loop(0, nb)
        def _(q):
            def add(at):
                r = at(q * rb)
                acc[i, r] = (acc[i, r].astype(f32) + pair_recv[j, r].astype(f32)).astype(bf16)

            strips(add)
            if i < 2:
                send(
                    acc.at[i, rows(q)],
                    hop_one.at[i, rows(q)],
                    sem["one_s"].at[0],
                    sem["one_r"].at[i * nb + q],
                    2 * one + k,
                )

    locals_in[6].wait()

    @pl.loop(0, nb)
    def _(b):
        def narrow(at):
            low_send[b, at(0)] = new_master[b, at(0)].astype(bf16)

        strips(narrow)

    def own_low(at):
        low_recv[c, at(0)] = new_master[c, at(0)].astype(bf16)

    strips(own_low)

    def send_low(i):
        send(
            low_send.at[chip(i)], low_recv.at[c], sem["low_s"].at[0], sem["low_r"].at[i], device(i)
        )

    def send_low_part(t):
        part_rows = pl.ds(t * rb // 2, rb // 2)
        send(
            low_send.at[chip(0), part_rows],
            low_recv.at[c, part_rows],
            sem["low_s"].at[0],
            sem["low_r"].at[0],
            device(0),
        )

    send_low(1)

    for _, x, name, slot in bases:
        for i in range(3):
            s = device(i)
            received(x.at[rows(s)], sem[name + "_r"].at[i])
            send(
                x.at[rows(s)],
                x.at[rows(s)],
                sem["pass_bases_s"].at[0],
                sem[name + "_pass_r"].at[0],
                partner,
            )

    @pl.loop(0, nb)
    def _(q):
        received(hop_one.at[0, rows(q)], sem["one_r"].at[q])

        def add(at):
            r = at(q * rb)
            acc[2, r] = (acc[2, r].astype(f32) + hop_one[0, r].astype(f32)).astype(bf16)

        strips(add)
        send(
            acc.at[2, rows(q)],
            hop_two.at[rows(q)],
            sem["two_s"].at[0],
            sem["two_r"].at[q],
            2 * two + k,
        )

    for _, x, name, slot in bases:
        locals_in[slot].wait()
        received(x.at[pl.ds(0, half)], sem[name + "_pass_r"].at[0])

    @pl.loop(0, nb)
    def _(i):
        left_t[i] = left[:, rows(device(i))].T

    squares[...] = jnp.zeros_like(squares)

    @pl.loop(0, nb)
    def _(q):
        received(hop_two.at[rows(q)], sem["two_r"].at[q])
        received(hop_one.at[1, rows(q)], sem["one_r"].at[nb + q])

        def add(at):
            r = at(q * rb)
            g = acc[3, r].astype(f32) + hop_one[1, r].astype(f32) + hop_two[r].astype(f32)
            acc[3, r] = g.astype(bf16)
            squares[...] += jnp.sum((g * g).reshape(-1, 8, cols), axis=0)

        strips(add)

        @pl.when(q == nb - 1)
        def _():
            send_low_part(0)
            folded = squares[:, 0:128]
            for t in range(1, cols // 128):
                folded = folded + squares[:, t * 128 : (t + 1) * 128]
            part[...] = folded
            for j in range(1, n):
                send(
                    part,
                    parts_dp.at[me],
                    sem["norm_s"].at[0],
                    sem["norm_r"].at[0],
                    lax.rem(me + j, n),
                )

        s = k * nb + q
        for t in range(2):
            at = pl.ds(t * wide, wide)
            turned[rows(s), at] = jnp.dot(
                acc[3, rows(q)], right[:, at], preferred_element_type=f32
            ).astype(bf16)
        send(
            turned.at[rows(s)],
            turned.at[rows(s)],
            sem["turned_s"].at[0],
            sem["turned_r"].at[0],
            partner,
        )

    received(turned.at[pl.ds((1 - k) * half, half)], sem["turned_r"].at[0])

    def mesh_copy(t, slot, target):
        return remote(
            totals.at[t], parts_mp.at[slot], sem["mesh_s"].at[0], sem["mesh_r"].at[slot], "mp", target
        )

    sent(rot_send, sem["left_s"].at[0])

    @pl.loop(0, nb)
    def _(i):
        for t in range(2):
            at = pl.ds(t * wide, wide)
            rot_send[i, :, at] = jnp.dot(
                left_t[i], turned[:, at], preferred_element_type=f32
            ).astype(bf16)

        @pl.when(i < 3)
        def _():
            send(
                rot_send.at[i], rot_recv.at[i], sem["rot_s"].at[0], sem["rot_r"].at[i], device(i)
            )

        @pl.when(i == 0)
        def _():
            folded = part[...]
            received(parts_dp.at[pl.ds(0, n - 1)], sem["norm_r"].at[0])
            for j in range(1, n):
                folded = folded + parts_dp[lax.rem(me + j, n)]
            totals[0] = folded

            @pl.when(z > 0)
            def _():
                mesh_copy(0, z - 1, 0).start()

    @pl.when(z == 0)
    def _():
        folded = totals[0]
        for j in range(1, m):
            mesh_copy(0, j - 1, 0).wait_recv()
            folded = folded + parts_mp[j - 1]
        totals[1] = folded
        for j in range(1, m):
            mesh_copy(1, 0, j).start()

    @pl.when(z > 0)
    def _():
        mesh_copy(1, 0, 0).wait_recv()
        totals[1] = parts_mp[0]

    squares_sum = jnp.sum(totals[1])
    clip_scale = jnp.minimum(
        1.0, 2.0 * D / jnp.sqrt(jnp.full((8, 128), squares_sum + norm_epsilon, f32))
    )
    total_scale = clip_scale[0:1, 0:1]

    locals_in[7].wait()
    locals_in[8].wait()
    bias_one = 1.0 - beta_one**STEP
    bias_two = 1.0 - beta_two**STEP

    def moments(i, src):
        b = chip(i)

        def strip(at):
            r = at(0)
            clipped = total_scale * src[i, r].astype(f32)
            mean = beta_one * new_first[b, r] + (1.0 - beta_one) * clipped
            var = beta_two * new_second[b, r] + (1.0 - beta_two) * clipped * clipped
            new_first[b, r] = mean
            new_second[b, r] = var
            dir_send[i, r] = (
                mean / bias_one / (jnp.sqrt(var / bias_two) + epsilon)
            ).astype(bf16)

        strips(strip, 16)

    sent(dir_send, sem["right_s"].at[0])
    moments(3, rot_send)

    @pl.loop(0, 3)
    def _(i):
        received(rot_recv.at[i], sem["rot_r"].at[i])
        moments(i, rot_recv)
        send(dir_send.at[i], dir_recv.at[i], sem["dir_s"].at[0], sem["dir_r"].at[i], device(i))

    def back_slab(i, src):
        s = device(i)
        for t in range(2):
            at = pl.ds(t * wide, wide)
            back[rows(s), at] = lax.dot_general(
                src[i], right[at, :], (((1,), (1,)), ((), ())), preferred_element_type=f32
            ).astype(bf16)
        send(back.at[rows(s)], back.at[rows(s)], sem["back_s"].at[0], sem["back_r"].at[0], partner)

    back_slab(3, dir_send)

    @pl.loop(0, 3)
    def _(i):
        received(dir_recv.at[i], sem["dir_r"].at[i])

        @pl.when(i == 0)
        def _():
            send_low(2)
            send_low_part(1)

        back_slab(i, dir_recv)

    received(back.at[pl.ds(0, half)], sem["back_r"].at[0])

    def hand_on(b, s, name, recv_sem, target):
        send(weights.at[b, rows(s)], weights.at[b, rows(s)], sem[name].at[0], recv_sem, target)

    def slot(t, q):
        return sem["out_r"].at[t * nb + q]

    to_partner = sem["out_pass_r"].at[0]

    def relative(first_flip, second_flip):
        return c + first_flip * (one - c) + second_flip * (two - c)

    @pl.loop(0, nb)
    def _(q):
        b = relative(q % 2, q // 2)
        s = 2 * b + k

        @pl.when((q == 1) + (q == 2) > 0)
        def _():
            received(low_recv.at[b], sem["low_r"].at[q])

        @pl.when(q == 3)
        def _():
            received(low_recv.at[b], sem["low_r"].at[0])

        for t in range(2):
            at = pl.ds(t * wide, wide)
            update = jnp.dot(left[rows(s)], back[:, at], preferred_element_type=f32)
            weights[c, rows(s), at] = (
                low_recv[b, :, at].astype(f32) * keep - learning_rate * update
            ).astype(bf16)
        hand_on(c, s, "out_s", slot(0, q), 2 * one + k)
        hand_on(c, s, "out_s", slot(1, q), 2 * two + k)
        hand_on(c, s, "out_s", to_partner, partner)

    def finish(i):
        b = chip(i)

        def strip(at):
            r = at(0)
            low = low_send[b, r].astype(f32)
            new_master[b, r] = weights[b, at(me * rb)].astype(f32) + keep * (new_master[b, r] - low)

        strips(strip)

    finish(3)

    for q in range(nb):
        s = 2 * relative(1 - q % 2, q // 2) + k
        received(weights.at[one, rows(s)], slot(0, q))
        hand_on(one, s, "pass_s", slot(2, q), 2 * two + k)
        hand_on(one, s, "pass_s", to_partner, partner)
        s = 2 * relative(q % 2, 1 - q // 2) + k
        received(weights.at[two, rows(s)], slot(1, q))
        hand_on(two, s, "pass_s", to_partner, partner)

    finish(1)
    finish(2)

    for q in range(nb):
        s = 2 * relative(1 - q % 2, 1 - q // 2) + k
        received(weights.at[chip(0), rows(s)], slot(2, q))
        hand_on(chip(0), s, "pass_s", to_partner, partner)

    finish(0)

    for ref, name in (
        (pair_recv, "pair_s"),
        (hop_one, "one_s"),
        (hop_two, "two_s"),
        (turned.at[pl.ds(0, half)], "turned_s"),
        (back.at[pl.ds(0, half)], "back_s"),
        (rot_send.at[pl.ds(0, 3)], "rot_s"),
        (dir_send.at[pl.ds(0, 3)], "dir_s"),
        (low_send.at[pl.ds(0, 3)], "low_s"),
        (left.at[pl.ds(0, 6 * rb)], "pass_bases_s"),
        (parts_dp.at[pl.ds(0, n - 1)], "norm_s"),
        (acc.at[pl.ds(0, 3)], "out_s"),
        (weights.at[pl.ds(0, 2)], "pass_s"),
    ):
        sent(ref, sem[name].at[0])

    @pl.when(z == 0)
    def _():
        sent(parts_mp, sem["mesh_s"].at[0])

    @pl.when(z > 0)
    def _():
        sent(totals.at[0], sem["mesh_s"].at[0])

    received(weights.at[pl.ds(0, 2)], to_partner)


def store_kernel(weights, master, first, second, weights_out, master_out, first_out, second_out, sem):
    nb = weights.shape[0]
    pairs = [(weights.at[b], weights_out.at[b]) for b in range(nb)]
    pairs += [(master, master_out), (first, first_out), (second, second_out)]
    copies = [
        pltpu.make_async_copy(src, dst, sem.at[i]) for i, (src, dst) in enumerate(pairs)
    ]
    for copy in copies:
        copy.start()
    for copy in copies:
        copy.wait()


def per_device(n, m, grad_parts, master, first_moment, second_moment, left_basis, right_basis):
    nb, rb, cols = master.shape
    blk = rb * n
    args = (grad_parts, master, first_moment, second_moment, left_basis, right_basis)
    if n != 2 * nb or nb != 4 or m != 4:
        return per_device_general(n, m, *args)
    bf16, f32 = jnp.bfloat16, jnp.float32
    half = blk // 2
    scratch = [
        pltpu.VMEM((nb, half, cols), bf16),
        pltpu.VMEM((nb, half, cols), bf16),
        pltpu.VMEM((blk, cols), bf16),
        pltpu.VMEM((blk, cols), bf16),
        pltpu.VMEM((nb, rb, blk), bf16),
        pltpu.VMEM((2, half, cols), bf16),
        pltpu.VMEM((half, cols), bf16),
        pltpu.VMEM((blk, cols), bf16),
        pltpu.VMEM((nb, rb, cols), bf16),
        pltpu.VMEM((nb, rb, cols), bf16),
        pltpu.VMEM((nb, rb, cols), bf16),
        pltpu.VMEM((nb, rb, cols), bf16),
        pltpu.VMEM((blk, cols), bf16),
        pltpu.VMEM((nb, rb, cols), bf16),
        pltpu.VMEM((nb, rb, cols), bf16),
        pltpu.VMEM((8, cols), f32),
        pltpu.VMEM((8, 128), f32),
        pltpu.VMEM((n, 8, 128), f32),
        pltpu.VMEM((2, 8, 128), f32),
        pltpu.VMEM((m - 1, 8, 128), f32),
    ] + [pltpu.SemaphoreType.DMA((size,)) for _, size in SEMAPHORES]
    shapes = [
        jax.ShapeDtypeStruct((nb, blk, cols), bf16),
        jax.ShapeDtypeStruct(master.shape, f32),
        jax.ShapeDtypeStruct(master.shape, f32),
        jax.ShapeDtypeStruct(master.shape, f32),
    ]
    hbm = pl.BlockSpec(memory_space=pltpu.HBM)
    results = pl.pallas_call(
        functools.partial(step_kernel, n, m),
        out_shape=[pltpu.VMEM(shape.shape, shape.dtype) for shape in shapes],
        in_specs=[hbm] * 6,
        out_specs=[VMEM] * 4,
        scratch_shapes=scratch,
        compiler_params=pltpu.CompilerParams(
            collective_id=0, has_side_effects=True, vmem_limit_bytes=44 * 1024 * 1024
        ),
    )(grad_parts.reshape(nb, blk, cols), *args[1:])
    return pl.pallas_call(
        store_kernel,
        out_shape=shapes,
        in_specs=[VMEM] * 4,
        out_specs=[hbm] * 4,
        scratch_shapes=[pltpu.SemaphoreType.DMA((nb + 3,))],
        compiler_params=pltpu.CompilerParams(vmem_limit_bytes=1024 * 1024),
    )(*results)


def solution(mesh):
    n, m = mesh.shape["dp"], mesh.shape["mp"]
    return jax.shard_map(
        functools.partial(per_device, n, m),
        mesh=mesh,
        in_specs=(
            P("dp", None, None, "mp"),
            P(None, "dp", "mp"),
            P(None, "dp", "mp"),
            P(None, "dp", "mp"),
            P(None, "dp", "mp"),
            P(None, "dp", "mp"),
        ),
        out_specs=(
            P(None, None, "mp"),
            P(None, "dp", "mp"),
            P(None, "dp", "mp"),
            P(None, "dp", "mp"),
        ),
        check_vma=False,
    )
```

```python
import functools

import jax
import jax.numpy as jnp
from jax import lax
from jax.experimental import pallas as pl
from jax.experimental.pallas import tpu as pltpu
from jax.sharding import PartitionSpec as P

D = 4096
STEP = 10


beta_one = 0.95
beta_two = 0.95
epsilon = 1e-08
norm_epsilon = 1e-06
learning_rate = 0.3
decay_rate = 0.1

VMEM = pl.BlockSpec(memory_space=pltpu.VMEM)
MESH = pl.DeviceIdType.MESH


def remote(src, dst, send, recv, axis, index):
    return pltpu.make_async_remote_copy(
        src_ref=src,
        dst_ref=dst,
        send_sem=send,
        recv_sem=recv,
        device_id={axis: index},
        device_id_type=MESH,
    )


def enter(axes):
    barrier = pltpu.get_barrier_semaphore()
    total = 0
    for axis, size in axes:
        me = lax.axis_index(axis)
        for step in range(1, size):
            pl.semaphore_signal(
                barrier,
                inc=1,
                device_id={axis: lax.rem(me + step, size)},
                device_id_type=MESH,
            )
        total += size - 1
    pl.semaphore_wait(barrier, total)


class Gather:
    def __init__(self, n, nb, x, y, local, first, recv, second):
        self.n, self.nb, self.q = n, nb, n // nb
        self.x, self.y = x, y
        self.local, self.first, self.recv, self.second = local, first, recv, second
        self.me = lax.axis_index("dp")
        self.g, self.r = self.me // self.q, lax.rem(self.me, self.q)
        self.sent = []

    def go(self, src, slot, send, target):
        copy = remote(src, self.y.at[slot], send, self.recv.at[slot], "dp", target)
        copy.start()
        self.sent.append(copy)

    def arrived(self, slot):
        remote(
            self.y.at[slot], self.y.at[slot], self.first.at[0], self.recv.at[slot], "dp", self.me
        ).wait_recv()

    def start(self):
        nb, q, me, g, r = self.nb, self.q, self.me, self.g, self.r
        for j in range(1, nb):
            other = lax.rem(g + j, nb)
            self.go(self.x.at[other], me, self.first.at[j], other * q + r)
        for p in range(1, q):
            self.go(self.x.at[g], me, self.second.at[p], g * q + lax.rem(r + p, q))
        self.own = pltpu.make_async_copy(self.x.at[g], self.y.at[me], self.local.at[0])
        self.own.start()

    def forward(self):
        nb, q, g, r = self.nb, self.q, self.g, self.r
        for j in range(1, nb):
            slot = lax.rem(g + nb - j, nb) * q + r
            self.arrived(slot)
            for p in range(1, q):
                self.go(
                    self.y.at[slot], slot, self.second.at[j * q + p], g * q + lax.rem(r + p, q)
                )

    def finish(self):
        nb, q, r = self.nb, self.q, self.r
        self.own.wait()
        for p in range(1, q):
            for j in range(nb):
                self.arrived(j * q + lax.rem(r + p, q))
        for copy in self.sent:
            copy.wait_send()

    @staticmethod
    def scratch(n, nb):
        return [
            pltpu.SemaphoreType.DMA((1,)),
            pltpu.SemaphoreType.DMA((nb,)),
            pltpu.SemaphoreType.DMA((n,)),
            pltpu.SemaphoreType.DMA((n,)),
        ]


class Exchange:
    def __init__(self, n, nb, to_rows, x, y, local, send, recv):
        q = n // nb
        me = lax.axis_index("dp")
        self.nb, self.x, self.y = nb, x, y
        self.local, self.send, self.recv, self.me = local, send, recv, me
        owner = lax.rem(me, q) * nb
        first = me // nb
        if to_rows:
            self.targets = [owner + k for k in range(nb)]
            self.slot = me // q
            self.sources = [k * q + first for k in range(nb)]
        else:
            self.targets = [k * q + first for k in range(nb)]
            self.slot = lax.rem(me, nb)
            self.sources = [owner + k for k in range(nb)]

    def copy(self, k):
        return remote(
            self.x.at[k],
            self.y.at[self.slot],
            self.send.at[k],
            self.recv.at[self.slot],
            "dp",
            self.targets[k],
        )

    def mine(self, k):
        return pltpu.make_async_copy(self.x.at[k], self.y.at[self.slot], self.local.at[0])

    def start(self):
        for k in range(self.nb):

            @pl.when(self.targets[k] != self.me)
            def _():
                self.copy(k).start()

            @pl.when(self.targets[k] == self.me)
            def _():
                self.mine(k).start()

    def finish(self):
        for k in range(self.nb):

            @pl.when(self.sources[k] != self.me)
            def _():
                remote(
                    self.y.at[k], self.y.at[k], self.send.at[k], self.recv.at[k], "dp", self.me
                ).wait_recv()

            @pl.when(self.targets[k] != self.me)
            def _():
                self.copy(k).wait_send()

            @pl.when(self.targets[k] == self.me)
            def _():
                self.mine(k).wait()

    @staticmethod
    def scratch(nb):
        return [
            pltpu.SemaphoreType.DMA((1,)),
            pltpu.SemaphoreType.DMA((nb,)),
            pltpu.SemaphoreType.DMA((nb,)),
        ]


class Share:
    def __init__(self, axis, size, x, y, local, send, recv):
        self.axis, self.size, self.x, self.y = axis, size, x, y
        self.local, self.send, self.recv = local, send, recv
        self.me = lax.axis_index(axis)

    def copy(self, j):
        return remote(
            self.x,
            self.y.at[self.me],
            self.send.at[j],
            self.recv.at[self.me],
            self.axis,
            lax.rem(self.me + j, self.size),
        )

    def start(self):
        for j in range(1, self.size):
            self.copy(j).start()
        self.own = pltpu.make_async_copy(self.x, self.y.at[self.me], self.local.at[0])
        self.own.start()

    def finish(self):
        self.own.wait()
        for j in range(1, self.size):
            slot = lax.rem(self.me + j, self.size)
            remote(
                self.y.at[slot], self.y.at[slot], self.send.at[j], self.recv.at[slot], self.axis, slot
            ).wait_recv()
        for j in range(1, self.size):
            self.copy(j).wait_send()

    @staticmethod
    def scratch(size):
        return [
            pltpu.SemaphoreType.DMA((1,)),
            pltpu.SemaphoreType.DMA((size,)),
            pltpu.SemaphoreType.DMA((size,)),
        ]


def bases_kernel(n, nb, left, right, master, left_out, right_out, master_out, *sems):
    enter([("dp", n)])
    one = Gather(n, nb, right, right_out, *sems[0:4])
    two = Gather(n, nb, left, left_out, *sems[4:8])
    three = Exchange(n, nb, False, master, master_out, *sems[8:11])
    one.start()
    two.start()
    three.start()
    one.forward()
    two.forward()
    one.finish()
    two.finish()
    three.finish()


def gather_kernel(n, nb, x, y, *sems):
    enter([("dp", n)])
    one = Gather(n, nb, x, y, *sems)
    one.start()
    one.forward()
    one.finish()


def scatter_kernel(n, nb, x, y, *sems):
    enter([("dp", n)])
    one = Exchange(n, nb, True, x, y, *sems)
    one.start()
    one.finish()


def scatter_sum_kernel(n, m, nb, x, part, y, parts, *sems):
    enter([("dp", n), ("mp", m)])
    two = Share("mp", m, part, parts, *sems[3:6])
    two.start()
    one = Exchange(n, nb, True, x, y, *sems[0:3])
    one.start()
    two.finish()
    one.finish()


def group_kernel(n, nb, x, part, y, parts, *sems):
    enter([("dp", n)])
    q = n // nb
    me = lax.axis_index("dp")
    g, r = me // q, lax.rem(me, q)
    local, send, recv = sems[0:3]
    copies = []
    for p in range(1, q):
        copy = remote(
            x, y.at[r], send.at[p], recv.at[r], "dp", g * q + lax.rem(r + p, q)
        )
        copy.start()
        copies.append(copy)
    two = Share("dp", n, part, parts, *sems[3:6])
    two.start()
    own = pltpu.make_async_copy(x, y.at[r], local.at[0])
    own.start()
    own.wait()
    for p in range(1, q):
        slot = lax.rem(r + p, q)
        remote(y.at[slot], y.at[slot], send.at[p], recv.at[slot], "dp", me).wait_recv()
    two.finish()
    for copy in copies:
        copy.wait_send()


def call(kernel, shapes, scratch, collective_id, *args):
    moved = sum(s.size * s.dtype.itemsize for s in shapes)
    return pl.pallas_call(
        kernel,
        out_shape=shapes,
        in_specs=[VMEM] * len(args),
        out_specs=[VMEM] * len(shapes),
        scratch_shapes=scratch,
        compiler_params=pltpu.CompilerParams(
            collective_id=collective_id, has_side_effects=True, vmem_limit_bytes=32 * 1024 * 1024
        ),
        cost_estimate=pl.CostEstimate(flops=0, bytes_accessed=16 * moved, transcendentals=0),
    )(*args)


def per_device_general(n, m, grad_parts, master, first_moment, second_moment, left_basis, right_basis):
    bf16, f32 = jnp.bfloat16, jnp.float32
    nb, rb, cols = master.shape
    blk = rb * n
    q = n // nb
    hb = blk // q
    r = lax.rem(lax.axis_index("dp"), q)
    pieces = jax.ShapeDtypeStruct((nb, rb, cols), bf16)
    block = jax.ShapeDtypeStruct((n, rb, cols), bf16)
    low_sum = lax.psum_scatter(
        grad_parts.reshape(nb * blk, cols), "dp", scatter_dimension=0, tiled=True
    )
    left, right, master_low = call(
        functools.partial(bases_kernel, n, nb),
        [block, block, pieces],
        Gather.scratch(n, nb) * 2 + Exchange.scratch(nb),
        0,
        left_basis,
        right_basis,
        master.astype(bf16),
    )
    left, right = left.reshape(blk, cols), right.reshape(blk, cols)
    left_cols = lax.dynamic_slice_in_dim(left, r * hb, hb, axis=1)
    left_rows = lax.dynamic_slice_in_dim(left, r * hb, hb, axis=0)
    gradient = low_sum.astype(f32)
    part = jnp.full((8, 128), jnp.sum(gradient * gradient), f32)
    grad_block, parts = call(
        functools.partial(group_kernel, n, nb),
        [
            jax.ShapeDtypeStruct((q, hb, cols), bf16),
            jax.ShapeDtypeStruct((n, 8, 128), f32),
        ],
        Share.scratch(q) + Share.scratch(n),
        1,
        low_sum,
        part,
    )
    part = jnp.sum(parts, axis=0)
    turned = jnp.dot(
        grad_block.reshape(blk, cols), right, preferred_element_type=f32
    ).astype(bf16)
    rotated_rows = lax.dot_general(
        left_cols, turned, (((0,), (0,)), ((), ())), preferred_element_type=f32
    ).astype(bf16)
    rotated, parts = call(
        functools.partial(scatter_sum_kernel, n, m, nb),
        [pieces, jax.ShapeDtypeStruct((m, 8, 128), f32)],
        Exchange.scratch(nb) + Share.scratch(m),
        2,
        rotated_rows.reshape(nb, rb, cols),
        part,
    )
    squares_sum = jnp.sum(parts[:, 0, 0])
    clip_scale = jnp.minimum(1.0, 2.0 * D / jnp.sqrt(squares_sum + norm_epsilon))
    clipped = clip_scale * rotated.astype(f32)
    new_first = beta_one * first_moment + (1.0 - beta_one) * clipped
    new_second = beta_two * second_moment + (1.0 - beta_two) * clipped * clipped
    bias_one = 1.0 - beta_one**STEP
    bias_two = 1.0 - beta_two**STEP
    direction = (new_first / bias_one / (jnp.sqrt(new_second / bias_two) + epsilon)).astype(bf16)
    (direction_block,) = call(
        functools.partial(gather_kernel, n, nb), [block], Gather.scratch(n, nb), 3, direction
    )
    back = lax.dot_general(
        direction_block.reshape(blk, cols),
        right,
        (((1,), (1,)), ((), ())),
        preferred_element_type=f32,
    ).astype(bf16)
    update = jnp.dot(left_rows, back, preferred_element_type=f32)
    keep = 1.0 - learning_rate * decay_rate
    weight_rows = (
        master_low.reshape(hb, cols).astype(f32) * keep - learning_rate * update
    ).astype(bf16)
    weights = lax.all_gather(weight_rows, "dp", axis=0, tiled=True).reshape(nb, blk, cols)
    (update_rows,) = call(
        functools.partial(scatter_kernel, n, nb),
        [pieces],
        Exchange.scratch(nb),
        4,
        update.astype(bf16).reshape(nb, rb, cols),
    )
    new_master = master * keep - learning_rate * update_rows.astype(f32)
    return (weights, new_master, new_first, new_second)


SEMAPHORES = (
    ("local", 7),
    ("grad", 1),
    ("pair_s", 1),
    ("pair_r", 1),
    ("right_s", 1),
    ("right_r", 3),
    ("right_pass_r", 1),
    ("left_s", 1),
    ("left_r", 3),
    ("left_pass_r", 1),
    ("pass_bases_s", 1),
    ("one_s", 1),
    ("one_r", 4),
    ("two_s", 1),
    ("two_r", 4),
    ("turned_s", 1),
    ("turned_r", 1),
    ("rot_s", 1),
    ("rot_r", 3),
    ("dir_s", 1),
    ("dir_r", 3),
    ("back_s", 1),
    ("back_r", 1),
    ("low_s", 1),
    ("low_r", 3),
    ("out_s", 1),
    ("pass_s", 1),
    ("out_r", 15),
    ("out_pass_r", 1),
    ("norm_s", 1),
    ("norm_r", 1),
    ("mesh_s", 1),
    ("mesh_r", 3),
)


def step_kernel(
    n,
    m,
    grad,
    master,
    first,
    second,
    left_in,
    right_in,
    weights,
    new_master,
    new_first,
    new_second,
    acc,
    pair_recv,
    left,
    right,
    left_t,
    hop_one,
    hop_two,
    turned,
    rot_send,
    rot_recv,
    dir_send,
    dir_recv,
    back,
    low_send,
    low_recv,
    squares,
    part,
    parts_dp,
    totals,
    parts_mp,
    *sem_refs,
):
    sem = {name: ref for (name, _), ref in zip(SEMAPHORES, sem_refs)}
    f32, bf16 = jnp.float32, jnp.bfloat16
    nb, rb, cols = master.shape
    half = nb * rb
    wide = cols // 2
    me = lax.axis_index("dp")
    c, k = me // 2, lax.rem(me, 2)
    cy, cx = c // 2, lax.rem(c, 2)
    xn, yn = 2 * cy + (1 - cx), 2 * (1 - cy) + cx
    one, two = (1 - k) * xn + k * yn, k * xn + (1 - k) * yn
    partner = me + 1 - 2 * k
    swapped = (0, 2, 1, 3)
    keep = 1.0 - learning_rate * decay_rate

    def chip(i):
        return c + (1 - i // 2) * (one - c) + (1 - i % 2) * (two - c)

    def device(i):
        return 2 * chip(i) + k

    def rows(s):
        return pl.ds(pl.multiple_of(s * rb, rb), rb)

    def send(src, dst, send_sem, recv_sem, target):
        remote(src, dst, send_sem, recv_sem, "dp", target).start()

    def received(ref, recv_sem):
        remote(ref, ref, recv_sem, recv_sem, "dp", me).wait_recv()

    def sent(ref, send_sem):
        remote(ref, ref, send_sem, send_sem, "dp", me).wait_send()

    def strips(body, step=32):
        @pl.loop(0, rb // step)
        def _(t):
            body(lambda base: pl.ds(pl.multiple_of(base + t * step, step), step))

    bases = ((dir_send, right, "right", 4), (rot_send, left, "left", 5))
    locals_in = []

    def fetch(src, dst, local_sem):
        copy = pltpu.make_async_copy(src, dst, local_sem)
        copy.start()
        locals_in.append(copy)

    stages = []
    for t, (src, stage) in enumerate(((right_in, dir_send), (left_in, rot_send))):
        stages.append(pltpu.make_async_copy(src, stage, sem["local"].at[4 + t]))
        stages[t].start()
    for i in range(nb):
        fetch(grad.at[chip(i), pl.ds(k * half, half)], acc.at[i], sem["grad"].at[0])
    fetch(right_in.at[c], right.at[rows(me)], sem["local"].at[0])
    fetch(left_in.at[c], left.at[rows(me)], sem["local"].at[1])
    fetch(master, new_master, sem["local"].at[2])
    fetch(first, new_first, sem["local"].at[3])
    fetch(second, new_second, sem["local"].at[6])

    z = lax.axis_index("mp")
    barrier = pltpu.get_barrier_semaphore()
    for target in (device(1), device(2), partner):
        pl.semaphore_signal(barrier, inc=1, device_id={"dp": target}, device_id_type=MESH)

    @pl.when(z == 0)
    def _():
        for j in range(1, m):
            pl.semaphore_signal(barrier, inc=1, device_id={"mp": j}, device_id_type=MESH)
        pl.semaphore_wait(barrier, 3)

    @pl.when(z > 0)
    def _():
        pl.semaphore_wait(barrier, 4)

    def send_base(t, i):
        stage, x, name, _ = bases[t]
        send(
            stage.at[chip(i)],
            x.at[rows(me)],
            sem[name + "_s"].at[0],
            sem[name + "_r"].at[i],
            device(i),
        )

    for t in range(2):
        stages[t].wait()
        send_base(t, 1)
        send_base(t, 2)
    for i in range(nb):
        send(
            grad.at[chip(i), pl.ds((1 - k) * half, half)],
            pair_recv.at[i],
            sem["pair_s"].at[0],
            sem["pair_r"].at[0],
            partner,
        )
    for stage, x, name, _ in bases:
        send(
            stage.at[c], x.at[rows(me)], sem[name + "_s"].at[0], sem[name + "_pass_r"].at[0], partner
        )

    def pass_base(t, i):
        _, x, name, _ = bases[t]
        s = device(i)
        received(x.at[rows(s)], sem[name + "_r"].at[i])
        send(
            x.at[rows(s)],
            x.at[rows(s)],
            sem["pass_bases_s"].at[0],
            sem[name + "_pass_r"].at[0],
            partner,
        )

    pass_base(0, 1)
    pass_base(0, 2)
    send_base(0, 0)
    send_base(1, 0)

    pltpu.make_async_copy(pair_recv, acc, sem["grad"].at[0]).wait()
    received(pair_recv, sem["pair_r"].at[0])
    for i in range(nb):
        j = swapped[i]

        @pl.loop(0, nb)
        def _(q):
            def add(at):
                r = at(q * rb)
                acc[i, r] = (acc[i, r].astype(f32) + pair_recv[j, r].astype(f32)).astype(bf16)

            strips(add)
            if i < 2:
                send(
                    acc.at[i, rows(q)],
                    hop_one.at[i, rows(q)],
                    sem["one_s"].at[0],
                    sem["one_r" if i == 0 else "two_r"].at[q],
                    2 * one + k,
                )

    locals_in[6].wait()

    @pl.loop(0, nb)
    def _(b):
        def narrow(at):
            low_send[b, at(0)] = new_master[b, at(0)].astype(bf16)

        strips(narrow)

    def own_low(at):
        low_recv[c, at(0)] = new_master[c, at(0)].astype(bf16)

    strips(own_low)

    def send_low(i):
        send(
            low_send.at[chip(i)], low_recv.at[c], sem["low_s"].at[0], sem["low_r"].at[i], device(i)
        )

    def send_low_part(t):
        part_rows = pl.ds(t * rb // 2, rb // 2)
        send(
            low_send.at[chip(0), part_rows],
            low_recv.at[c, part_rows],
            sem["low_s"].at[0],
            sem["low_r"].at[0],
            device(0),
        )

    send_low(1)

    for t, i in ((1, 1), (1, 2), (0, 0), (1, 0)):
        pass_base(t, i)

    @pl.loop(0, nb)
    def _(q):
        received(hop_one.at[0, rows(q)], sem["one_r"].at[q])

        def add(at):
            r = at(q * rb)
            acc[2, r] = (acc[2, r].astype(f32) + hop_one[0, r].astype(f32)).astype(bf16)

        strips(add)
        send(
            acc.at[2, rows(q)],
            hop_two.at[rows(q)],
            sem["two_s"].at[0],
            sem["two_r"].at[q],
            2 * two + k,
        )

    for _, x, name, slot in bases:
        locals_in[slot].wait()
        received(x.at[pl.ds(0, half)], sem[name + "_pass_r"].at[0])

    @pl.loop(0, nb)
    def _(i):
        left_t[i] = left[:, rows(device(i))].T

    squares[...] = jnp.zeros_like(squares)

    @pl.loop(0, nb)
    def _(q):
        received(hop_one.at[1, pl.ds(0, 2 * rb)], sem["two_r"].at[q])

        def add(at):
            r = at(q * rb)
            g = acc[3, r].astype(f32) + hop_one[1, r].astype(f32) + hop_two[r].astype(f32)
            acc[3, r] = g.astype(bf16)
            squares[...] += jnp.sum((g * g).reshape(-1, 8, cols), axis=0)

        strips(add)

        @pl.when(q == nb - 1)
        def _():
            send_low_part(0)
            folded = squares[:, 0:128]
            for t in range(1, cols // 128):
                folded = folded + squares[:, t * 128 : (t + 1) * 128]
            part[...] = folded
            for j in range(1, n):
                send(
                    part,
                    parts_dp.at[me],
                    sem["norm_s"].at[0],
                    sem["norm_r"].at[0],
                    lax.rem(me + j, n),
                )

        s = k * nb + q
        for t in range(2):
            at = pl.ds(t * wide, wide)
            turned[rows(s), at] = jnp.dot(
                acc[3, rows(q)], right[:, at], preferred_element_type=f32
            ).astype(bf16)
        send(
            turned.at[rows(s)],
            turned.at[rows(s)],
            sem["turned_s"].at[0],
            sem["turned_r"].at[0],
            partner,
        )

    received(turned.at[pl.ds((1 - k) * half, half)], sem["turned_r"].at[0])

    def mesh_copy(t, slot, target):
        return remote(
            totals.at[t], parts_mp.at[slot], sem["mesh_s"].at[0], sem["mesh_r"].at[slot], "mp", target
        )

    sent(rot_send, sem["left_s"].at[0])

    @pl.loop(0, nb)
    def _(i):
        for t in range(2):
            at = pl.ds(t * wide, wide)
            rot_send[i, :, at] = jnp.dot(
                left_t[i], turned[:, at], preferred_element_type=f32
            ).astype(bf16)

        @pl.when(i < 3)
        def _():
            send(
                rot_send.at[i], rot_recv.at[i], sem["rot_s"].at[0], sem["rot_r"].at[i], device(i)
            )

        @pl.when(i == 0)
        def _():
            folded = part[...]
            received(parts_dp.at[pl.ds(0, n - 1)], sem["norm_r"].at[0])
            for j in range(1, n):
                folded = folded + parts_dp[lax.rem(me + j, n)]
            totals[0] = folded

            @pl.when(z > 0)
            def _():
                mesh_copy(0, z - 1, 0).start()

    @pl.when(z == 0)
    def _():
        folded = totals[0]
        for j in range(1, m):
            mesh_copy(0, j - 1, 0).wait_recv()
            folded = folded + parts_mp[j - 1]
        totals[1] = folded
        for j in range(1, m):
            mesh_copy(1, 0, j).start()

    @pl.when(z > 0)
    def _():
        mesh_copy(1, 0, 0).wait_recv()
        totals[1] = parts_mp[0]

    squares_sum = jnp.sum(totals[1])
    clip_scale = jnp.minimum(
        1.0, 2.0 * D / jnp.sqrt(jnp.full((8, 128), squares_sum + norm_epsilon, f32))
    )
    total_scale = clip_scale[0:1, 0:1]

    locals_in[7].wait()
    locals_in[8].wait()
    bias_one = 1.0 - beta_one**STEP
    bias_two = 1.0 - beta_two**STEP

    def moments(i, src):
        b = chip(i)

        def strip(at):
            r = at(0)
            clipped = total_scale * src[i, r].astype(f32)
            mean = beta_one * new_first[b, r] + (1.0 - beta_one) * clipped
            var = beta_two * new_second[b, r] + (1.0 - beta_two) * clipped * clipped
            new_first[b, r] = mean
            new_second[b, r] = var
            dir_send[i, r] = (
                mean / bias_one / (jnp.sqrt(var / bias_two) + epsilon)
            ).astype(bf16)

        strips(strip, 16)

    sent(dir_send, sem["right_s"].at[0])
    moments(3, rot_send)

    @pl.loop(0, 3)
    def _(i):
        received(rot_recv.at[i], sem["rot_r"].at[i])
        moments(i, rot_recv)
        send(dir_send.at[i], dir_recv.at[i], sem["dir_s"].at[0], sem["dir_r"].at[i], device(i))

    def back_slab(i, src):
        s = device(i)
        for t in range(2):
            at = pl.ds(t * wide, wide)
            back[rows(s), at] = lax.dot_general(
                src[i], right[at, :], (((1,), (1,)), ((), ())), preferred_element_type=f32
            ).astype(bf16)
        send(back.at[rows(s)], back.at[rows(s)], sem["back_s"].at[0], sem["back_r"].at[0], partner)

    back_slab(3, dir_send)

    @pl.loop(0, 3)
    def _(i):
        received(dir_recv.at[i], sem["dir_r"].at[i])

        @pl.when(i == 0)
        def _():
            send_low(2)
            send_low_part(1)

        back_slab(i, dir_recv)

    received(back.at[pl.ds(0, half)], sem["back_r"].at[0])

    def hand_on(b, s, name, recv_sem, target):
        send(weights.at[b, rows(s)], weights.at[b, rows(s)], sem[name].at[0], recv_sem, target)

    def piece(s, p):
        return pl.ds(pl.multiple_of(s * rb + p * (rb // 4), rb // 4), rb // 4)

    def hand_on_piece(b, s, p, recv_sem, target):
        ref = weights.at[b, piece(s, p)]
        send(ref, ref, sem["pass_s"].at[0], recv_sem, target)

    def slot(t, q):
        return sem["out_r"].at[t * nb + q]

    to_partner = sem["out_pass_r"].at[0]

    def relative(first_flip, second_flip):
        return c + first_flip * (one - c) + second_flip * (two - c)

    @pl.loop(0, nb)
    def _(q):
        b = relative(q % 2, q // 2)
        s = 2 * b + k

        @pl.when((q == 1) + (q == 2) > 0)
        def _():
            received(low_recv.at[b], sem["low_r"].at[q])

        @pl.when(q == 3)
        def _():
            received(low_recv.at[b], sem["low_r"].at[0])

        for t in range(2):
            at = pl.ds(t * wide, wide)
            update = jnp.dot(left[rows(s)], back[:, at], preferred_element_type=f32)
            weights[c, rows(s), at] = (
                low_recv[b, :, at].astype(f32) * keep - learning_rate * update
            ).astype(bf16)
        hand_on(c, s, "out_s", slot(0, q), 2 * one + k)
        hand_on(c, s, "out_s", slot(1, q), 2 * two + k)
        hand_on(c, s, "out_s", to_partner, partner)

    def finish(i):
        b = chip(i)

        def strip(at):
            r = at(0)
            low = low_send[b, r].astype(f32)
            new_master[b, r] = weights[b, at(me * rb)].astype(f32) + keep * (new_master[b, r] - low)

        strips(strip)

    finish(3)

    for q in range(nb):
        s = 2 * relative(1 - q % 2, q // 2) + k
        received(weights.at[one, rows(s)], slot(0, q))
        if q < nb - 1:
            hand_on(one, s, "pass_s", slot(2, q), 2 * two + k)
        else:
            for p in range(4):
                hand_on_piece(one, s, p, slot(2, q + p), 2 * two + k)
        hand_on(one, s, "pass_s", to_partner, partner)
        s = 2 * relative(q % 2, 1 - q // 2) + k
        received(weights.at[two, rows(s)], slot(1, q))
        hand_on(two, s, "pass_s", to_partner, partner)

    finish(1)
    finish(2)

    for q in range(nb):
        s = 2 * relative(1 - q % 2, 1 - q // 2) + k
        if q < nb - 1:
            received(weights.at[chip(0), rows(s)], slot(2, q))
            hand_on(chip(0), s, "pass_s", to_partner, partner)
        else:
            for p in range(4):
                received(weights.at[chip(0), piece(s, p)], slot(2, q + p))
                hand_on_piece(chip(0), s, p, to_partner, partner)

    finish(0)

    for ref, name in (
        (pair_recv, "pair_s"),
        (hop_one, "one_s"),
        (hop_two, "two_s"),
        (turned.at[pl.ds(0, half)], "turned_s"),
        (back.at[pl.ds(0, half)], "back_s"),
        (rot_send.at[pl.ds(0, 3)], "rot_s"),
        (dir_send.at[pl.ds(0, 3)], "dir_s"),
        (low_send.at[pl.ds(0, 3)], "low_s"),
        (left.at[pl.ds(0, 6 * rb)], "pass_bases_s"),
        (parts_dp.at[pl.ds(0, n - 1)], "norm_s"),
        (acc.at[pl.ds(0, 3)], "out_s"),
        (weights.at[pl.ds(0, 2)], "pass_s"),
    ):
        sent(ref, sem[name].at[0])

    @pl.when(z == 0)
    def _():
        sent(parts_mp, sem["mesh_s"].at[0])

    @pl.when(z > 0)
    def _():
        sent(totals.at[0], sem["mesh_s"].at[0])

    received(weights.at[pl.ds(0, 2)], to_partner)


def store_kernel(weights, master, first, second, weights_out, master_out, first_out, second_out, sem):
    nb = weights.shape[0]
    pairs = [(weights.at[b], weights_out.at[b]) for b in range(nb)]
    pairs += [(master, master_out), (first, first_out), (second, second_out)]
    copies = [
        pltpu.make_async_copy(src, dst, sem.at[i]) for i, (src, dst) in enumerate(pairs)
    ]
    for copy in copies:
        copy.start()
    for copy in copies:
        copy.wait()


def per_device(n, m, grad_parts, master, first_moment, second_moment, left_basis, right_basis):
    nb, rb, cols = master.shape
    blk = rb * n
    args = (grad_parts, master, first_moment, second_moment, left_basis, right_basis)
    if n != 2 * nb or nb != 4 or m != 4:
        return per_device_general(n, m, *args)
    bf16, f32 = jnp.bfloat16, jnp.float32
    half = blk // 2
    scratch = [
        pltpu.VMEM((nb, half, cols), bf16),
        pltpu.VMEM((nb, half, cols), bf16),
        pltpu.VMEM((blk, cols), bf16),
        pltpu.VMEM((blk, cols), bf16),
        pltpu.VMEM((nb, rb, blk), bf16),
        pltpu.VMEM((2, half, cols), bf16),
        pltpu.VMEM((half, cols), bf16),
        pltpu.VMEM((blk, cols), bf16),
        pltpu.VMEM((nb, rb, cols), bf16),
        pltpu.VMEM((nb, rb, cols), bf16),
        pltpu.VMEM((nb, rb, cols), bf16),
        pltpu.VMEM((nb, rb, cols), bf16),
        pltpu.VMEM((blk, cols), bf16),
        pltpu.VMEM((nb, rb, cols), bf16),
        pltpu.VMEM((nb, rb, cols), bf16),
        pltpu.VMEM((8, cols), f32),
        pltpu.VMEM((8, 128), f32),
        pltpu.VMEM((n, 8, 128), f32),
        pltpu.VMEM((2, 8, 128), f32),
        pltpu.VMEM((m - 1, 8, 128), f32),
    ] + [pltpu.SemaphoreType.DMA((size,)) for _, size in SEMAPHORES]
    shapes = [
        jax.ShapeDtypeStruct((nb, blk, cols), bf16),
        jax.ShapeDtypeStruct(master.shape, f32),
        jax.ShapeDtypeStruct(master.shape, f32),
        jax.ShapeDtypeStruct(master.shape, f32),
    ]
    hbm = pl.BlockSpec(memory_space=pltpu.HBM)
    results = pl.pallas_call(
        functools.partial(step_kernel, n, m),
        out_shape=[pltpu.VMEM(shape.shape, shape.dtype) for shape in shapes],
        in_specs=[hbm] * 6,
        out_specs=[VMEM] * 4,
        scratch_shapes=scratch,
        compiler_params=pltpu.CompilerParams(
            collective_id=0, has_side_effects=True, vmem_limit_bytes=44 * 1024 * 1024
        ),
    )(grad_parts.reshape(nb, blk, cols), *args[1:])
    return pl.pallas_call(
        store_kernel,
        out_shape=shapes,
        in_specs=[VMEM] * 4,
        out_specs=[hbm] * 4,
        scratch_shapes=[pltpu.SemaphoreType.DMA((nb + 3,))],
        compiler_params=pltpu.CompilerParams(vmem_limit_bytes=1024 * 1024),
    )(*results)


def solution(mesh):
    n, m = mesh.shape["dp"], mesh.shape["mp"]
    return jax.shard_map(
        functools.partial(per_device, n, m),
        mesh=mesh,
        in_specs=(
            P("dp", None, None, "mp"),
            P(None, "dp", "mp"),
            P(None, "dp", "mp"),
            P(None, "dp", "mp"),
            P(None, "dp", "mp"),
            P(None, "dp", "mp"),
        ),
        out_specs=(
            P(None, None, "mp"),
            P(None, "dp", "mp"),
            P(None, "dp", "mp"),
            P(None, "dp", "mp"),
        ),
        check_vma=False,
    )
```

```python
import functools

import jax
import jax.numpy as jnp
from jax import lax
from jax.experimental import pallas as pl
from jax.experimental.pallas import tpu as pltpu
from jax.sharding import PartitionSpec as P

D = 4096
STEP = 10


beta_one = 0.95
beta_two = 0.95
epsilon = 1e-08
norm_epsilon = 1e-06
learning_rate = 0.3
decay_rate = 0.1

VMEM = pl.BlockSpec(memory_space=pltpu.VMEM)
MESH = pl.DeviceIdType.MESH


def remote(src, dst, send, recv, axis, index):
    return pltpu.make_async_remote_copy(
        src_ref=src,
        dst_ref=dst,
        send_sem=send,
        recv_sem=recv,
        device_id={axis: index},
        device_id_type=MESH,
    )


def enter(axes):
    barrier = pltpu.get_barrier_semaphore()
    total = 0
    for axis, size in axes:
        me = lax.axis_index(axis)
        for step in range(1, size):
            pl.semaphore_signal(
                barrier,
                inc=1,
                device_id={axis: lax.rem(me + step, size)},
                device_id_type=MESH,
            )
        total += size - 1
    pl.semaphore_wait(barrier, total)


class Gather:
    def __init__(self, n, nb, x, y, local, first, recv, second):
        self.n, self.nb, self.q = n, nb, n // nb
        self.x, self.y = x, y
        self.local, self.first, self.recv, self.second = local, first, recv, second
        self.me = lax.axis_index("dp")
        self.g, self.r = self.me // self.q, lax.rem(self.me, self.q)
        self.sent = []

    def go(self, src, slot, send, target):
        copy = remote(src, self.y.at[slot], send, self.recv.at[slot], "dp", target)
        copy.start()
        self.sent.append(copy)

    def arrived(self, slot):
        remote(
            self.y.at[slot], self.y.at[slot], self.first.at[0], self.recv.at[slot], "dp", self.me
        ).wait_recv()

    def start(self):
        nb, q, me, g, r = self.nb, self.q, self.me, self.g, self.r
        for j in range(1, nb):
            other = lax.rem(g + j, nb)
            self.go(self.x.at[other], me, self.first.at[j], other * q + r)
        for p in range(1, q):
            self.go(self.x.at[g], me, self.second.at[p], g * q + lax.rem(r + p, q))
        self.own = pltpu.make_async_copy(self.x.at[g], self.y.at[me], self.local.at[0])
        self.own.start()

    def forward(self):
        nb, q, g, r = self.nb, self.q, self.g, self.r
        for j in range(1, nb):
            slot = lax.rem(g + nb - j, nb) * q + r
            self.arrived(slot)
            for p in range(1, q):
                self.go(
                    self.y.at[slot], slot, self.second.at[j * q + p], g * q + lax.rem(r + p, q)
                )

    def finish(self):
        nb, q, r = self.nb, self.q, self.r
        self.own.wait()
        for p in range(1, q):
            for j in range(nb):
                self.arrived(j * q + lax.rem(r + p, q))
        for copy in self.sent:
            copy.wait_send()

    @staticmethod
    def scratch(n, nb):
        return [
            pltpu.SemaphoreType.DMA((1,)),
            pltpu.SemaphoreType.DMA((nb,)),
            pltpu.SemaphoreType.DMA((n,)),
            pltpu.SemaphoreType.DMA((n,)),
        ]


class Exchange:
    def __init__(self, n, nb, to_rows, x, y, local, send, recv):
        q = n // nb
        me = lax.axis_index("dp")
        self.nb, self.x, self.y = nb, x, y
        self.local, self.send, self.recv, self.me = local, send, recv, me
        owner = lax.rem(me, q) * nb
        first = me // nb
        if to_rows:
            self.targets = [owner + k for k in range(nb)]
            self.slot = me // q
            self.sources = [k * q + first for k in range(nb)]
        else:
            self.targets = [k * q + first for k in range(nb)]
            self.slot = lax.rem(me, nb)
            self.sources = [owner + k for k in range(nb)]

    def copy(self, k):
        return remote(
            self.x.at[k],
            self.y.at[self.slot],
            self.send.at[k],
            self.recv.at[self.slot],
            "dp",
            self.targets[k],
        )

    def mine(self, k):
        return pltpu.make_async_copy(self.x.at[k], self.y.at[self.slot], self.local.at[0])

    def start(self):
        for k in range(self.nb):

            @pl.when(self.targets[k] != self.me)
            def _():
                self.copy(k).start()

            @pl.when(self.targets[k] == self.me)
            def _():
                self.mine(k).start()

    def finish(self):
        for k in range(self.nb):

            @pl.when(self.sources[k] != self.me)
            def _():
                remote(
                    self.y.at[k], self.y.at[k], self.send.at[k], self.recv.at[k], "dp", self.me
                ).wait_recv()

            @pl.when(self.targets[k] != self.me)
            def _():
                self.copy(k).wait_send()

            @pl.when(self.targets[k] == self.me)
            def _():
                self.mine(k).wait()

    @staticmethod
    def scratch(nb):
        return [
            pltpu.SemaphoreType.DMA((1,)),
            pltpu.SemaphoreType.DMA((nb,)),
            pltpu.SemaphoreType.DMA((nb,)),
        ]


class Share:
    def __init__(self, axis, size, x, y, local, send, recv):
        self.axis, self.size, self.x, self.y = axis, size, x, y
        self.local, self.send, self.recv = local, send, recv
        self.me = lax.axis_index(axis)

    def copy(self, j):
        return remote(
            self.x,
            self.y.at[self.me],
            self.send.at[j],
            self.recv.at[self.me],
            self.axis,
            lax.rem(self.me + j, self.size),
        )

    def start(self):
        for j in range(1, self.size):
            self.copy(j).start()
        self.own = pltpu.make_async_copy(self.x, self.y.at[self.me], self.local.at[0])
        self.own.start()

    def finish(self):
        self.own.wait()
        for j in range(1, self.size):
            slot = lax.rem(self.me + j, self.size)
            remote(
                self.y.at[slot], self.y.at[slot], self.send.at[j], self.recv.at[slot], self.axis, slot
            ).wait_recv()
        for j in range(1, self.size):
            self.copy(j).wait_send()

    @staticmethod
    def scratch(size):
        return [
            pltpu.SemaphoreType.DMA((1,)),
            pltpu.SemaphoreType.DMA((size,)),
            pltpu.SemaphoreType.DMA((size,)),
        ]


def bases_kernel(n, nb, left, right, master, left_out, right_out, master_out, *sems):
    enter([("dp", n)])
    one = Gather(n, nb, right, right_out, *sems[0:4])
    two = Gather(n, nb, left, left_out, *sems[4:8])
    three = Exchange(n, nb, False, master, master_out, *sems[8:11])
    one.start()
    two.start()
    three.start()
    one.forward()
    two.forward()
    one.finish()
    two.finish()
    three.finish()


def gather_kernel(n, nb, x, y, *sems):
    enter([("dp", n)])
    one = Gather(n, nb, x, y, *sems)
    one.start()
    one.forward()
    one.finish()


def scatter_kernel(n, nb, x, y, *sems):
    enter([("dp", n)])
    one = Exchange(n, nb, True, x, y, *sems)
    one.start()
    one.finish()


def scatter_sum_kernel(n, m, nb, x, part, y, parts, *sems):
    enter([("dp", n), ("mp", m)])
    two = Share("mp", m, part, parts, *sems[3:6])
    two.start()
    one = Exchange(n, nb, True, x, y, *sems[0:3])
    one.start()
    two.finish()
    one.finish()


def group_kernel(n, nb, x, part, y, parts, *sems):
    enter([("dp", n)])
    q = n // nb
    me = lax.axis_index("dp")
    g, r = me // q, lax.rem(me, q)
    local, send, recv = sems[0:3]
    copies = []
    for p in range(1, q):
        copy = remote(
            x, y.at[r], send.at[p], recv.at[r], "dp", g * q + lax.rem(r + p, q)
        )
        copy.start()
        copies.append(copy)
    two = Share("dp", n, part, parts, *sems[3:6])
    two.start()
    own = pltpu.make_async_copy(x, y.at[r], local.at[0])
    own.start()
    own.wait()
    for p in range(1, q):
        slot = lax.rem(r + p, q)
        remote(y.at[slot], y.at[slot], send.at[p], recv.at[slot], "dp", me).wait_recv()
    two.finish()
    for copy in copies:
        copy.wait_send()


def call(kernel, shapes, scratch, collective_id, *args):
    moved = sum(s.size * s.dtype.itemsize for s in shapes)
    return pl.pallas_call(
        kernel,
        out_shape=shapes,
        in_specs=[VMEM] * len(args),
        out_specs=[VMEM] * len(shapes),
        scratch_shapes=scratch,
        compiler_params=pltpu.CompilerParams(
            collective_id=collective_id, has_side_effects=True, vmem_limit_bytes=32 * 1024 * 1024
        ),
        cost_estimate=pl.CostEstimate(flops=0, bytes_accessed=16 * moved, transcendentals=0),
    )(*args)


def per_device_general(n, m, grad_parts, master, first_moment, second_moment, left_basis, right_basis):
    bf16, f32 = jnp.bfloat16, jnp.float32
    nb, rb, cols = master.shape
    blk = rb * n
    q = n // nb
    hb = blk // q
    r = lax.rem(lax.axis_index("dp"), q)
    pieces = jax.ShapeDtypeStruct((nb, rb, cols), bf16)
    block = jax.ShapeDtypeStruct((n, rb, cols), bf16)
    low_sum = lax.psum_scatter(
        grad_parts.reshape(nb * blk, cols), "dp", scatter_dimension=0, tiled=True
    )
    left, right, master_low = call(
        functools.partial(bases_kernel, n, nb),
        [block, block, pieces],
        Gather.scratch(n, nb) * 2 + Exchange.scratch(nb),
        0,
        left_basis,
        right_basis,
        master.astype(bf16),
    )
    left, right = left.reshape(blk, cols), right.reshape(blk, cols)
    left_cols = lax.dynamic_slice_in_dim(left, r * hb, hb, axis=1)
    left_rows = lax.dynamic_slice_in_dim(left, r * hb, hb, axis=0)
    gradient = low_sum.astype(f32)
    part = jnp.full((8, 128), jnp.sum(gradient * gradient), f32)
    grad_block, parts = call(
        functools.partial(group_kernel, n, nb),
        [
            jax.ShapeDtypeStruct((q, hb, cols), bf16),
            jax.ShapeDtypeStruct((n, 8, 128), f32),
        ],
        Share.scratch(q) + Share.scratch(n),
        1,
        low_sum,
        part,
    )
    part = jnp.sum(parts, axis=0)
    turned = jnp.dot(
        grad_block.reshape(blk, cols), right, preferred_element_type=f32
    ).astype(bf16)
    rotated_rows = lax.dot_general(
        left_cols, turned, (((0,), (0,)), ((), ())), preferred_element_type=f32
    ).astype(bf16)
    rotated, parts = call(
        functools.partial(scatter_sum_kernel, n, m, nb),
        [pieces, jax.ShapeDtypeStruct((m, 8, 128), f32)],
        Exchange.scratch(nb) + Share.scratch(m),
        2,
        rotated_rows.reshape(nb, rb, cols),
        part,
    )
    squares_sum = jnp.sum(parts[:, 0, 0])
    clip_scale = jnp.minimum(1.0, 2.0 * D / jnp.sqrt(squares_sum + norm_epsilon))
    clipped = clip_scale * rotated.astype(f32)
    new_first = beta_one * first_moment + (1.0 - beta_one) * clipped
    new_second = beta_two * second_moment + (1.0 - beta_two) * clipped * clipped
    bias_one = 1.0 - beta_one**STEP
    bias_two = 1.0 - beta_two**STEP
    direction = (new_first / bias_one / (jnp.sqrt(new_second / bias_two) + epsilon)).astype(bf16)
    (direction_block,) = call(
        functools.partial(gather_kernel, n, nb), [block], Gather.scratch(n, nb), 3, direction
    )
    back = lax.dot_general(
        direction_block.reshape(blk, cols),
        right,
        (((1,), (1,)), ((), ())),
        preferred_element_type=f32,
    ).astype(bf16)
    update = jnp.dot(left_rows, back, preferred_element_type=f32)
    keep = 1.0 - learning_rate * decay_rate
    weight_rows = (
        master_low.reshape(hb, cols).astype(f32) * keep - learning_rate * update
    ).astype(bf16)
    weights = lax.all_gather(weight_rows, "dp", axis=0, tiled=True).reshape(nb, blk, cols)
    (update_rows,) = call(
        functools.partial(scatter_kernel, n, nb),
        [pieces],
        Exchange.scratch(nb),
        4,
        update.astype(bf16).reshape(nb, rb, cols),
    )
    new_master = master * keep - learning_rate * update_rows.astype(f32)
    return (weights, new_master, new_first, new_second)


SEMAPHORES = (
    ("local", 7),
    ("grad", 1),
    ("pair_s", 1),
    ("pair_r", 1),
    ("right_s", 1),
    ("right_r", 3),
    ("right_pass_r", 1),
    ("left_s", 1),
    ("left_r", 3),
    ("left_pass_r", 1),
    ("pass_bases_s", 1),
    ("one_s", 1),
    ("one_r", 4),
    ("two_s", 1),
    ("two_r", 4),
    ("turned_s", 1),
    ("turned_r", 1),
    ("rot_s", 1),
    ("rot_r", 3),
    ("dir_s", 1),
    ("dir_r", 3),
    ("back_s", 1),
    ("back_r", 1),
    ("low_s", 1),
    ("low_r", 3),
    ("out_s", 1),
    ("pass_s", 1),
    ("out_r", 15),
    ("out_pass_r", 1),
    ("norm_s", 1),
    ("norm_r", 1),
    ("mesh_s", 1),
    ("mesh_r", 3),
)


def step_kernel(
    n,
    m,
    grad,
    master,
    first,
    second,
    left_in,
    right_in,
    weights,
    new_master,
    new_first,
    new_second,
    acc,
    pair_recv,
    left,
    right,
    left_t,
    hop_one,
    hop_two,
    turned,
    rot_send,
    rot_recv,
    dir_send,
    dir_recv,
    back,
    low_send,
    low_recv,
    squares,
    part,
    parts_dp,
    totals,
    parts_mp,
    *sem_refs,
):
    sem = {name: ref for (name, _), ref in zip(SEMAPHORES, sem_refs)}
    f32, bf16 = jnp.float32, jnp.bfloat16
    nb, rb, cols = master.shape
    half = nb * rb
    wide = cols // 2
    me = lax.axis_index("dp")
    c, k = me // 2, lax.rem(me, 2)
    cy, cx = c // 2, lax.rem(c, 2)
    xn, yn = 2 * cy + (1 - cx), 2 * (1 - cy) + cx
    one, two = k * xn + (1 - k) * yn, (1 - k) * xn + k * yn
    partner = me + 1 - 2 * k
    swapped = (0, 2, 1, 3)
    keep = 1.0 - learning_rate * decay_rate

    def chip(i):
        return c + (1 - i // 2) * (one - c) + (1 - i % 2) * (two - c)

    def device(i):
        return 2 * chip(i) + k

    def rows(s):
        return pl.ds(pl.multiple_of(s * rb, rb), rb)

    def send(src, dst, send_sem, recv_sem, target):
        remote(src, dst, send_sem, recv_sem, "dp", target).start()

    def received(ref, recv_sem):
        remote(ref, ref, recv_sem, recv_sem, "dp", me).wait_recv()

    def sent(ref, send_sem):
        remote(ref, ref, send_sem, send_sem, "dp", me).wait_send()

    def strips(body, step=32):
        @pl.loop(0, rb // step)
        def _(t):
            body(lambda base: pl.ds(pl.multiple_of(base + t * step, step), step))

    bases = ((dir_send, right, "right", 4), (rot_send, left, "left", 5))
    locals_in = []

    def fetch(src, dst, local_sem):
        copy = pltpu.make_async_copy(src, dst, local_sem)
        copy.start()
        locals_in.append(copy)

    stages = []
    for t, (src, stage) in enumerate(((right_in, dir_send), (left_in, rot_send))):
        stages.append(pltpu.make_async_copy(src, stage, sem["local"].at[4 + t]))
        stages[t].start()
    for i in range(nb):
        fetch(grad.at[chip(i), pl.ds(k * half, half)], acc.at[i], sem["grad"].at[0])
    fetch(right_in.at[c], right.at[rows(me)], sem["local"].at[0])
    fetch(left_in.at[c], left.at[rows(me)], sem["local"].at[1])
    fetch(master, new_master, sem["local"].at[2])
    fetch(first, new_first, sem["local"].at[3])
    fetch(second, new_second, sem["local"].at[6])

    z = lax.axis_index("mp")
    barrier = pltpu.get_barrier_semaphore()
    for target in (device(1), device(2), partner):
        pl.semaphore_signal(barrier, inc=1, device_id={"dp": target}, device_id_type=MESH)

    @pl.when(z == 0)
    def _():
        for j in range(1, m):
            pl.semaphore_signal(barrier, inc=1, device_id={"mp": j}, device_id_type=MESH)
        pl.semaphore_wait(barrier, 3)

    @pl.when(z > 0)
    def _():
        pl.semaphore_wait(barrier, 4)

    def send_base(t, i):
        stage, x, name, _ = bases[t]
        send(
            stage.at[chip(i)],
            x.at[rows(me)],
            sem[name + "_s"].at[0],
            sem[name + "_r"].at[i],
            device(i),
        )

    for t in range(2):
        stages[t].wait()
        send_base(t, 1)
        send_base(t, 2)
    for i in range(nb):
        send(
            grad.at[chip(i), pl.ds((1 - k) * half, half)],
            pair_recv.at[i],
            sem["pair_s"].at[0],
            sem["pair_r"].at[0],
            partner,
        )
    for stage, x, name, _ in bases:
        send(
            stage.at[c], x.at[rows(me)], sem[name + "_s"].at[0], sem[name + "_pass_r"].at[0], partner
        )

    def pass_base(t, i):
        _, x, name, _ = bases[t]
        s = device(i)
        received(x.at[rows(s)], sem[name + "_r"].at[i])
        send(
            x.at[rows(s)],
            x.at[rows(s)],
            sem["pass_bases_s"].at[0],
            sem[name + "_pass_r"].at[0],
            partner,
        )

    pass_base(0, 1)
    pass_base(0, 2)
    send_base(0, 0)
    send_base(1, 0)

    pltpu.make_async_copy(pair_recv, acc, sem["grad"].at[0]).wait()
    received(pair_recv, sem["pair_r"].at[0])
    for i in range(nb):
        j = swapped[i]

        @pl.loop(0, nb)
        def _(q):
            def add(at):
                r = at(q * rb)
                acc[i, r] = (acc[i, r].astype(f32) + pair_recv[j, r].astype(f32)).astype(bf16)

            strips(add)
            if i < 2:
                send(
                    acc.at[i, rows(q)],
                    hop_one.at[i, rows(q)],
                    sem["one_s"].at[0],
                    sem["one_r" if i == 0 else "two_r"].at[q],
                    2 * one + k,
                )

    locals_in[6].wait()

    @pl.loop(0, nb)
    def _(b):
        def narrow(at):
            low_send[b, at(0)] = new_master[b, at(0)].astype(bf16)

        strips(narrow)

    def own_low(at):
        low_recv[c, at(0)] = new_master[c, at(0)].astype(bf16)

    strips(own_low)

    def send_low(i):
        send(
            low_send.at[chip(i)], low_recv.at[c], sem["low_s"].at[0], sem["low_r"].at[i], device(i)
        )

    def send_low_part(t):
        part_rows = pl.ds(t * rb // 2, rb // 2)
        send(
            low_send.at[chip(0), part_rows],
            low_recv.at[c, part_rows],
            sem["low_s"].at[0],
            sem["low_r"].at[0],
            device(0),
        )

    send_low(1)

    for t, i in ((1, 1), (1, 2), (0, 0), (1, 0)):
        pass_base(t, i)

    @pl.loop(0, nb)
    def _(q):
        received(hop_one.at[0, rows(q)], sem["one_r"].at[q])

        def add(at):
            r = at(q * rb)
            acc[2, r] = (acc[2, r].astype(f32) + hop_one[0, r].astype(f32)).astype(bf16)

        strips(add)
        send(
            acc.at[2, rows(q)],
            hop_two.at[rows(q)],
            sem["two_s"].at[0],
            sem["two_r"].at[q],
            2 * two + k,
        )

    for _, x, name, slot in bases:
        locals_in[slot].wait()
        received(x.at[pl.ds(0, half)], sem[name + "_pass_r"].at[0])

    @pl.loop(0, nb)
    def _(i):
        left_t[i] = left[:, rows(device(i))].T

    squares[...] = jnp.zeros_like(squares)

    @pl.loop(0, nb)
    def _(q):
        received(hop_one.at[1, pl.ds(0, 2 * rb)], sem["two_r"].at[q])

        def add(at):
            r = at(q * rb)
            g = acc[3, r].astype(f32) + hop_one[1, r].astype(f32) + hop_two[r].astype(f32)
            acc[3, r] = g.astype(bf16)
            squares[...] += jnp.sum((g * g).reshape(-1, 8, cols), axis=0)

        strips(add)

        @pl.when(q == nb - 1)
        def _():
            send_low_part(0)
            folded = squares[:, 0:128]
            for t in range(1, cols // 128):
                folded = folded + squares[:, t * 128 : (t + 1) * 128]
            part[...] = folded
            for j in range(1, n):
                send(
                    part,
                    parts_dp.at[me],
                    sem["norm_s"].at[0],
                    sem["norm_r"].at[0],
                    lax.rem(me + j, n),
                )

        s = k * nb + q
        for t in range(2):
            at = pl.ds(t * wide, wide)
            turned[rows(s), at] = jnp.dot(
                acc[3, rows(q)], right[:, at], preferred_element_type=f32
            ).astype(bf16)
        send(
            turned.at[rows(s)],
            turned.at[rows(s)],
            sem["turned_s"].at[0],
            sem["turned_r"].at[0],
            partner,
        )

    received(turned.at[pl.ds((1 - k) * half, half)], sem["turned_r"].at[0])

    def mesh_copy(t, slot, target):
        return remote(
            totals.at[t], parts_mp.at[slot], sem["mesh_s"].at[0], sem["mesh_r"].at[slot], "mp", target
        )

    sent(rot_send, sem["left_s"].at[0])

    @pl.loop(0, nb)
    def _(i):
        for t in range(2):
            at = pl.ds(t * wide, wide)
            rot_send[i, :, at] = jnp.dot(
                left_t[i], turned[:, at], preferred_element_type=f32
            ).astype(bf16)

        @pl.when(i < 3)
        def _():
            send(
                rot_send.at[i], rot_recv.at[i], sem["rot_s"].at[0], sem["rot_r"].at[i], device(i)
            )

        @pl.when(i == 0)
        def _():
            folded = part[...]
            received(parts_dp.at[pl.ds(0, n - 1)], sem["norm_r"].at[0])
            for j in range(1, n):
                folded = folded + parts_dp[lax.rem(me + j, n)]
            totals[0] = folded

            @pl.when(z > 0)
            def _():
                mesh_copy(0, z - 1, 0).start()

    @pl.when(z == 0)
    def _():
        folded = totals[0]
        for j in range(1, m):
            mesh_copy(0, j - 1, 0).wait_recv()
            folded = folded + parts_mp[j - 1]
        totals[1] = folded
        for j in range(1, m):
            mesh_copy(1, 0, j).start()

    @pl.when(z > 0)
    def _():
        mesh_copy(1, 0, 0).wait_recv()
        totals[1] = parts_mp[0]

    squares_sum = jnp.sum(totals[1])
    clip_scale = jnp.minimum(
        1.0, 2.0 * D / jnp.sqrt(jnp.full((8, 128), squares_sum + norm_epsilon, f32))
    )
    total_scale = clip_scale[0:1, 0:1]

    locals_in[7].wait()
    locals_in[8].wait()
    bias_one = 1.0 - beta_one**STEP
    bias_two = 1.0 - beta_two**STEP

    def moments(i, src):
        b = chip(i)

        def strip(at):
            r = at(0)
            clipped = total_scale * src[i, r].astype(f32)
            mean = beta_one * new_first[b, r] + (1.0 - beta_one) * clipped
            var = beta_two * new_second[b, r] + (1.0 - beta_two) * clipped * clipped
            new_first[b, r] = mean
            new_second[b, r] = var
            dir_send[i, r] = (
                mean / bias_one / (jnp.sqrt(var / bias_two) + epsilon)
            ).astype(bf16)

        strips(strip, 16)

    sent(dir_send, sem["right_s"].at[0])
    moments(3, rot_send)

    @pl.loop(0, 3)
    def _(i):
        received(rot_recv.at[i], sem["rot_r"].at[i])
        moments(i, rot_recv)
        send(dir_send.at[i], dir_recv.at[i], sem["dir_s"].at[0], sem["dir_r"].at[i], device(i))

    def back_slab(i, src):
        s = device(i)
        for t in range(2):
            at = pl.ds(t * wide, wide)
            back[rows(s), at] = lax.dot_general(
                src[i], right[at, :], (((1,), (1,)), ((), ())), preferred_element_type=f32
            ).astype(bf16)
        send(back.at[rows(s)], back.at[rows(s)], sem["back_s"].at[0], sem["back_r"].at[0], partner)

    back_slab(3, dir_send)
    send_low(2)

    @pl.loop(0, 3)
    def _(i):
        received(dir_recv.at[i], sem["dir_r"].at[i])

        @pl.when(i == 0)
        def _():
            send_low_part(1)

        back_slab(i, dir_recv)

    received(back.at[pl.ds(0, half)], sem["back_r"].at[0])

    def hand_on(b, s, name, recv_sem, target):
        send(weights.at[b, rows(s)], weights.at[b, rows(s)], sem[name].at[0], recv_sem, target)

    def piece(s, p):
        return pl.ds(pl.multiple_of(s * rb + p * (rb // 4), rb // 4), rb // 4)

    def hand_on_piece(b, s, p, recv_sem, target):
        ref = weights.at[b, piece(s, p)]
        send(ref, ref, sem["pass_s"].at[0], recv_sem, target)

    def slot(t, q):
        return sem["out_r"].at[t * nb + q]

    to_partner = sem["out_pass_r"].at[0]

    def relative(first_flip, second_flip):
        return c + first_flip * (one - c) + second_flip * (two - c)

    @pl.loop(0, nb)
    def _(q):
        b = relative(q % 2, q // 2)
        s = 2 * b + k

        @pl.when((q == 1) + (q == 2) > 0)
        def _():
            received(low_recv.at[b], sem["low_r"].at[q])

        @pl.when(q == 3)
        def _():
            received(low_recv.at[b], sem["low_r"].at[0])

        for t in range(2):
            at = pl.ds(t * wide, wide)
            update = jnp.dot(left[rows(s)], back[:, at], preferred_element_type=f32)
            weights[c, rows(s), at] = (
                low_recv[b, :, at].astype(f32) * keep - learning_rate * update
            ).astype(bf16)
        hand_on(c, s, "out_s", slot(0, q), 2 * one + k)
        hand_on(c, s, "out_s", slot(1, q), 2 * two + k)
        hand_on(c, s, "out_s", to_partner, partner)

    def finish(i):
        b = chip(i)

        def strip(at):
            r = at(0)
            low = low_send[b, r].astype(f32)
            new_master[b, r] = weights[b, at(me * rb)].astype(f32) + keep * (new_master[b, r] - low)

        strips(strip)

    finish(3)

    for q in range(nb):
        s = 2 * relative(1 - q % 2, q // 2) + k
        received(weights.at[one, rows(s)], slot(0, q))
        if q < nb - 1:
            hand_on(one, s, "pass_s", slot(2, q), 2 * two + k)
        else:
            for p in range(4):
                hand_on_piece(one, s, p, slot(2, q + p), 2 * two + k)
        hand_on(one, s, "pass_s", to_partner, partner)
        s = 2 * relative(q % 2, 1 - q // 2) + k
        received(weights.at[two, rows(s)], slot(1, q))
        hand_on(two, s, "pass_s", to_partner, partner)

    finish(1)
    finish(2)

    for q in range(nb):
        s = 2 * relative(1 - q % 2, 1 - q // 2) + k
        if q < nb - 1:
            received(weights.at[chip(0), rows(s)], slot(2, q))
            hand_on(chip(0), s, "pass_s", to_partner, partner)
        else:
            for p in range(4):
                received(weights.at[chip(0), piece(s, p)], slot(2, q + p))
                hand_on_piece(chip(0), s, p, to_partner, partner)

    finish(0)

    for ref, name in (
        (pair_recv, "pair_s"),
        (hop_one, "one_s"),
        (hop_two, "two_s"),
        (turned.at[pl.ds(0, half)], "turned_s"),
        (back.at[pl.ds(0, half)], "back_s"),
        (rot_send.at[pl.ds(0, 3)], "rot_s"),
        (dir_send.at[pl.ds(0, 3)], "dir_s"),
        (low_send.at[pl.ds(0, 3)], "low_s"),
        (left.at[pl.ds(0, 6 * rb)], "pass_bases_s"),
        (parts_dp.at[pl.ds(0, n - 1)], "norm_s"),
        (acc.at[pl.ds(0, 3)], "out_s"),
        (weights.at[pl.ds(0, 2)], "pass_s"),
    ):
        sent(ref, sem[name].at[0])

    @pl.when(z == 0)
    def _():
        sent(parts_mp, sem["mesh_s"].at[0])

    @pl.when(z > 0)
    def _():
        sent(totals.at[0], sem["mesh_s"].at[0])

    received(weights.at[pl.ds(0, 2)], to_partner)


def store_kernel(weights, master, first, second, weights_out, master_out, first_out, second_out, sem):
    nb = weights.shape[0]
    pairs = [(weights.at[b], weights_out.at[b]) for b in range(nb)]
    pairs += [(master, master_out), (first, first_out), (second, second_out)]
    copies = [
        pltpu.make_async_copy(src, dst, sem.at[i]) for i, (src, dst) in enumerate(pairs)
    ]
    for copy in copies:
        copy.start()
    for copy in copies:
        copy.wait()


def per_device(n, m, grad_parts, master, first_moment, second_moment, left_basis, right_basis):
    nb, rb, cols = master.shape
    blk = rb * n
    args = (grad_parts, master, first_moment, second_moment, left_basis, right_basis)
    if n != 2 * nb or nb != 4 or m != 4:
        return per_device_general(n, m, *args)
    bf16, f32 = jnp.bfloat16, jnp.float32
    half = blk // 2
    scratch = [
        pltpu.VMEM((nb, half, cols), bf16),
        pltpu.VMEM((nb, half, cols), bf16),
        pltpu.VMEM((blk, cols), bf16),
        pltpu.VMEM((blk, cols), bf16),
        pltpu.VMEM((nb, rb, blk), bf16),
        pltpu.VMEM((2, half, cols), bf16),
        pltpu.VMEM((half, cols), bf16),
        pltpu.VMEM((blk, cols), bf16),
        pltpu.VMEM((nb, rb, cols), bf16),
        pltpu.VMEM((nb, rb, cols), bf16),
        pltpu.VMEM((nb, rb, cols), bf16),
        pltpu.VMEM((nb, rb, cols), bf16),
        pltpu.VMEM((blk, cols), bf16),
        pltpu.VMEM((nb, rb, cols), bf16),
        pltpu.VMEM((nb, rb, cols), bf16),
        pltpu.VMEM((8, cols), f32),
        pltpu.VMEM((8, 128), f32),
        pltpu.VMEM((n, 8, 128), f32),
        pltpu.VMEM((2, 8, 128), f32),
        pltpu.VMEM((m - 1, 8, 128), f32),
    ] + [pltpu.SemaphoreType.DMA((size,)) for _, size in SEMAPHORES]
    shapes = [
        jax.ShapeDtypeStruct((nb, blk, cols), bf16),
        jax.ShapeDtypeStruct(master.shape, f32),
        jax.ShapeDtypeStruct(master.shape, f32),
        jax.ShapeDtypeStruct(master.shape, f32),
    ]
    hbm = pl.BlockSpec(memory_space=pltpu.HBM)
    results = pl.pallas_call(
        functools.partial(step_kernel, n, m),
        out_shape=[pltpu.VMEM(shape.shape, shape.dtype) for shape in shapes],
        in_specs=[hbm] * 6,
        out_specs=[VMEM] * 4,
        scratch_shapes=scratch,
        compiler_params=pltpu.CompilerParams(
            collective_id=0, has_side_effects=True, vmem_limit_bytes=44 * 1024 * 1024
        ),
    )(grad_parts.reshape(nb, blk, cols), *args[1:])
    return pl.pallas_call(
        store_kernel,
        out_shape=shapes,
        in_specs=[VMEM] * 4,
        out_specs=[hbm] * 4,
        scratch_shapes=[pltpu.SemaphoreType.DMA((nb + 3,))],
        compiler_params=pltpu.CompilerParams(vmem_limit_bytes=1024 * 1024),
    )(*results)


def solution(mesh):
    n, m = mesh.shape["dp"], mesh.shape["mp"]
    return jax.shard_map(
        functools.partial(per_device, n, m),
        mesh=mesh,
        in_specs=(
            P("dp", None, None, "mp"),
            P(None, "dp", "mp"),
            P(None, "dp", "mp"),
            P(None, "dp", "mp"),
            P(None, "dp", "mp"),
            P(None, "dp", "mp"),
        ),
        out_specs=(
            P(None, None, "mp"),
            P(None, "dp", "mp"),
            P(None, "dp", "mp"),
            P(None, "dp", "mp"),
        ),
        check_vma=False,
    )
```

```python
import functools

import jax
import jax.numpy as jnp
from jax import lax
from jax.experimental import pallas as pl
from jax.experimental.pallas import tpu as pltpu
from jax.sharding import PartitionSpec as P

D = 4096
STEP = 10


beta_one = 0.95
beta_two = 0.95
epsilon = 1e-08
norm_epsilon = 1e-06
learning_rate = 0.3
decay_rate = 0.1

VMEM = pl.BlockSpec(memory_space=pltpu.VMEM)
MESH = pl.DeviceIdType.MESH


def remote(src, dst, send, recv, axis, index):
    return pltpu.make_async_remote_copy(
        src_ref=src,
        dst_ref=dst,
        send_sem=send,
        recv_sem=recv,
        device_id={axis: index},
        device_id_type=MESH,
    )


def enter(axes):
    barrier = pltpu.get_barrier_semaphore()
    total = 0
    for axis, size in axes:
        me = lax.axis_index(axis)
        for step in range(1, size):
            pl.semaphore_signal(
                barrier,
                inc=1,
                device_id={axis: lax.rem(me + step, size)},
                device_id_type=MESH,
            )
        total += size - 1
    pl.semaphore_wait(barrier, total)


class Gather:
    def __init__(self, n, nb, x, y, local, first, recv, second):
        self.n, self.nb, self.q = n, nb, n // nb
        self.x, self.y = x, y
        self.local, self.first, self.recv, self.second = local, first, recv, second
        self.me = lax.axis_index("dp")
        self.g, self.r = self.me // self.q, lax.rem(self.me, self.q)
        self.sent = []

    def go(self, src, slot, send, target):
        copy = remote(src, self.y.at[slot], send, self.recv.at[slot], "dp", target)
        copy.start()
        self.sent.append(copy)

    def arrived(self, slot):
        remote(
            self.y.at[slot], self.y.at[slot], self.first.at[0], self.recv.at[slot], "dp", self.me
        ).wait_recv()

    def start(self):
        nb, q, me, g, r = self.nb, self.q, self.me, self.g, self.r
        for j in range(1, nb):
            other = lax.rem(g + j, nb)
            self.go(self.x.at[other], me, self.first.at[j], other * q + r)
        for p in range(1, q):
            self.go(self.x.at[g], me, self.second.at[p], g * q + lax.rem(r + p, q))
        self.own = pltpu.make_async_copy(self.x.at[g], self.y.at[me], self.local.at[0])
        self.own.start()

    def forward(self):
        nb, q, g, r = self.nb, self.q, self.g, self.r
        for j in range(1, nb):
            slot = lax.rem(g + nb - j, nb) * q + r
            self.arrived(slot)
            for p in range(1, q):
                self.go(
                    self.y.at[slot], slot, self.second.at[j * q + p], g * q + lax.rem(r + p, q)
                )

    def finish(self):
        nb, q, r = self.nb, self.q, self.r
        self.own.wait()
        for p in range(1, q):
            for j in range(nb):
                self.arrived(j * q + lax.rem(r + p, q))
        for copy in self.sent:
            copy.wait_send()

    @staticmethod
    def scratch(n, nb):
        return [
            pltpu.SemaphoreType.DMA((1,)),
            pltpu.SemaphoreType.DMA((nb,)),
            pltpu.SemaphoreType.DMA((n,)),
            pltpu.SemaphoreType.DMA((n,)),
        ]


class Exchange:
    def __init__(self, n, nb, to_rows, x, y, local, send, recv):
        q = n // nb
        me = lax.axis_index("dp")
        self.nb, self.x, self.y = nb, x, y
        self.local, self.send, self.recv, self.me = local, send, recv, me
        owner = lax.rem(me, q) * nb
        first = me // nb
        if to_rows:
            self.targets = [owner + k for k in range(nb)]
            self.slot = me // q
            self.sources = [k * q + first for k in range(nb)]
        else:
            self.targets = [k * q + first for k in range(nb)]
            self.slot = lax.rem(me, nb)
            self.sources = [owner + k for k in range(nb)]

    def copy(self, k):
        return remote(
            self.x.at[k],
            self.y.at[self.slot],
            self.send.at[k],
            self.recv.at[self.slot],
            "dp",
            self.targets[k],
        )

    def mine(self, k):
        return pltpu.make_async_copy(self.x.at[k], self.y.at[self.slot], self.local.at[0])

    def start(self):
        for k in range(self.nb):

            @pl.when(self.targets[k] != self.me)
            def _():
                self.copy(k).start()

            @pl.when(self.targets[k] == self.me)
            def _():
                self.mine(k).start()

    def finish(self):
        for k in range(self.nb):

            @pl.when(self.sources[k] != self.me)
            def _():
                remote(
                    self.y.at[k], self.y.at[k], self.send.at[k], self.recv.at[k], "dp", self.me
                ).wait_recv()

            @pl.when(self.targets[k] != self.me)
            def _():
                self.copy(k).wait_send()

            @pl.when(self.targets[k] == self.me)
            def _():
                self.mine(k).wait()

    @staticmethod
    def scratch(nb):
        return [
            pltpu.SemaphoreType.DMA((1,)),
            pltpu.SemaphoreType.DMA((nb,)),
            pltpu.SemaphoreType.DMA((nb,)),
        ]


class Share:
    def __init__(self, axis, size, x, y, local, send, recv):
        self.axis, self.size, self.x, self.y = axis, size, x, y
        self.local, self.send, self.recv = local, send, recv
        self.me = lax.axis_index(axis)

    def copy(self, j):
        return remote(
            self.x,
            self.y.at[self.me],
            self.send.at[j],
            self.recv.at[self.me],
            self.axis,
            lax.rem(self.me + j, self.size),
        )

    def start(self):
        for j in range(1, self.size):
            self.copy(j).start()
        self.own = pltpu.make_async_copy(self.x, self.y.at[self.me], self.local.at[0])
        self.own.start()

    def finish(self):
        self.own.wait()
        for j in range(1, self.size):
            slot = lax.rem(self.me + j, self.size)
            remote(
                self.y.at[slot], self.y.at[slot], self.send.at[j], self.recv.at[slot], self.axis, slot
            ).wait_recv()
        for j in range(1, self.size):
            self.copy(j).wait_send()

    @staticmethod
    def scratch(size):
        return [
            pltpu.SemaphoreType.DMA((1,)),
            pltpu.SemaphoreType.DMA((size,)),
            pltpu.SemaphoreType.DMA((size,)),
        ]


def bases_kernel(n, nb, left, right, master, left_out, right_out, master_out, *sems):
    enter([("dp", n)])
    one = Gather(n, nb, right, right_out, *sems[0:4])
    two = Gather(n, nb, left, left_out, *sems[4:8])
    three = Exchange(n, nb, False, master, master_out, *sems[8:11])
    one.start()
    two.start()
    three.start()
    one.forward()
    two.forward()
    one.finish()
    two.finish()
    three.finish()


def gather_kernel(n, nb, x, y, *sems):
    enter([("dp", n)])
    one = Gather(n, nb, x, y, *sems)
    one.start()
    one.forward()
    one.finish()


def scatter_kernel(n, nb, x, y, *sems):
    enter([("dp", n)])
    one = Exchange(n, nb, True, x, y, *sems)
    one.start()
    one.finish()


def scatter_sum_kernel(n, m, nb, x, part, y, parts, *sems):
    enter([("dp", n), ("mp", m)])
    two = Share("mp", m, part, parts, *sems[3:6])
    two.start()
    one = Exchange(n, nb, True, x, y, *sems[0:3])
    one.start()
    two.finish()
    one.finish()


def group_kernel(n, nb, x, part, y, parts, *sems):
    enter([("dp", n)])
    q = n // nb
    me = lax.axis_index("dp")
    g, r = me // q, lax.rem(me, q)
    local, send, recv = sems[0:3]
    copies = []
    for p in range(1, q):
        copy = remote(
            x, y.at[r], send.at[p], recv.at[r], "dp", g * q + lax.rem(r + p, q)
        )
        copy.start()
        copies.append(copy)
    two = Share("dp", n, part, parts, *sems[3:6])
    two.start()
    own = pltpu.make_async_copy(x, y.at[r], local.at[0])
    own.start()
    own.wait()
    for p in range(1, q):
        slot = lax.rem(r + p, q)
        remote(y.at[slot], y.at[slot], send.at[p], recv.at[slot], "dp", me).wait_recv()
    two.finish()
    for copy in copies:
        copy.wait_send()


def call(kernel, shapes, scratch, collective_id, *args):
    moved = sum(s.size * s.dtype.itemsize for s in shapes)
    return pl.pallas_call(
        kernel,
        out_shape=shapes,
        in_specs=[VMEM] * len(args),
        out_specs=[VMEM] * len(shapes),
        scratch_shapes=scratch,
        compiler_params=pltpu.CompilerParams(
            collective_id=collective_id, has_side_effects=True, vmem_limit_bytes=32 * 1024 * 1024
        ),
        cost_estimate=pl.CostEstimate(flops=0, bytes_accessed=16 * moved, transcendentals=0),
    )(*args)


def per_device_general(n, m, grad_parts, master, first_moment, second_moment, left_basis, right_basis):
    bf16, f32 = jnp.bfloat16, jnp.float32
    nb, rb, cols = master.shape
    blk = rb * n
    q = n // nb
    hb = blk // q
    r = lax.rem(lax.axis_index("dp"), q)
    pieces = jax.ShapeDtypeStruct((nb, rb, cols), bf16)
    block = jax.ShapeDtypeStruct((n, rb, cols), bf16)
    low_sum = lax.psum_scatter(
        grad_parts.reshape(nb * blk, cols), "dp", scatter_dimension=0, tiled=True
    )
    left, right, master_low = call(
        functools.partial(bases_kernel, n, nb),
        [block, block, pieces],
        Gather.scratch(n, nb) * 2 + Exchange.scratch(nb),
        0,
        left_basis,
        right_basis,
        master.astype(bf16),
    )
    left, right = left.reshape(blk, cols), right.reshape(blk, cols)
    left_cols = lax.dynamic_slice_in_dim(left, r * hb, hb, axis=1)
    left_rows = lax.dynamic_slice_in_dim(left, r * hb, hb, axis=0)
    gradient = low_sum.astype(f32)
    part = jnp.full((8, 128), jnp.sum(gradient * gradient), f32)
    grad_block, parts = call(
        functools.partial(group_kernel, n, nb),
        [
            jax.ShapeDtypeStruct((q, hb, cols), bf16),
            jax.ShapeDtypeStruct((n, 8, 128), f32),
        ],
        Share.scratch(q) + Share.scratch(n),
        1,
        low_sum,
        part,
    )
    part = jnp.sum(parts, axis=0)
    turned = jnp.dot(
        grad_block.reshape(blk, cols), right, preferred_element_type=f32
    ).astype(bf16)
    rotated_rows = lax.dot_general(
        left_cols, turned, (((0,), (0,)), ((), ())), preferred_element_type=f32
    ).astype(bf16)
    rotated, parts = call(
        functools.partial(scatter_sum_kernel, n, m, nb),
        [pieces, jax.ShapeDtypeStruct((m, 8, 128), f32)],
        Exchange.scratch(nb) + Share.scratch(m),
        2,
        rotated_rows.reshape(nb, rb, cols),
        part,
    )
    squares_sum = jnp.sum(parts[:, 0, 0])
    clip_scale = jnp.minimum(1.0, 2.0 * D / jnp.sqrt(squares_sum + norm_epsilon))
    clipped = clip_scale * rotated.astype(f32)
    new_first = beta_one * first_moment + (1.0 - beta_one) * clipped
    new_second = beta_two * second_moment + (1.0 - beta_two) * clipped * clipped
    bias_one = 1.0 - beta_one**STEP
    bias_two = 1.0 - beta_two**STEP
    direction = (new_first / bias_one / (jnp.sqrt(new_second / bias_two) + epsilon)).astype(bf16)
    (direction_block,) = call(
        functools.partial(gather_kernel, n, nb), [block], Gather.scratch(n, nb), 3, direction
    )
    back = lax.dot_general(
        direction_block.reshape(blk, cols),
        right,
        (((1,), (1,)), ((), ())),
        preferred_element_type=f32,
    ).astype(bf16)
    update = jnp.dot(left_rows, back, preferred_element_type=f32)
    keep = 1.0 - learning_rate * decay_rate
    weight_rows = (
        master_low.reshape(hb, cols).astype(f32) * keep - learning_rate * update
    ).astype(bf16)
    weights = lax.all_gather(weight_rows, "dp", axis=0, tiled=True).reshape(nb, blk, cols)
    (update_rows,) = call(
        functools.partial(scatter_kernel, n, nb),
        [pieces],
        Exchange.scratch(nb),
        4,
        update.astype(bf16).reshape(nb, rb, cols),
    )
    new_master = master * keep - learning_rate * update_rows.astype(f32)
    return (weights, new_master, new_first, new_second)


SEMAPHORES = (
    ("local", 7),
    ("grad", 1),
    ("pair_s", 1),
    ("pair_r", 1),
    ("right_s", 1),
    ("right_r", 3),
    ("right_pass_r", 1),
    ("left_s", 1),
    ("left_r", 3),
    ("left_pass_r", 1),
    ("one_s", 1),
    ("one_r", 4),
    ("two_r", 4),
    ("turned_r", 1),
    ("rot_s", 1),
    ("rot_r", 3),
    ("dir_r", 3),
    ("back_r", 1),
    ("low_s", 1),
    ("low_r", 3),
    ("out_s", 1),
    ("pass_s", 1),
    ("out_pass_r", 1),
    ("norm_s", 1),
    ("norm_r", 1),
    ("mesh_s", 1),
    ("mesh_r", 3),
)


def step_kernel(
    n,
    m,
    grad,
    master,
    first,
    second,
    left_in,
    right_in,
    weights,
    new_master,
    new_first,
    new_second,
    acc,
    pair_recv,
    left,
    right,
    left_t,
    hop_one,
    hop_two,
    turned,
    rot_send,
    rot_recv,
    dir_send,
    dir_recv,
    back,
    low_send,
    low_recv,
    squares,
    part,
    parts_dp,
    totals,
    parts_mp,
    *sem_refs,
):
    sem = {name: ref for (name, _), ref in zip(SEMAPHORES, sem_refs)}
    f32, bf16 = jnp.float32, jnp.bfloat16
    nb, rb, cols = master.shape
    half = nb * rb
    wide = cols // 2
    me = lax.axis_index("dp")
    c, k = me // 2, lax.rem(me, 2)
    cy, cx = c // 2, lax.rem(c, 2)
    xn, yn = 2 * cy + (1 - cx), 2 * (1 - cy) + cx
    one, two = k * xn + (1 - k) * yn, (1 - k) * xn + k * yn
    partner = me + 1 - 2 * k
    swapped = (0, 2, 1, 3)
    keep = 1.0 - learning_rate * decay_rate

    def chip(i):
        return c + (1 - i // 2) * (one - c) + (1 - i % 2) * (two - c)

    def device(i):
        return 2 * chip(i) + k

    def rows(s):
        return pl.ds(pl.multiple_of(s * rb, rb), rb)

    def send(src, dst, send_sem, recv_sem, target):
        remote(src, dst, send_sem, recv_sem, "dp", target).start()

    def received(ref, recv_sem):
        remote(ref, ref, recv_sem, recv_sem, "dp", me).wait_recv()

    def sent(ref, send_sem):
        remote(ref, ref, send_sem, send_sem, "dp", me).wait_send()

    def strips(body, step=32):
        @pl.loop(0, rb // step)
        def _(t):
            body(lambda base: pl.ds(pl.multiple_of(base + t * step, step), step))

    bases = ((dir_send, right, "right", 4), (rot_send, left, "left", 5))
    locals_in = []

    def fetch(src, dst, local_sem):
        copy = pltpu.make_async_copy(src, dst, local_sem)
        copy.start()
        locals_in.append(copy)

    stages = []
    for t, (src, stage) in enumerate(((right_in, dir_send), (left_in, rot_send))):
        stages.append(pltpu.make_async_copy(src, stage, sem["local"].at[4 + t]))
        stages[t].start()
    for i in range(nb):
        fetch(grad.at[chip(i), pl.ds(k * half, half)], acc.at[i], sem["grad"].at[0])
    fetch(right_in.at[c], right.at[rows(me)], sem["local"].at[0])
    fetch(left_in.at[c], left.at[rows(me)], sem["local"].at[1])
    fetch(master, new_master, sem["local"].at[2])
    fetch(first, new_first, sem["local"].at[3])
    fetch(second, new_second, sem["local"].at[6])

    z = lax.axis_index("mp")
    barrier = pltpu.get_barrier_semaphore()
    for target in (device(1), device(2), partner):
        pl.semaphore_signal(barrier, inc=1, device_id={"dp": target}, device_id_type=MESH)

    @pl.when(z == 0)
    def _():
        for j in range(1, m):
            pl.semaphore_signal(barrier, inc=1, device_id={"mp": j}, device_id_type=MESH)
        pl.semaphore_wait(barrier, 3)

    @pl.when(z > 0)
    def _():
        pl.semaphore_wait(barrier, 4)

    def send_base(t, i):
        stage, x, name, _ = bases[t]
        send(
            stage.at[chip(i)],
            x.at[rows(me)],
            sem[name + "_s"].at[0],
            sem[name + "_r"].at[i],
            device(i),
        )

    for t in range(2):
        stages[t].wait()
        send_base(t, 1)
        send_base(t, 2)
    for i in range(nb):
        send(
            grad.at[chip(i), pl.ds((1 - k) * half, half)],
            pair_recv.at[i],
            sem["pair_s"].at[0],
            sem["pair_r"].at[0],
            partner,
        )
    for stage, x, name, _ in bases:
        send(
            stage.at[c], x.at[rows(me)], sem[name + "_s"].at[0], sem[name + "_pass_r"].at[0], partner
        )

    def pass_base(t, i):
        _, x, name, _ = bases[t]
        s = device(i)
        received(x.at[rows(s)], sem[name + "_r"].at[i])
        send(
            x.at[rows(s)],
            x.at[rows(s)],
            sem["rot_s"].at[0],
            sem[name + "_pass_r"].at[0],
            partner,
        )

    pass_base(0, 1)
    pass_base(0, 2)
    send_base(0, 0)
    send_base(1, 0)

    pltpu.make_async_copy(pair_recv, acc, sem["grad"].at[0]).wait()
    received(pair_recv, sem["pair_r"].at[0])
    for i in range(nb):
        j = swapped[i]

        @pl.loop(0, nb)
        def _(q):
            def add(at):
                r = at(q * rb)
                acc[i, r] = (acc[i, r].astype(f32) + pair_recv[j, r].astype(f32)).astype(bf16)

            strips(add)
            if i < 2:
                send(
                    acc.at[i, rows(q)],
                    hop_one.at[i, rows(q)],
                    sem["one_s"].at[0],
                    sem["one_r" if i == 0 else "two_r"].at[q],
                    2 * one + k,
                )

    locals_in[6].wait()

    @pl.loop(0, nb)
    def _(b):
        def narrow(at):
            low_send[b, at(0)] = new_master[b, at(0)].astype(bf16)

        strips(narrow)

    def own_low(at):
        low_recv[c, at(0)] = new_master[c, at(0)].astype(bf16)

    strips(own_low)

    def send_low(i):
        send(
            low_send.at[chip(i)], low_recv.at[c], sem["low_s"].at[0], sem["low_r"].at[i], device(i)
        )

    def send_low_part(t):
        part_rows = pl.ds(t * rb // 2, rb // 2)
        send(
            low_send.at[chip(0), part_rows],
            low_recv.at[c, part_rows],
            sem["low_s"].at[0],
            sem["low_r"].at[0],
            device(0),
        )

    send_low(1)

    for t, i in ((1, 1), (1, 2), (0, 0), (1, 0)):
        pass_base(t, i)

    @pl.loop(0, nb)
    def _(q):
        received(hop_one.at[0, rows(q)], sem["one_r"].at[q])

        def add(at):
            r = at(q * rb)
            acc[2, r] = (acc[2, r].astype(f32) + hop_one[0, r].astype(f32)).astype(bf16)

        strips(add)
        send(
            acc.at[2, rows(q)],
            hop_two.at[rows(q)],
            sem["one_s"].at[0],
            sem["two_r"].at[q],
            2 * two + k,
        )

    for _, x, name, slot in bases:
        locals_in[slot].wait()
        received(x.at[pl.ds(0, half)], sem[name + "_pass_r"].at[0])

    @pl.loop(0, nb)
    def _(i):
        left_t[i] = left[:, rows(device(i))].T

    squares[...] = jnp.zeros_like(squares)

    @pl.loop(0, nb)
    def _(q):
        received(hop_one.at[1, pl.ds(0, 2 * rb)], sem["two_r"].at[q])

        def add(at):
            r = at(q * rb)
            g = acc[3, r].astype(f32) + hop_one[1, r].astype(f32) + hop_two[r].astype(f32)
            acc[3, r] = g.astype(bf16)
            squares[...] += jnp.sum((g * g).reshape(-1, 8, cols), axis=0)

        strips(add)

        @pl.when(q == nb - 1)
        def _():
            send_low_part(0)
            folded = squares[:, 0:128]
            for t in range(1, cols // 128):
                folded = folded + squares[:, t * 128 : (t + 1) * 128]
            part[...] = folded
            for j in range(1, n):
                send(
                    part,
                    parts_dp.at[me],
                    sem["norm_s"].at[0],
                    sem["norm_r"].at[0],
                    lax.rem(me + j, n),
                )

        s = k * nb + q
        for t in range(2):
            at = pl.ds(t * wide, wide)
            turned[rows(s), at] = jnp.dot(
                acc[3, rows(q)], right[:, at], preferred_element_type=f32
            ).astype(bf16)
        send(
            turned.at[rows(s)],
            turned.at[rows(s)],
            sem["one_s"].at[0],
            sem["turned_r"].at[0],
            partner,
        )

    received(turned.at[pl.ds((1 - k) * half, half)], sem["turned_r"].at[0])

    def mesh_copy(t, slot, target):
        return remote(
            totals.at[t], parts_mp.at[slot], sem["mesh_s"].at[0], sem["mesh_r"].at[slot], "mp", target
        )

    sent(rot_send, sem["left_s"].at[0])

    @pl.loop(0, nb)
    def _(i):
        for t in range(2):
            at = pl.ds(t * wide, wide)
            rot_send[i, :, at] = jnp.dot(
                left_t[i], turned[:, at], preferred_element_type=f32
            ).astype(bf16)

        @pl.when(i < 3)
        def _():
            send(
                rot_send.at[i], rot_recv.at[i], sem["rot_s"].at[0], sem["rot_r"].at[i], device(i)
            )

        @pl.when(i == 0)
        def _():
            folded = part[...]
            received(parts_dp.at[pl.ds(0, n - 1)], sem["norm_r"].at[0])
            for j in range(1, n):
                folded = folded + parts_dp[lax.rem(me + j, n)]
            totals[0] = folded

            @pl.when(z > 0)
            def _():
                mesh_copy(0, z - 1, 0).start()

    @pl.when(z == 0)
    def _():
        folded = totals[0]
        for j in range(1, m):
            mesh_copy(0, j - 1, 0).wait_recv()
            folded = folded + parts_mp[j - 1]
        totals[1] = folded
        for j in range(1, m):
            mesh_copy(1, 0, j).start()

    @pl.when(z > 0)
    def _():
        mesh_copy(1, 0, 0).wait_recv()
        totals[1] = parts_mp[0]

    squares_sum = jnp.sum(totals[1])
    clip_scale = jnp.minimum(
        1.0, 2.0 * D / jnp.sqrt(jnp.full((8, 128), squares_sum + norm_epsilon, f32))
    )
    total_scale = clip_scale[0:1, 0:1]

    locals_in[7].wait()
    locals_in[8].wait()
    bias_one = 1.0 - beta_one**STEP
    bias_two = 1.0 - beta_two**STEP

    def moments(i, src):
        b = chip(i)

        def strip(at):
            r = at(0)
            clipped = total_scale * src[i, r].astype(f32)
            mean = beta_one * new_first[b, r] + (1.0 - beta_one) * clipped
            var = beta_two * new_second[b, r] + (1.0 - beta_two) * clipped * clipped
            new_first[b, r] = mean
            new_second[b, r] = var
            dir_send[i, r] = (
                mean / bias_one / (jnp.sqrt(var / bias_two) + epsilon)
            ).astype(bf16)

        strips(strip, 16)

    sent(dir_send, sem["right_s"].at[0])
    moments(3, rot_send)

    @pl.loop(0, 3)
    def _(i):
        received(rot_recv.at[i], sem["rot_r"].at[i])
        moments(i, rot_recv)
        send(dir_send.at[i], dir_recv.at[i], sem["rot_s"].at[0], sem["dir_r"].at[i], device(i))

    def back_slab(i, src):
        s = device(i)
        for t in range(2):
            at = pl.ds(t * wide, wide)
            back[rows(s), at] = lax.dot_general(
                src[i], right[at, :], (((1,), (1,)), ((), ())), preferred_element_type=f32
            ).astype(bf16)
        send(back.at[rows(s)], back.at[rows(s)], sem["out_s"].at[0], sem["back_r"].at[0], partner)

    back_slab(3, dir_send)
    send_low(2)

    @pl.loop(0, 3)
    def _(i):
        received(dir_recv.at[i], sem["dir_r"].at[i])

        @pl.when(i == 0)
        def _():
            send_low_part(1)

        back_slab(i, dir_recv)

    received(back.at[pl.ds(0, half)], sem["back_r"].at[0])

    def hand_on(b, s, name, recv_sem, target):
        send(weights.at[b, rows(s)], weights.at[b, rows(s)], sem[name].at[0], recv_sem, target)

    def piece(s, p):
        return pl.ds(pl.multiple_of(s * rb + p * (rb // 4), rb // 4), rb // 4)

    def hand_on_piece(b, s, p, recv_sem, target):
        ref = weights.at[b, piece(s, p)]
        send(ref, ref, sem["pass_s"].at[0], recv_sem, target)

    def slot(t, q):
        if t < 2:
            return sem[("one_r", "two_r")[t]].at[q]
        return sem[("right_r", "left_r", "pair_r")[q // 3]].at[q % 3]

    to_partner = sem["out_pass_r"].at[0]

    def relative(first_flip, second_flip):
        return c + first_flip * (one - c) + second_flip * (two - c)

    @pl.loop(0, nb)
    def _(q):
        b = relative(q % 2, q // 2)
        s = 2 * b + k

        @pl.when((q == 1) + (q == 2) > 0)
        def _():
            received(low_recv.at[b], sem["low_r"].at[q])

        @pl.when(q == 3)
        def _():
            received(low_recv.at[b], sem["low_r"].at[0])

        for t in range(2):
            at = pl.ds(t * wide, wide)
            update = jnp.dot(left[rows(s)], back[:, at], preferred_element_type=f32)
            weights[c, rows(s), at] = (
                low_recv[b, :, at].astype(f32) * keep - learning_rate * update
            ).astype(bf16)
        hand_on(c, s, "out_s", slot(0, q), 2 * one + k)
        hand_on(c, s, "out_s", slot(1, q), 2 * two + k)
        hand_on(c, s, "out_s", to_partner, partner)

    def finish(i):
        b = chip(i)

        def strip(at):
            r = at(0)
            low = low_send[b, r].astype(f32)
            new_master[b, r] = weights[b, at(me * rb)].astype(f32) + keep * (new_master[b, r] - low)

        strips(strip)

    finish(3)

    for q in range(nb):
        s = 2 * relative(1 - q % 2, q // 2) + k
        received(weights.at[one, rows(s)], slot(0, q))
        if q < nb - 1:
            hand_on(one, s, "pass_s", slot(2, q), 2 * two + k)
        else:
            for p in range(4):
                hand_on_piece(one, s, p, slot(2, q + p), 2 * two + k)
        hand_on(one, s, "pass_s", to_partner, partner)
        s = 2 * relative(q % 2, 1 - q // 2) + k
        received(weights.at[two, rows(s)], slot(1, q))
        hand_on(two, s, "pass_s", to_partner, partner)

    finish(1)
    finish(2)

    for q in range(nb):
        s = 2 * relative(1 - q % 2, 1 - q // 2) + k
        if q < nb - 1:
            received(weights.at[chip(0), rows(s)], slot(2, q))
            hand_on(chip(0), s, "pass_s", to_partner, partner)
        else:
            for p in range(4):
                received(weights.at[chip(0), piece(s, p)], slot(2, q + p))
                hand_on_piece(chip(0), s, p, to_partner, partner)

    finish(0)

    for ref, name in (
        (pair_recv, "pair_s"),
        (acc, "one_s"),
        (acc.at[pl.ds(0, 3)], "rot_s"),
        (low_send.at[pl.ds(0, 3)], "low_s"),
        (parts_dp.at[pl.ds(0, n - 1)], "norm_s"),
        (acc, "out_s"),
        (weights.at[pl.ds(0, 2)], "pass_s"),
    ):
        sent(ref, sem[name].at[0])

    @pl.when(z == 0)
    def _():
        sent(parts_mp, sem["mesh_s"].at[0])

    @pl.when(z > 0)
    def _():
        sent(totals.at[0], sem["mesh_s"].at[0])

    received(weights.at[pl.ds(0, 2)], to_partner)


def store_kernel(weights, master, first, second, weights_out, master_out, first_out, second_out, sem):
    nb = weights.shape[0]
    pairs = [(weights.at[b], weights_out.at[b]) for b in range(nb)]
    pairs += [(master, master_out), (first, first_out), (second, second_out)]
    copies = [
        pltpu.make_async_copy(src, dst, sem.at[i]) for i, (src, dst) in enumerate(pairs)
    ]
    for copy in copies:
        copy.start()
    for copy in copies:
        copy.wait()


def per_device(n, m, grad_parts, master, first_moment, second_moment, left_basis, right_basis):
    nb, rb, cols = master.shape
    blk = rb * n
    args = (grad_parts, master, first_moment, second_moment, left_basis, right_basis)
    if n != 2 * nb or nb != 4 or m != 4:
        return per_device_general(n, m, *args)
    bf16, f32 = jnp.bfloat16, jnp.float32
    half = blk // 2
    scratch = [
        pltpu.VMEM((nb, half, cols), bf16),
        pltpu.VMEM((nb, half, cols), bf16),
        pltpu.VMEM((blk, cols), bf16),
        pltpu.VMEM((blk, cols), bf16),
        pltpu.VMEM((nb, rb, blk), bf16),
        pltpu.VMEM((2, half, cols), bf16),
        pltpu.VMEM((half, cols), bf16),
        pltpu.VMEM((blk, cols), bf16),
        pltpu.VMEM((nb, rb, cols), bf16),
        pltpu.VMEM((nb, rb, cols), bf16),
        pltpu.VMEM((nb, rb, cols), bf16),
        pltpu.VMEM((nb, rb, cols), bf16),
        pltpu.VMEM((blk, cols), bf16),
        pltpu.VMEM((nb, rb, cols), bf16),
        pltpu.VMEM((nb, rb, cols), bf16),
        pltpu.VMEM((8, cols), f32),
        pltpu.VMEM((8, 128), f32),
        pltpu.VMEM((n, 8, 128), f32),
        pltpu.VMEM((2, 8, 128), f32),
        pltpu.VMEM((m - 1, 8, 128), f32),
    ] + [pltpu.SemaphoreType.DMA((size,)) for _, size in SEMAPHORES]
    shapes = [
        jax.ShapeDtypeStruct((nb, blk, cols), bf16),
        jax.ShapeDtypeStruct(master.shape, f32),
        jax.ShapeDtypeStruct(master.shape, f32),
        jax.ShapeDtypeStruct(master.shape, f32),
    ]
    hbm = pl.BlockSpec(memory_space=pltpu.HBM)
    results = pl.pallas_call(
        functools.partial(step_kernel, n, m),
        out_shape=[pltpu.VMEM(shape.shape, shape.dtype) for shape in shapes],
        in_specs=[hbm] * 6,
        out_specs=[VMEM] * 4,
        scratch_shapes=scratch,
        compiler_params=pltpu.CompilerParams(
            collective_id=0, has_side_effects=True, vmem_limit_bytes=44 * 1024 * 1024
        ),
    )(grad_parts.reshape(nb, blk, cols), *args[1:])
    return pl.pallas_call(
        store_kernel,
        out_shape=shapes,
        in_specs=[VMEM] * 4,
        out_specs=[hbm] * 4,
        scratch_shapes=[pltpu.SemaphoreType.DMA((nb + 3,))],
        compiler_params=pltpu.CompilerParams(vmem_limit_bytes=1024 * 1024),
    )(*results)


def solution(mesh):
    n, m = mesh.shape["dp"], mesh.shape["mp"]
    return jax.shard_map(
        functools.partial(per_device, n, m),
        mesh=mesh,
        in_specs=(
            P("dp", None, None, "mp"),
            P(None, "dp", "mp"),
            P(None, "dp", "mp"),
            P(None, "dp", "mp"),
            P(None, "dp", "mp"),
            P(None, "dp", "mp"),
        ),
        out_specs=(
            P(None, None, "mp"),
            P(None, "dp", "mp"),
            P(None, "dp", "mp"),
            P(None, "dp", "mp"),
        ),
        check_vma=False,
    )
```
